32 devices in a mesh: dp: 8 (over y, x, core), mp: 4 (over z).
Axes of the slice: x: 2, y: 2, z: 4, core: 2. Of those that a mesh axis runs over, the one named last changes fastest.
Arguments:
- block_input: bfloat16 [4096, 2048], P('dp', 'mp'), may hold values from -6 to 6
- segment_ids: int32 [8, 512], P('dp'), may hold values from 0 to 3, never falling along the last dimension, each value on 1 to 256 neighbouring positions
- expert_ids: int32 [4096, 6], P('dp'), may hold values from 0 to 15, all different within a row; in each aligned block of 512 rows (0 to 511, 512 to 1023, ...) at most 384 rows name the same one
- norm_gain: float32 [2048], replicated, may hold values from 0.5 to 1.5
- query_weight: bfloat16 [3072, 2048], P('mp', 'dp'), may hold values from -0.125 to 0.125
- latent_down: bfloat16 [576, 2048], P('mp', 'dp'), may hold values from -0.125 to 0.125
- latent_gain: float32 [512], replicated, may hold values from 0.5 to 1.5
- latent_up: bfloat16 [4096, 512], P('mp', 'dp'), may hold values from -0.25 to 0.25
- output_weight: bfloat16 [2048, 2048], P('mp', 'dp'), may hold values from -0.375 to 0.375
- moe_gain: float32 [2048], replicated, may hold values from 0.5 to 1.5
- router_weight: bfloat16 [16, 2048], P(None, 'dp'), may hold values from -0.125 to 0.125
- shared_gate: bfloat16 [2816, 2048], P('mp', 'dp'), may hold values from -0.125 to 0.125
- shared_up: bfloat16 [2816, 2048], P('mp', 'dp'), may hold values from -0.125 to 0.125
- shared_down: bfloat16 [2816, 2048], P('mp', 'dp'), may hold values from -0.109375 to 0.109375
- expert_gate: bfloat16 [32, 704, 2048], P(('dp', 'mp')), may hold values from -0.125 to 0.125
- expert_up: bfloat16 [32, 704, 2048], P(('dp', 'mp')), may hold values from -0.125 to 0.125
- expert_down: bfloat16 [32, 704, 2048], P(('dp', 'mp')), may hold values from -0.15625 to 0.15625
- output_grad: bfloat16 [4096, 2048], P('dp', 'mp'), may hold values from -6 to 6
Outputs:
- block_output: bfloat16 [4096, 2048], P('dp', 'mp')
- input_grad: float32 [4096, 2048], P('dp', 'mp')
- norm_gain_grad: float32 [2048], replicated
- query_weight_grad: float32 [3072, 2048], P('mp', 'dp')
- latent_down_grad: float32 [576, 2048], P('mp', 'dp')
- latent_gain_grad: float32 [512], replicated
- latent_up_grad: float32 [4096, 512], P('mp', 'dp')
- output_weight_grad: float32 [2048, 2048], P('mp', 'dp')
- moe_gain_grad: float32 [2048], replicated
- router_grad: float32 [16, 2048], P(None, 'dp')
- shared_gate_grad: float32 [2816, 2048], P('mp', 'dp')
- shared_up_grad: float32 [2816, 2048], P('mp', 'dp')
- shared_down_grad: float32 [2816, 2048], P('mp', 'dp')
- expert_gate_grad: float32 [32, 704, 2048], P(('dp', 'mp'))
- expert_up_grad: float32 [32, 704, 2048], P(('dp', 'mp'))
- expert_down_grad: float32 [32, 704, 2048], P(('dp', 'mp'))
The draws below stay inside these ranges and needn't reach their ends.
Inputs may be any that keep to these rules, and one draw needn't show every extreme that they name: `expert_ids`: each token names 6 different experts. Among the tokens of one index of dp (aligned blocks of 512 tokens) no expert is named more than 384 times, and in every draw some expert is named exactly 384 times there. `segment_ids`: along each packed row the numbers never fall; a document spans 1 to 256 positions and one spans exactly that many.
All inputs are finite; a program needn't handle non-finite values.
Results may differ from the reference program's by a relative error of at most 0.018.
Values may be sent and summed in bfloat16 or wider, within the bound.
A program may use at most 384 MiB of HBM per device.

```python
import math
import jax
import jax.numpy as jnp
import numpy as np
from jax import lax

D = 2048
H = 16
DN = 128
DR = 64
DV = 128
KVL = 512
FE = 1408
TOPK = 6
LEN = 512
FS = 2816
E = 16
TOK_DEV = 512
TOKENS = 4096
ROWS = 8
CAP = 384
N_DP = 8


def block_scale(stream_key, extent, split, low, largest):
    level, own = 1.0, jax.random.fold_in(stream_key, 6)
    for dim, blocks in split:
        steps = jnp.exp(jax.random.uniform(jax.random.fold_in(own, dim), (blocks,), jnp.float32, low / len(split), largest / len(split)))
        level = level * jnp.repeat(steps, extent[dim] // blocks).reshape([-1 if axis == dim else 1 for axis in range(len(extent))])
    return level


def profile(amount, total, reach, slope):
    weights = [(1 << 20) // math.isqrt(rank ** slope) + 1 for rank in range(2, amount + 1)]
    spare, holding = total - reach - (amount - 1), [1] * (amount - 1)
    while spare > 0:
        candidates = [i for i in range(amount - 1) if holding[i] < reach]
        pool, left = sum([weights[i] for i in candidates]), spare
        for i in candidates:
            extra = min(reach - holding[i], max(1, left * weights[i] // pool), spare)
            holding[i] = holding[i] + extra
            spare = spare - extra
    return np.array([reach] + holding)


def ragged(key, amount, total, limit, slope):
    if amount == 2:
        one = jax.random.randint(key, (), max(1, total - limit), min(limit, total - 1) + 1)
        return jnp.stack([one, total - one])
    tallies = jnp.asarray(profile(amount, total, limit, slope), jnp.int32)
    pairs = (amount - 1) // 2
    donor, taker = tallies[1:1 + 2 * pairs:2], tallies[2:2 + 2 * pairs:2]
    margin = jnp.minimum(donor - 1, limit - taker)
    passed = jax.random.randint(jax.random.fold_in(key, 1), (pairs,), 0, 1 << 20) % (margin + 1)
    tallies = tallies.at[1:1 + 2 * pairs:2].set(donor - passed).at[2:2 + 2 * pairs:2].set(taker + passed)
    return tallies[jax.random.permutation(jax.random.fold_in(key, 2), amount)]


def routed_block(key, own, number, rows, number_of, top, bound, lean):
    order = jax.random.permutation(key, number_of)
    packed, ordinary = load_shares(number_of, rows * top, bound, lean, True), load_shares(number_of, rows * top, bound, lean, False)
    places = jnp.arange(number_of)

    def named(lengths, turn):
        used = int((lengths > 0).sum())
        fixed = max(1, used // 4)
        shifted = fixed + (places - fixed + turn * (used - fixed)) % max(1, number_of - fixed)
        return jnp.zeros((number_of,), jnp.int32).at[order[jnp.where(places < fixed, places, shifted)]].set(jnp.asarray(lengths, jnp.int32))

    lengths = jnp.where(number % 4 == 0, named(packed, number // 4), named(ordinary, number - number // 4 - 1))
    mixed = jax.random.permutation(jax.random.fold_in(own, 3), number_of)
    giver, receiver = mixed[0:number_of // 2 * 2:2], mixed[1:number_of // 2 * 2:2]
    room = jnp.minimum(lengths[giver] - 1, bound - lengths[receiver]) // 2
    room = jnp.where((giver == order[0]) | (receiver == order[0]) | (lengths[receiver] == 0), 0, jnp.maximum(room, 0))
    shifted = jax.random.randint(jax.random.fold_in(own, 4), (number_of // 2,), 0, 1 << 20) % (room + 1)
    lengths = lengths.at[giver].add(-shifted).at[receiver].add(shifted)
    labels = jnp.searchsorted(jnp.cumsum(lengths), jnp.arange(rows * top), side="right").astype(jnp.int32)
    grid = labels.reshape(top, rows).T
    grid = grid[jax.random.permutation(jax.random.fold_in(own, 1), rows)]
    turn = jax.random.randint(jax.random.fold_in(own, 2), (rows, 1), 0, top)
    return jnp.take_along_axis(grid, (jnp.arange(top)[None, :] + turn) % top, axis=1)


def load_shares(count, total, bound, slope, full):
    portions = [(1 << 20) // math.isqrt(rank ** slope) + 1 for rank in range(1, count + 1)]
    largest = bound if full else min(bound, max(-(-total // count), total * portions[0] // sum(portions)))
    least = 1 if total - largest >= count - 1 else 0
    counts, surplus = [largest] + [least] * (count - 1), total - largest - least * (count - 1)
    while surplus > 0:
        candidates = [i for i in range(1, count) if counts[i] < largest] or [i for i in range(1, count) if counts[i] < bound]
        pool, remaining = sum([portions[i] for i in candidates]), surplus
        for i in candidates:
            extra = min(bound - counts[i], max(1, remaining * portions[i] // pool), surplus)
            counts[i] = counts[i] + extra
            surplus = surplus - extra
    return np.array(counts)


def scatter_about(stream_key, dims, deviation, bound, shards=(), kind=jnp.bfloat16):
    factor_of = block_scale(stream_key, dims, shards, -0.22, 0.18) if shards else 1.0
    entries = jax.random.normal(stream_key, dims, jnp.float32) * deviation * factor_of
    return jnp.minimum(jnp.maximum(entries, -bound), bound).astype(kind)


def setup_inputs(seed: int = 0) -> dict:
    arg_keys = jax.random.split(jax.random.key(seed), 19)
    block_input = scatter_about(arg_keys[0], (TOKENS, D), 1.0, 6.0, ((0, 8), (1, 4)))
    segment_ids = jax.vmap(lambda own: jnp.searchsorted(jnp.cumsum(ragged(own, 4, LEN, LEN // 2, 1)), jnp.arange(LEN), side="right"))(jax.random.split(arg_keys[1], ROWS)).reshape((ROWS, LEN)).astype(jnp.int32)
    expert_ids_keys = jax.random.split(jax.random.fold_in(arg_keys[2], 1), TOKENS // TOK_DEV)
    expert_ids_turns = jax.random.permutation(jax.random.fold_in(arg_keys[2], 3), TOKENS // TOK_DEV)
    expert_ids = jax.vmap(lambda own, number: routed_block(jax.random.fold_in(arg_keys[2], 2), own, number, TOK_DEV, E, TOPK, CAP, 2))(expert_ids_keys, expert_ids_turns).reshape((TOKENS, TOPK))
    norm_gain = jnp.clip(1.0 + 0.1 * jax.random.normal(arg_keys[3], (D,), jnp.float32), 0.5, 1.5)
    query_weight = scatter_about(arg_keys[4], (H * (DN + DR), D), D ** -0.5, 0.125, ((0, 4), (1, 8)))
    latent_down = scatter_about(arg_keys[5], (KVL + DR, D), D ** -0.5, 0.125, ((0, 4), (1, 8)))
    latent_gain = jnp.clip(1.0 + 0.1 * jax.random.normal(arg_keys[6], (KVL,), jnp.float32), 0.5, 1.5)
    latent_up = scatter_about(arg_keys[7], (H * (DN + DV), KVL), KVL ** -0.5, 0.25, ((0, 4), (1, 8)))
    output_weight = scatter_about(arg_keys[8], (H * DV, D), (H * DV // 8) ** -0.5, 0.375, ((0, 4), (1, 8)))
    moe_gain = jnp.clip(1.0 + 0.1 * jax.random.normal(arg_keys[9], (D,), jnp.float32), 0.5, 1.5)
    router_weight = scatter_about(arg_keys[10], (E, D), D ** -0.5, 0.125, ((1, 8),))
    shared_gate = scatter_about(arg_keys[11], (FS, D), D ** -0.5, 0.125, ((0, 4), (1, 8)))
    shared_up = scatter_about(arg_keys[12], (FS, D), D ** -0.5, 0.125, ((0, 4), (1, 8)))
    shared_down = scatter_about(arg_keys[13], (FS, D), FS ** -0.5, 0.109375, ((0, 4), (1, 8)))
    expert_gate = scatter_about(arg_keys[14], (2 * E, FE // 2, D), D ** -0.5, 0.125, ((0, 32),))
    expert_up = scatter_about(arg_keys[15], (2 * E, FE // 2, D), D ** -0.5, 0.125, ((0, 32),))
    expert_down = scatter_about(arg_keys[16], (2 * E, FE // 2, D), FE ** -0.5, 0.15625, ((0, 32),))
    output_grad = scatter_about(arg_keys[17], (TOKENS, D), 1.0, 6.0, ((0, 8), (1, 4)))
    return {"block_input": block_input, "segment_ids": segment_ids, "expert_ids": expert_ids, "norm_gain": norm_gain, "query_weight": query_weight, "latent_down": latent_down, "latent_gain": latent_gain, "latent_up": latent_up, "output_weight": output_weight, "moe_gain": moe_gain, "router_weight": router_weight, "shared_gate": shared_gate, "shared_up": shared_up, "shared_down": shared_down, "expert_gate": expert_gate, "expert_up": expert_up, "expert_down": expert_down, "output_grad": output_grad}


epsilon = 1e-06
negative = -1e+30

def bround(values):
    return lax.optimization_barrier(values.astype(jnp.bfloat16))

def inv_rms(values):
    return lax.rsqrt(lax.optimization_barrier(jnp.mean(values * values, axis=-1, keepdims=True)) + epsilon)

def rope_tables(length, rot_width):
    half_width = rot_width // 2
    frequency = 10000.0 ** (-(2.0 / rot_width) * jnp.arange(half_width, dtype=jnp.float32))
    angles = jnp.arange(length, dtype=jnp.float32)[:, None] * frequency[None, :]
    return (jnp.cos(angles), jnp.sin(angles))

def rotate(values, cosine, sine_tab):
    half_width = values.shape[-1] // 2
    leading = values[..., :half_width]
    trailing = values[..., half_width:]
    return jnp.concatenate([leading * cosine - trailing * sine_tab, trailing * cosine + leading * sine_tab], axis=-1)

def unrotate(values, cosine, sine_tab):
    half_width = values.shape[-1] // 2
    leading = values[..., :half_width]
    trailing = values[..., half_width:]
    return jnp.concatenate([leading * cosine + trailing * sine_tab, trailing * cosine - leading * sine_tab], axis=-1)

def silu_grad(preact):
    sigmoid_val = jax.nn.sigmoid(preact)
    return sigmoid_val * (1.0 + preact * (1.0 - sigmoid_val))

def seg_mask(seg_row):
    places = jnp.arange(seg_row.shape[0], dtype=jnp.int32)
    return (seg_row[:, None] == seg_row[None, :]) & (places[None, :] <= places[:, None])

def scores(q_no, q_ro, k_no, k_ro, seg_row):
    logit_raw = jnp.einsum('ihd,jhd->hij', q_no.astype(jnp.float32), k_no.astype(jnp.float32))
    logit_raw = logit_raw + jnp.einsum('ihd,jd->hij', q_ro.astype(jnp.float32), k_ro.astype(jnp.float32))
    logit_raw = logit_raw * (DN + DR) ** (-0.5)
    return jnp.where(seg_mask(seg_row)[None], logit_raw, negative)

def attend_forward(pieces):
    q_no, q_ro, k_no, k_ro, v_all, seg_row = pieces
    logits = scores(q_no, q_ro, k_no, k_ro, seg_row)
    log_total = jnp.log(lax.optimization_barrier(jnp.sum(jnp.exp(logits), axis=-1, keepdims=True)))
    prob_bf = bround(jnp.exp(logits - log_total))
    mixed_rows = jnp.einsum('hij,jhd->ihd', prob_bf.astype(jnp.float32), v_all.astype(jnp.float32))
    return (bround(mixed_rows), log_total[..., 0])

def attend_backward(pieces):
    q_no, q_ro, k_no, k_ro, v_all, seg_row, log_total, grad_out = pieces
    logits = scores(q_no, q_ro, k_no, k_ro, seg_row)
    probs = jnp.exp(logits - log_total[..., None])
    prob_bf = bround(probs).astype(jnp.float32)
    grad_f = grad_out.astype(jnp.float32)
    prob_grad = jnp.einsum('ihd,jhd->hij', grad_f, v_all.astype(jnp.float32))
    row_dot = lax.optimization_barrier(jnp.sum(probs * prob_grad, axis=-1, keepdims=True))
    score_grad = bround(probs * (prob_grad - row_dot) * (DN + DR) ** (-0.5)).astype(jnp.float32)
    dq_nope = jnp.einsum('hij,jhd->ihd', score_grad, k_no.astype(jnp.float32))
    dq_rope = jnp.einsum('hij,jd->ihd', score_grad, k_ro.astype(jnp.float32))
    dk_nope = jnp.einsum('hij,ihd->jhd', score_grad, q_no.astype(jnp.float32))
    dk_rope = jnp.einsum('hij,ihd->jd', score_grad, q_ro.astype(jnp.float32))
    dv_all = jnp.einsum('hij,ihd->jhd', prob_bf, grad_f)
    return (dq_nope, dq_rope, dk_nope, dk_rope, dv_all)

def reference(block_input, segment_ids, expert_ids, norm_gain, query_weight, latent_down, latent_gain, latent_up, output_weight, moe_gain, router_weight, shared_gate, shared_up, shared_down, expert_gate, expert_up, expert_down, output_grad):
    cosine, sine_tab = rope_tables(LEN, DR)
    inputs = block_input.astype(jnp.float32)
    scale_one = inv_rms(inputs)
    normed = bround(inputs * scale_one * norm_gain)
    query_all = jnp.dot(normed, query_weight.T, preferred_element_type=jnp.float32).reshape(ROWS, LEN, H, DN + DR)
    latent = bround(jnp.dot(normed, latent_down.T, preferred_element_type=jnp.float32)).astype(jnp.float32)
    latent_main = latent[:, :KVL]
    scale_lat = inv_rms(latent_main)
    latent_normed = bround(latent_main * scale_lat * latent_gain)
    key_rope = bround(rotate(latent[:, KVL:].reshape(ROWS, LEN, DR), cosine, sine_tab))
    keys_values = jnp.dot(latent_normed, latent_up.T, preferred_element_type=jnp.float32).reshape(ROWS, LEN, H, DN + DV)
    key_nope = bround(keys_values[..., :DN])
    head_values = bround(keys_values[..., DN:])
    query_nope = bround(query_all[..., :DN])
    query_rope = bround(rotate(query_all[..., DN:], cosine[:, None, :], sine_tab[:, None, :]))
    attended, log_totals = lax.map(attend_forward, (query_nope, query_rope, key_nope, key_rope, head_values, segment_ids))
    attended_flat = attended.reshape(TOKENS, H * DV)
    residual = inputs + jnp.dot(attended_flat, output_weight, preferred_element_type=jnp.float32)
    scale_two = inv_rms(residual)
    moe_in = bround(residual * scale_two * moe_gain)
    router_logits = jnp.dot(moe_in, router_weight.T, preferred_element_type=jnp.float32)
    picked = jnp.take_along_axis(router_logits, expert_ids, axis=1)
    picked_exp = jnp.exp(picked)
    gate_prob = picked_exp / lax.optimization_barrier(jnp.sum(picked_exp, axis=-1, keepdims=True))
    shared_g = jnp.dot(moe_in, shared_gate.T, preferred_element_type=jnp.float32)
    shared_u = jnp.dot(moe_in, shared_up.T, preferred_element_type=jnp.float32)
    shared_act = bround(jax.nn.silu(shared_g) * shared_u)
    shared_out = jnp.dot(shared_act, shared_down, preferred_element_type=jnp.float32)
    per_slots = N_DP * CAP
    hidden_block = FE // 2
    block_ids = expert_ids.reshape(N_DP, TOK_DEV * TOPK)
    onehot = (block_ids[..., None] == jnp.arange(E, dtype=jnp.int32)).astype(jnp.int32)
    slot_ids = lax.optimization_barrier(jnp.sum((jnp.cumsum(onehot, axis=1) - onehot) * onehot, axis=-1))
    sources = jnp.arange(N_DP, dtype=jnp.int32)[:, None]
    places = (block_ids * per_slots + sources * CAP + slot_ids).reshape(-1).astype(jnp.int32)
    owners = jnp.full((E * per_slots,), TOKENS * TOPK, dtype=jnp.int32)
    owners = owners.at[places].set(jnp.arange(TOKENS * TOPK, dtype=jnp.int32)).reshape(E, per_slots)
    rows_pad = jnp.concatenate([moe_in, jnp.zeros((1, D), jnp.bfloat16)], axis=0)
    grads_pad = jnp.concatenate([output_grad.astype(jnp.float32), jnp.zeros((1, D), jnp.float32)], axis=0)
    gates_pad = jnp.concatenate([gate_prob.reshape(-1), jnp.zeros((1,), jnp.float32)], axis=0)

    def expert_pass(carry, inputs_e):
        routed, gate_grad, routed_grad = carry
        owner_idx, w_gate, w_up, w_down = inputs_e
        token_idx = owner_idx // TOPK
        row_data = rows_pad[token_idx]
        weight = gates_pad[owner_idx]
        pre_gate = jnp.dot(row_data, w_gate.T, preferred_element_type=jnp.float32)
        pre_up = jnp.dot(row_data, w_up.T, preferred_element_type=jnp.float32)
        activation = bround(jax.nn.silu(pre_gate) * pre_up)
        part_out = bround(jnp.einsum('sjf,jfd->sjd', activation.reshape(per_slots, 2, hidden_block).astype(jnp.float32), w_down.reshape(2, hidden_block, D).astype(jnp.float32)))
        outputs = lax.optimization_barrier(jnp.sum(part_out.astype(jnp.float32), axis=1))
        routed = routed.at[token_idx].add(weight[:, None] * outputs, mode='drop')
        upstream = grads_pad[token_idx]
        gate_grad = gate_grad.at[owner_idx].set(lax.optimization_barrier(jnp.sum(upstream * outputs, axis=-1)), mode='drop')
        scaled = bround(weight[:, None] * upstream)
        act_grad = jnp.dot(scaled, w_down.T, preferred_element_type=jnp.float32)
        gate_pre_grad = bround(act_grad * pre_up * silu_grad(pre_gate))
        up_pre_grad = bround(act_grad * jax.nn.silu(pre_gate))
        down_w_grad = jnp.dot(activation.T, scaled, preferred_element_type=jnp.float32)
        gate_w_grad = jnp.dot(gate_pre_grad.T, row_data, preferred_element_type=jnp.float32)
        up_w_grad = jnp.dot(up_pre_grad.T, row_data, preferred_element_type=jnp.float32)
        back_parts = jnp.einsum('sjf,jfd->sjd', gate_pre_grad.reshape(per_slots, 2, hidden_block).astype(jnp.float32), w_gate.reshape(2, hidden_block, D).astype(jnp.float32))
        back_parts = back_parts + jnp.einsum('sjf,jfd->sjd', up_pre_grad.reshape(per_slots, 2, hidden_block).astype(jnp.float32), w_up.reshape(2, hidden_block, D).astype(jnp.float32))
        row_grads = lax.optimization_barrier(jnp.sum(bround(back_parts).astype(jnp.float32), axis=1))
        routed_grad = routed_grad.at[token_idx].add(row_grads, mode='drop')
        return ((routed, gate_grad, routed_grad), (gate_w_grad, up_w_grad, down_w_grad))
    start_carry = (jnp.zeros((TOKENS, D), jnp.float32), jnp.zeros((TOKENS * TOPK,), jnp.float32), jnp.zeros((TOKENS, D), jnp.float32))
    expert_weights = (owners, expert_gate.reshape(E, FE, D), expert_up.reshape(E, FE, D), expert_down.reshape(E, FE, D))
    (routed, gate_grad, routed_grad), (gate_grads_all, up_grads_all, down_grads_all) = lax.scan(expert_pass, start_carry, expert_weights)
    expert_gate_grad = gate_grads_all.reshape(2 * E, FE // 2, D)
    expert_up_grad = up_grads_all.reshape(2 * E, FE // 2, D)
    expert_down_grad = down_grads_all.reshape(2 * E, FE // 2, D)
    block_output = (residual + routed + shared_out).astype(jnp.bfloat16)
    gate_grad = gate_grad.reshape(TOKENS, TOPK)
    logit_pick_grad = gate_prob * (gate_grad - lax.optimization_barrier(jnp.sum(gate_prob * gate_grad, axis=-1, keepdims=True)))
    chosen = (expert_ids[..., None] == jnp.arange(E, dtype=jnp.int32)).astype(jnp.float32)
    logit_grad = bround(lax.optimization_barrier(jnp.sum(logit_pick_grad[..., None] * chosen, axis=1)))
    router_grad = jnp.dot(logit_grad.T, moe_in, preferred_element_type=jnp.float32)
    shared_act_grad = jnp.dot(output_grad, shared_down.T, preferred_element_type=jnp.float32)
    shared_gate_pre = bround(shared_act_grad * shared_u * silu_grad(shared_g))
    shared_up_pre = bround(shared_act_grad * jax.nn.silu(shared_g))
    shared_down_grad = jnp.dot(shared_act.T, output_grad, preferred_element_type=jnp.float32)
    shared_gate_grad = jnp.dot(shared_gate_pre.T, moe_in, preferred_element_type=jnp.float32)
    shared_up_grad = jnp.dot(shared_up_pre.T, moe_in, preferred_element_type=jnp.float32)
    moe_in_grad = jnp.dot(shared_gate_pre, shared_gate, preferred_element_type=jnp.float32) + jnp.dot(shared_up_pre, shared_up, preferred_element_type=jnp.float32)
    moe_in_grad = moe_in_grad + routed_grad + jnp.dot(logit_grad, router_weight, preferred_element_type=jnp.float32)
    moe_gain_grad = lax.optimization_barrier(jnp.sum(moe_in_grad * residual * scale_two, axis=0))
    residual_grad = output_grad.astype(jnp.float32) + scale_two * moe_gain * moe_in_grad - residual * scale_two ** 3 * lax.optimization_barrier(jnp.mean(moe_in_grad * residual * moe_gain, axis=-1, keepdims=True))
    residual_bf = bround(residual_grad)
    output_weight_grad = jnp.dot(attended_flat.T, residual_bf, preferred_element_type=jnp.float32)
    attended_grad = bround(jnp.dot(residual_bf, output_weight.T, preferred_element_type=jnp.float32)).reshape(ROWS, LEN, H, DV)
    dq_nope, dq_rope, dk_nope, dk_rope, dv_all = lax.map(attend_backward, (query_nope, query_rope, key_nope, key_rope, head_values, segment_ids, log_totals, attended_grad))
    query_grad = bround(jnp.concatenate([dq_nope, unrotate(dq_rope, cosine[:, None, :], sine_tab[:, None, :])], axis=-1).reshape(TOKENS, H * (DN + DR)))
    kv_grad = bround(jnp.concatenate([dk_nope, dv_all], axis=-1).reshape(TOKENS, H * (DN + DV)))
    latent_up_grad = jnp.dot(kv_grad.T, latent_normed, preferred_element_type=jnp.float32)
    normed_lat_grad = jnp.dot(kv_grad, latent_up, preferred_element_type=jnp.float32)
    latent_gain_grad = lax.optimization_barrier(jnp.sum(normed_lat_grad * latent_main * scale_lat, axis=0))
    main_grad = scale_lat * latent_gain * normed_lat_grad - latent_main * scale_lat ** 3 * lax.optimization_barrier(jnp.mean(normed_lat_grad * latent_main * latent_gain, axis=-1, keepdims=True))
    rope_grad = unrotate(dk_rope, cosine, sine_tab).reshape(TOKENS, DR)
    latent_grad = bround(jnp.concatenate([main_grad, rope_grad], axis=-1))
    latent_down_grad = jnp.dot(latent_grad.T, normed, preferred_element_type=jnp.float32)
    query_weight_grad = jnp.dot(query_grad.T, normed, preferred_element_type=jnp.float32)
    normed_grad = jnp.dot(query_grad, query_weight, preferred_element_type=jnp.float32) + jnp.dot(latent_grad, latent_down, preferred_element_type=jnp.float32)
    norm_gain_grad = lax.optimization_barrier(jnp.sum(normed_grad * inputs * scale_one, axis=0))
    input_grad = residual_grad + scale_one * norm_gain * normed_grad - inputs * scale_one ** 3 * lax.optimization_barrier(jnp.mean(normed_grad * inputs * norm_gain, axis=-1, keepdims=True))
    return (block_output, input_grad, norm_gain_grad, query_weight_grad, latent_down_grad, latent_gain_grad, latent_up_grad, output_weight_grad, moe_gain_grad, router_grad, shared_gate_grad, shared_up_grad, shared_down_grad, expert_gate_grad, expert_up_grad, expert_down_grad)
```

```python
import jax
import jax.numpy as jnp
from jax import lax
from jax.sharding import PartitionSpec as P

H = 16
DN = 128
DR = 64
DV = 128
KVL = 512
TOPK = 6
LEN = 512
SEQ_DEV = 1


epsilon = 1e-06
negative = -1e30


def rope_tables(length, rot_width):
    half_width = rot_width // 2
    frequency = 10000.0 ** (-(2.0 / rot_width) * jnp.arange(half_width, dtype=jnp.float32))
    angles = jnp.arange(length, dtype=jnp.float32)[:, None] * frequency[None, :]
    return (jnp.cos(angles), jnp.sin(angles))


def rotate(values, cosine, sine_tab):
    half_width = values.shape[-1] // 2
    leading = values[..., :half_width]
    trailing = values[..., half_width:]
    return jnp.concatenate(
        [leading * cosine - trailing * sine_tab, trailing * cosine + leading * sine_tab], axis=-1
    )


def unrotate(values, cosine, sine_tab):
    half_width = values.shape[-1] // 2
    leading = values[..., :half_width]
    trailing = values[..., half_width:]
    return jnp.concatenate(
        [leading * cosine + trailing * sine_tab, trailing * cosine - leading * sine_tab], axis=-1
    )


def silu_grad(preact):
    sigmoid_val = jax.nn.sigmoid(preact)
    return sigmoid_val * (1.0 + preact * (1.0 - sigmoid_val))


def seg_mask(seg_row):
    places = jnp.arange(seg_row.shape[0], dtype=jnp.int32)
    return (seg_row[:, None] == seg_row[None, :]) & (places[None, :] <= places[:, None])


def score_block(q_no, q_ro, k_no, k_ro, seg_row):
    logits = jnp.einsum("ihd,jhd->hij", q_no, k_no, preferred_element_type=jnp.float32)
    logits = logits + jnp.einsum("ihd,jd->hij", q_ro, k_ro, preferred_element_type=jnp.float32)
    logits = logits * (q_no.shape[-1] + q_ro.shape[-1]) ** (-0.5)
    return jnp.where(seg_mask(seg_row)[None], logits, negative)


def attend_forward(pieces):
    q_no, q_ro, k_no, k_ro, v_all, seg_row = pieces
    logits = score_block(q_no, q_ro, k_no, k_ro, seg_row)
    log_total = jnp.log(jnp.sum(jnp.exp(logits), axis=-1, keepdims=True))
    prob_bf = jnp.exp(logits - log_total).astype(jnp.bfloat16)
    mixed_rows = jnp.einsum("hij,jhd->ihd", prob_bf, v_all, preferred_element_type=jnp.float32)
    return (mixed_rows.astype(jnp.bfloat16), log_total[..., 0])


def attend_backward(pieces):
    q_no, q_ro, k_no, k_ro, v_all, seg_row, log_total, grad_out = pieces
    logits = score_block(q_no, q_ro, k_no, k_ro, seg_row)
    probs = jnp.exp(logits - log_total[..., None])
    prob_bf = probs.astype(jnp.bfloat16)
    prob_grad = jnp.einsum("ihd,jhd->hij", grad_out, v_all, preferred_element_type=jnp.float32)
    row_dot = jnp.sum(probs * prob_grad, axis=-1, keepdims=True)
    score_scale = (q_no.shape[-1] + q_ro.shape[-1]) ** (-0.5)
    score_grad = (probs * (prob_grad - row_dot) * score_scale).astype(jnp.bfloat16)
    dq_nope = jnp.einsum("hij,jhd->ihd", score_grad, k_no, preferred_element_type=jnp.float32)
    dq_rope = jnp.einsum("hij,jd->ihd", score_grad, k_ro, preferred_element_type=jnp.float32)
    dk_nope = jnp.einsum("hij,ihd->jhd", score_grad, q_no, preferred_element_type=jnp.float32)
    dk_rope = jnp.einsum("hij,ihd->jd", score_grad, q_ro, preferred_element_type=jnp.float32)
    dv_all = jnp.einsum("hij,ihd->jhd", prob_bf, grad_out, preferred_element_type=jnp.float32)
    return (dq_nope, dq_rope, dk_nope, dk_rope, dv_all)


def full_rows(piece_rows):
    return lax.all_gather(piece_rows, "mp", axis=1, tiled=True)


def mp_total(partial_value):
    return lax.psum(partial_value, "mp")


def mp_share(partial_value):
    return lax.psum_scatter(
        partial_value.astype(jnp.bfloat16), "mp", scatter_dimension=1, tiled=True
    ).astype(jnp.float32)


def dp_share(partial_value):
    return lax.psum_scatter(
        partial_value.astype(jnp.bfloat16), "dp", scatter_dimension=1, tiled=True
    ).astype(jnp.float32)


def ring_order(dp_count):
    chips = dp_count // 2
    return list(range(chips // 2)) + list(range(chips - 1, chips // 2 - 1, -1))


def ring_move(values, step):
    order = ring_order(lax.axis_size("dp"))
    chips = len(order)
    pairs = [
        (2 * chip + core, 2 * order[(pos + step) % chips] + core)
        for pos, chip in enumerate(order)
        for core in range(2)
    ]
    return lax.ppermute(values, "dp", pairs)


def core_swap(values):
    return lax.ppermute(values, "dp", [(i, i ^ 1) for i in range(lax.axis_size("dp"))])


def direct_move(values, step, swap):
    order = ring_order(lax.axis_size("dp"))
    chips = len(order)
    pairs = [
        (2 * chip + core, 2 * order[(pos + step) % chips] + (core ^ swap))
        for pos, chip in enumerate(order)
        for core in range(2)
    ]
    return lax.ppermute(values, "dp", pairs)


def spread(own):
    chips = lax.axis_size("dp") // 2
    half = own.shape[0] // 2
    same = [None] * chips
    same[0] = ahead = behind = own
    for step in range(1, chips // 2):
        ahead = same[step] = ring_move(ahead, 1)
        behind = same[chips - step] = ring_move(behind, -1)
    same[chips // 2] = jnp.concatenate(
        [ring_move(ahead[:half], 1), ring_move(behind[half:], -1)], axis=0
    )
    return [jnp.concatenate([rows, core_swap(rows)], axis=0) for rows in same]


def add_bf(left, right):
    return (left.astype(jnp.float32) + right.astype(jnp.float32)).astype(jnp.bfloat16)


def collect(chunks):
    chips = len(chunks)
    rows = chunks[0].shape[0] // 2
    half = rows // 2
    merged = [add_bf(chunk[:rows], core_swap(chunk[rows:])) for chunk in chunks]
    far = merged[chips // 2]
    carry_back, carry_on = ring_move(far[:half], -1), ring_move(far[half:], 1)
    for step in range(chips // 2 - 1, 0, -1):
        back, on = merged[step], merged[chips - step]
        if step == chips // 2 - 1:
            back = jnp.concatenate([add_bf(back[:half], carry_back), back[half:]], axis=0)
            on = jnp.concatenate([on[:half], add_bf(on[half:], carry_on)], axis=0)
        else:
            back, on = add_bf(back, carry_back), add_bf(on, carry_on)
        carry_back, carry_on = ring_move(back, -1), ring_move(on, 1)
    total = merged[0].astype(jnp.float32) + carry_back.astype(jnp.float32)
    return total + carry_on.astype(jnp.float32)


def shards(
    block_input,
    segment_ids,
    expert_ids,
    norm_gain,
    query_weight,
    latent_down,
    latent_gain,
    latent_up,
    output_weight,
    moe_gain,
    router_weight,
    shared_gate,
    shared_up,
    shared_down,
    expert_gate,
    expert_up,
    expert_down,
    output_grad,
):
    model_width = norm_gain.shape[0]
    tokens_here = block_input.shape[0]
    share_width = block_input.shape[1]
    mp_count = lax.axis_size("mp")
    mp_place = lax.axis_index("mp")
    dp_count = lax.axis_size("dp")
    heads_here = H // mp_count
    experts_all = router_weight.shape[0]
    experts_group = experts_all // dp_count
    chips = dp_count // 2
    own_expert = lax.axis_index("dp") * experts_group + mp_place // 2
    expert_places = jnp.arange(experts_all, dtype=jnp.int32)
    picked_mask = jnp.max(
        (expert_ids[..., None] == expert_places).astype(jnp.float32), axis=1
    )
    own_gate = expert_gate[0]
    own_up = expert_up[0]
    own_down = expert_down[0]
    cosine, sine_tab = rope_tables(LEN, DR)
    inputs = block_input.astype(jnp.float32)
    gain_one = lax.dynamic_slice_in_dim(norm_gain, mp_place * share_width, share_width)
    inputs_full = full_rows(block_input).astype(jnp.float32)
    scale_one = lax.rsqrt(jnp.mean(inputs_full * inputs_full, axis=1, keepdims=True) + epsilon)
    normed = (inputs_full * scale_one * norm_gain).astype(jnp.bfloat16)
    mask_chunks = spread(picked_mask)
    query_w, down_w, up_w, out_w, router_w, sgate_w, sup_w, sdown_w = (
        lax.all_gather(query_weight, "dp", axis=1, tiled=True),
        lax.all_gather(latent_down, "dp", axis=1, tiled=True),
        lax.all_gather(latent_up, "dp", axis=1, tiled=True),
        lax.all_gather(output_weight, "dp", axis=1, tiled=True),
        lax.all_gather(router_weight, "dp", axis=1, tiled=True),
        lax.all_gather(shared_gate, "dp", axis=1, tiled=True),
        lax.all_gather(shared_up, "dp", axis=1, tiled=True),
        lax.all_gather(shared_down, "dp", axis=1, tiled=True),
    )
    query_all = jnp.dot(normed, query_w.T, preferred_element_type=jnp.float32).reshape(
        SEQ_DEV, LEN, heads_here, DN + DR
    )
    latent = full_rows(
        jnp.dot(normed, down_w.T, preferred_element_type=jnp.float32).astype(jnp.bfloat16)
    ).astype(jnp.float32)
    latent_main = latent[:, :KVL]
    scale_lat = lax.rsqrt(jnp.mean(latent_main * latent_main, axis=-1, keepdims=True) + epsilon)
    latent_normed = (latent_main * scale_lat * latent_gain).astype(jnp.bfloat16)
    key_rope = rotate(latent[:, KVL:].reshape(SEQ_DEV, LEN, DR), cosine, sine_tab).astype(
        jnp.bfloat16
    )
    keys_values = jnp.dot(latent_normed, up_w.T, preferred_element_type=jnp.float32).reshape(
        SEQ_DEV, LEN, heads_here, DN + DV
    )
    key_nope = keys_values[..., :DN].astype(jnp.bfloat16)
    head_values = keys_values[..., DN:].astype(jnp.bfloat16)
    query_nope = query_all[..., :DN].astype(jnp.bfloat16)
    query_rope = rotate(query_all[..., DN:], cosine[:, None, :], sine_tab[:, None, :]).astype(
        jnp.bfloat16
    )
    attended, log_totals = lax.map(
        attend_forward, (query_nope, query_rope, key_nope, key_rope, head_values, segment_ids)
    )
    attended_flat = attended.reshape(tokens_here, heads_here * DV)
    residual = inputs + mp_share(jnp.dot(attended_flat, out_w, preferred_element_type=jnp.float32))
    gain_two = lax.dynamic_slice_in_dim(moe_gain, mp_place * share_width, share_width)
    scale_two = lax.rsqrt(mp_total(jnp.sum(residual * residual, axis=1)) / model_width + epsilon)[
        :, None
    ]
    moe_share = (residual * scale_two * gain_two).astype(jnp.bfloat16)
    moe_in = full_rows(moe_share)
    grad_full = full_rows(output_grad)
    grad_chunks = spread(grad_full)
    row_chunks = spread(moe_in)
    router_logits = jnp.dot(moe_in, router_w.T, preferred_element_type=jnp.float32)

    def masked_gates(logits, mask):
        pick_exp = jnp.exp(jnp.where(mask > 0, logits, negative))
        return pick_exp / jnp.sum(pick_exp, axis=-1, keepdims=True)

    gate_prob = masked_gates(router_logits, picked_mask)
    shared_g = jnp.dot(moe_in, sgate_w.T, preferred_element_type=jnp.float32)
    shared_u = jnp.dot(moe_in, sup_w.T, preferred_element_type=jnp.float32)
    shared_act = (jax.nn.silu(shared_g) * shared_u).astype(jnp.bfloat16)
    shared_part = jnp.dot(shared_act, sdown_w, preferred_element_type=jnp.float32)
    up_router = jnp.concatenate([own_up, router_w], axis=0)
    hidden = own_up.shape[0]
    own_column = (expert_places == own_expert).astype(jnp.float32)
    act_all, gate_pre_all, up_pre_all, out_chunks, back_chunks, gate_grads = [], [], [], [], [], []
    for rows_k, grads_k, mask_k in zip(row_chunks, grad_chunks, mask_chunks):
        pre_gate = jnp.dot(rows_k, own_gate.T, preferred_element_type=jnp.float32)
        up_logits = jnp.dot(rows_k, up_router.T, preferred_element_type=jnp.float32)
        pre_up = up_logits[:, :hidden]
        gate_k = jnp.sum(
            masked_gates(up_logits[:, hidden:], mask_k) * own_column, axis=1, keepdims=True
        )
        act_grad = jnp.dot(grads_k, own_down.T, preferred_element_type=jnp.float32)
        activation = jax.nn.silu(pre_gate) * pre_up
        gate_grads.append(jnp.sum(activation * act_grad, axis=1))
        act_grad = act_grad * gate_k
        act_bf = (activation * gate_k).astype(jnp.bfloat16)
        gate_pre = (act_grad * pre_up * silu_grad(pre_gate)).astype(jnp.bfloat16)
        up_pre = (act_grad * jax.nn.silu(pre_gate)).astype(jnp.bfloat16)
        back_chunks.append(
            (
                jnp.dot(gate_pre, own_gate, preferred_element_type=jnp.float32)
                + jnp.dot(up_pre, own_up, preferred_element_type=jnp.float32)
            ).astype(jnp.bfloat16)
        )
        out_chunks.append(
            jnp.dot(act_bf, own_down, preferred_element_type=jnp.float32).astype(jnp.bfloat16)
        )
        act_all.append(act_bf)
        gate_pre_all.append(gate_pre)
        up_pre_all.append(up_pre)
    routed_back = collect(back_chunks)
    rows_all, grads_all = jnp.concatenate(row_chunks), jnp.concatenate(grad_chunks)
    expert_down_grad = jnp.dot(
        jnp.concatenate(act_all).T, grads_all, preferred_element_type=jnp.float32
    )[None]
    expert_gate_grad = jnp.dot(
        jnp.concatenate(gate_pre_all).T, rows_all, preferred_element_type=jnp.float32
    )[None]
    expert_up_grad = jnp.dot(
        jnp.concatenate(up_pre_all).T, rows_all, preferred_element_type=jnp.float32
    )[None]
    order = jnp.array(ring_order(dp_count), jnp.int32)
    dp_place = lax.axis_index("dp")
    ring_place = jnp.argmax((order == dp_place // 2).astype(jnp.int32)).astype(jnp.int32)
    gate_grad = jnp.zeros((tokens_here, experts_all), jnp.float32)
    for k, both in enumerate(gate_grads):
        chip_from = jnp.sum(
            jnp.where(jnp.arange(chips) == (ring_place + k) % chips, order, 0)
        )
        for swap in range(2):
            piece = both[swap * tokens_here : (swap + 1) * tokens_here]
            if k or swap:
                piece = direct_move(piece, -k, swap)
            device_from = 2 * chip_from + (dp_place % 2 if swap == 0 else 1 - dp_place % 2)
            expert_from = device_from * experts_group + mp_place // 2
            gate_grad = gate_grad + piece[:, None] * (expert_places == expert_from).astype(
                jnp.float32
            )
    gate_grad = mp_total(gate_grad)
    routed_part = collect(out_chunks)
    moe_total = mp_share(shared_part + routed_part)
    block_output = (residual + moe_total).astype(jnp.bfloat16)
    logit_grad = (
        gate_prob * (gate_grad - jnp.sum(gate_prob * gate_grad, axis=-1, keepdims=True))
    ).astype(jnp.bfloat16)
    router_full_grad = jnp.dot(logit_grad.T, moe_in, preferred_element_type=jnp.float32)
    router_back = jnp.dot(logit_grad, router_w, preferred_element_type=jnp.float32)
    shared_act_grad = jnp.dot(grad_full, sdown_w.T, preferred_element_type=jnp.float32)
    shared_gate_pre = (shared_act_grad * shared_u * silu_grad(shared_g)).astype(jnp.bfloat16)
    shared_up_pre = (shared_act_grad * jax.nn.silu(shared_g)).astype(jnp.bfloat16)
    sdown_grad = jnp.dot(shared_act.T, grad_full, preferred_element_type=jnp.float32)
    sgate_grad = jnp.dot(shared_gate_pre.T, moe_in, preferred_element_type=jnp.float32)
    sup_grad = jnp.dot(shared_up_pre.T, moe_in, preferred_element_type=jnp.float32)
    shared_back = jnp.dot(shared_gate_pre, sgate_w, preferred_element_type=jnp.float32) + jnp.dot(
        shared_up_pre, sup_w, preferred_element_type=jnp.float32
    )
    router_mine = lax.dynamic_slice_in_dim(router_back, mp_place * share_width, share_width, axis=1)
    moe_in_grad = mp_share(shared_back + routed_back) + router_mine
    moe_gain_part = jnp.sum(moe_in_grad * residual * scale_two, axis=0)
    stat_two = mp_total(jnp.sum(moe_in_grad * residual * gain_two, axis=1))[:, None] / model_width
    residual_grad = (
        output_grad.astype(jnp.float32)
        + scale_two * gain_two * moe_in_grad
        - residual * scale_two**3 * stat_two
    )
    residual_bf = full_rows(residual_grad.astype(jnp.bfloat16))
    out_w_grad = jnp.dot(attended_flat.T, residual_bf, preferred_element_type=jnp.float32)
    attended_grad = (
        jnp.dot(residual_bf, out_w.T, preferred_element_type=jnp.float32)
        .astype(jnp.bfloat16)
        .reshape(SEQ_DEV, LEN, heads_here, DV)
    )
    dq_nope, dq_rope, dk_nope, dk_rope, dv_all = lax.map(
        attend_backward,
        (
            query_nope,
            query_rope,
            key_nope,
            key_rope,
            head_values,
            segment_ids,
            log_totals,
            attended_grad,
        ),
    )
    query_grad = (
        jnp.concatenate(
            [dq_nope, unrotate(dq_rope, cosine[:, None, :], sine_tab[:, None, :])], axis=-1
        )
        .reshape(tokens_here, heads_here * (DN + DR))
        .astype(jnp.bfloat16)
    )
    kv_grad = (
        jnp.concatenate([dk_nope, dv_all], axis=-1)
        .reshape(tokens_here, heads_here * (DN + DV))
        .astype(jnp.bfloat16)
    )
    up_w_grad = jnp.dot(kv_grad.T, latent_normed, preferred_element_type=jnp.float32)
    normed_lat_grad = jnp.dot(kv_grad, up_w, preferred_element_type=jnp.float32)
    latent_gain_part = jnp.sum(normed_lat_grad * latent_main * scale_lat, axis=0)
    main_grad = scale_lat * latent_gain * normed_lat_grad - latent_main * scale_lat**3 * jnp.mean(
        normed_lat_grad * latent_main * latent_gain, axis=-1, keepdims=True
    )
    rope_grad = unrotate(dk_rope, cosine, sine_tab).reshape(tokens_here, DR)
    latent_grad = mp_share(jnp.concatenate([main_grad, rope_grad], axis=-1)).astype(jnp.bfloat16)
    down_w_grad = jnp.dot(latent_grad.T, normed, preferred_element_type=jnp.float32)
    query_w_grad = jnp.dot(query_grad.T, normed, preferred_element_type=jnp.float32)
    normed_grad = mp_share(
        jnp.dot(query_grad, query_w, preferred_element_type=jnp.float32)
        + jnp.dot(latent_grad, down_w, preferred_element_type=jnp.float32)
    )
    norm_gain_part = jnp.sum(normed_grad * inputs * scale_one, axis=0)
    stat_one = mp_total(jnp.sum(normed_grad * inputs * gain_one, axis=1))[:, None] / model_width
    input_grad = (
        residual_grad + scale_one * gain_one * normed_grad - inputs * scale_one**3 * stat_one
    )
    zero_gain = jnp.zeros((model_width,), jnp.float32)
    gain_one_full = lax.dynamic_update_slice_in_dim(
        zero_gain, norm_gain_part, mp_place * share_width, axis=0
    )
    gain_two_full = lax.dynamic_update_slice_in_dim(
        zero_gain, moe_gain_part, mp_place * share_width, axis=0
    )
    norm_gain_grad, moe_gain_grad, latent_gain_grad = lax.psum(
        (gain_one_full, gain_two_full, latent_gain_part), ("dp", "mp")
    )
    (
        query_weight_grad,
        latent_down_grad,
        latent_up_grad,
        output_weight_grad,
        router_grad,
        shared_gate_grad,
        shared_up_grad,
        shared_down_grad,
    ) = (
        dp_share(query_w_grad),
        dp_share(down_w_grad),
        dp_share(up_w_grad),
        dp_share(out_w_grad),
        dp_share(router_full_grad),
        dp_share(sgate_grad),
        dp_share(sup_grad),
        dp_share(sdown_grad),
    )
    return (
        block_output,
        input_grad,
        norm_gain_grad,
        query_weight_grad,
        latent_down_grad,
        latent_gain_grad,
        latent_up_grad,
        output_weight_grad,
        moe_gain_grad,
        router_grad,
        shared_gate_grad,
        shared_up_grad,
        shared_down_grad,
        expert_gate_grad,
        expert_up_grad,
        expert_down_grad,
    )


def solution(mesh):
    in_specs = (
        P("dp", "mp"),
        P("dp", None),
        P("dp", None),
        P(),
        P("mp", "dp"),
        P("mp", "dp"),
        P(),
        P("mp", "dp"),
        P("mp", "dp"),
        P(),
        P(None, "dp"),
        P("mp", "dp"),
        P("mp", "dp"),
        P("mp", "dp"),
        P(("dp", "mp"), None, None),
        P(("dp", "mp"), None, None),
        P(("dp", "mp"), None, None),
        P("dp", "mp"),
    )
    out_specs = (
        P("dp", "mp"),
        P("dp", "mp"),
        P(),
        P("mp", "dp"),
        P("mp", "dp"),
        P(),
        P("mp", "dp"),
        P("mp", "dp"),
        P(),
        P(None, "dp"),
        P("mp", "dp"),
        P("mp", "dp"),
        P("mp", "dp"),
        P(("dp", "mp"), None, None),
        P(("dp", "mp"), None, None),
        P(("dp", "mp"), None, None),
    )
    return jax.shard_map(shards, mesh=mesh, in_specs=in_specs, out_specs=out_specs, check_vma=False)
```

```python
import functools

import jax
import jax.numpy as jnp
from jax import lax
from jax.experimental import pallas as pl
from jax.experimental.pallas import tpu as pltpu
from jax.sharding import PartitionSpec as P

MESH = pl.DeviceIdType.MESH

H = 16
DN = 128
DR = 64
DV = 128
KVL = 512
TOPK = 6
LEN = 512
SEQ_DEV = 1


epsilon = 1e-06
negative = -1e30


def rope_tables(length, rot_width):
    half_width = rot_width // 2
    frequency = 10000.0 ** (-(2.0 / rot_width) * jnp.arange(half_width, dtype=jnp.float32))
    angles = jnp.arange(length, dtype=jnp.float32)[:, None] * frequency[None, :]
    return (jnp.cos(angles), jnp.sin(angles))


def rotate(values, cosine, sine_tab):
    half_width = values.shape[-1] // 2
    leading = values[..., :half_width]
    trailing = values[..., half_width:]
    return jnp.concatenate(
        [leading * cosine - trailing * sine_tab, trailing * cosine + leading * sine_tab], axis=-1
    )


def unrotate(values, cosine, sine_tab):
    half_width = values.shape[-1] // 2
    leading = values[..., :half_width]
    trailing = values[..., half_width:]
    return jnp.concatenate(
        [leading * cosine + trailing * sine_tab, trailing * cosine - leading * sine_tab], axis=-1
    )


def silu_grad(preact):
    sigmoid_val = jax.nn.sigmoid(preact)
    return sigmoid_val * (1.0 + preact * (1.0 - sigmoid_val))


def seg_mask(seg_row):
    places = jnp.arange(seg_row.shape[0], dtype=jnp.int32)
    return (seg_row[:, None] == seg_row[None, :]) & (places[None, :] <= places[:, None])


def score_block(q_no, q_ro, k_no, k_ro, seg_row):
    logits = jnp.einsum("ihd,jhd->hij", q_no, k_no, preferred_element_type=jnp.float32)
    logits = logits + jnp.einsum("ihd,jd->hij", q_ro, k_ro, preferred_element_type=jnp.float32)
    logits = logits * (q_no.shape[-1] + q_ro.shape[-1]) ** (-0.5)
    return jnp.where(seg_mask(seg_row)[None], logits, negative)


def attend_forward(pieces):
    q_no, q_ro, k_no, k_ro, v_all, seg_row = pieces
    logits = score_block(q_no, q_ro, k_no, k_ro, seg_row)
    log_total = jnp.log(jnp.sum(jnp.exp(logits), axis=-1, keepdims=True))
    prob_bf = jnp.exp(logits - log_total).astype(jnp.bfloat16)
    mixed_rows = jnp.einsum("hij,jhd->ihd", prob_bf, v_all, preferred_element_type=jnp.float32)
    return (mixed_rows.astype(jnp.bfloat16), log_total[..., 0])


def attend_backward(pieces):
    q_no, q_ro, k_no, k_ro, v_all, seg_row, log_total, grad_out = pieces
    logits = score_block(q_no, q_ro, k_no, k_ro, seg_row)
    probs = jnp.exp(logits - log_total[..., None])
    prob_bf = probs.astype(jnp.bfloat16)
    prob_grad = jnp.einsum("ihd,jhd->hij", grad_out, v_all, preferred_element_type=jnp.float32)
    row_dot = jnp.sum(probs * prob_grad, axis=-1, keepdims=True)
    score_scale = (q_no.shape[-1] + q_ro.shape[-1]) ** (-0.5)
    score_grad = (probs * (prob_grad - row_dot) * score_scale).astype(jnp.bfloat16)
    dq_nope = jnp.einsum("hij,jhd->ihd", score_grad, k_no, preferred_element_type=jnp.float32)
    dq_rope = jnp.einsum("hij,jd->ihd", score_grad, k_ro, preferred_element_type=jnp.float32)
    dk_nope = jnp.einsum("hij,ihd->jhd", score_grad, q_no, preferred_element_type=jnp.float32)
    dk_rope = jnp.einsum("hij,ihd->jd", score_grad, q_ro, preferred_element_type=jnp.float32)
    dv_all = jnp.einsum("hij,ihd->jhd", prob_bf, grad_out, preferred_element_type=jnp.float32)
    return (dq_nope, dq_rope, dk_nope, dk_rope, dv_all)


def full_rows(piece_rows):
    return lax.all_gather(piece_rows, "mp", axis=1, tiled=True)


def mp_share(partial_value):
    return lax.psum_scatter(
        partial_value.astype(jnp.bfloat16), "mp", scatter_dimension=1, tiled=True
    ).astype(jnp.float32)


def ring_order(dp_count):
    chips = dp_count // 2
    return list(range(chips // 2)) + list(range(chips - 1, chips // 2 - 1, -1))


def ring_neighbours(dp_count):
    order = ring_order(dp_count)
    chips = len(order)
    place = lax.axis_index("dp")
    chip, core = place // 2, place % 2
    pos = jnp.where(chip < chips // 2, chip, chips // 2 + chips - 1 - chip)

    def device_at(p):
        p = lax.rem(p + 2 * chips, chips)
        c = jnp.where(p < chips // 2, p, chips // 2 + chips - 1 - p)
        return 2 * c + core

    return place, pos, core, device_at


def gather_kernel(dp_count, mp_count, axes, has_rows, *refs):
    count = len(axes)
    if not has_rows:
        refs = (None, *refs[:count], None, *refs[count:])
    rows_ref, parts = refs[0], refs[1 : 1 + count]
    rows_out, wholes = refs[1 + count], refs[2 + count : 2 + 2 * count]
    send, receive, local, line_send, line_receive, line_local = refs[2 + 2 * count :]
    chips = dp_count // 2
    reach = chips // 2
    place, pos, core, device_at = ring_neighbours(dp_count)
    line = lax.axis_index("mp")
    on, back = device_at(pos + 1), device_at(pos - 1)
    other = place + 1 - 2 * core

    barrier = pltpu.get_barrier_semaphore()
    for target in (on, back, other):
        pl.semaphore_signal(barrier, device_id={"dp": target}, device_id_type=MESH)

    waits = 3
    if has_rows:

        @pl.when(line > 0)
        def _():
            pl.semaphore_signal(barrier, device_id={"mp": line - 1}, device_id_type=MESH)

        @pl.when(line < mp_count - 1)
        def _():
            pl.semaphore_signal(barrier, device_id={"mp": line + 1}, device_id_type=MESH)

        waits = 3 + (line > 0).astype(jnp.int32) + (line < mp_count - 1).astype(jnp.int32)
    pl.semaphore_wait(barrier, waits)

    width = rows_ref.shape[1] if has_rows else 0

    def columns(owner):
        return rows_out.at[:, pl.ds(pl.multiple_of(owner * width, width), width)]

    def line_copy(way, hop, source, owner):
        target = line + 1 if way == 0 else line - 1
        return pltpu.make_async_remote_copy(
            source,
            columns(owner),
            line_send.at[way, hop],
            line_receive.at[way, hop],
            device_id={"mp": target},
            device_id_type=MESH,
        )

    ends = (line < mp_count - 1, line > 0)

    def holds(way, hop):
        return line >= hop if way == 0 else line + hop <= mp_count - 1

    def owner_of(way, hop):
        return jnp.clip(line - hop if way == 0 else line + hop, 0, mp_count - 1)

    if has_rows:
        for way in range(2):

            @pl.when(ends[way])
            def _(way=way):
                line_copy(way, 0, rows_ref, line).start()

        keep_rows = pltpu.make_async_copy(rows_ref, columns(line), line_local)
        keep_rows.start()

    def block(i, owner, low, high):
        size = parts[i].shape[axes[i]]
        start = pl.multiple_of(owner * size, size)
        if axes[i] == 1:
            return wholes[i].at[pl.ds(low, high - low), pl.ds(start, size)]
        return wholes[i].at[pl.ds(start + low, high - low), :]

    def split(i, piece):
        rows = parts[i].shape[0]
        middle = rows // 32 * 16
        return ((0, rows), (0, middle), (middle, rows))[piece]

    def ring_copy(i, slot, source, owner, piece, target):
        low, high = split(i, piece)
        if source is None:
            source = block(i, owner, low, high)
        return pltpu.make_async_remote_copy(
            source,
            block(i, owner, low, high),
            send.at[i, slot],
            receive.at[i, slot],
            device_id={"dp": target},
            device_id_type=MESH,
        )

    def empty(i, piece):
        low, high = split(i, piece)
        return low == high

    started, kept = [], []
    for i in range(count):
        for way, target in ((0, on), (1, back)):
            piece = 0 if reach > 1 else 1 + way
            if not empty(i, piece):
                low, high = split(i, piece)
                copy = ring_copy(
                    i, way * reach, parts[i].at[pl.ds(low, high - low), :], place, piece, target
                )
                copy.start()
                started.append(copy)
        copy = ring_copy(i, 2 * reach, parts[i], place, 0, other)
        copy.start()
        started.append(copy)
        copy = pltpu.make_async_copy(
            parts[i], block(i, place, 0, parts[i].shape[0]), local.at[i]
        )
        copy.start()
        kept.append(copy)

    def line_step(hop):
        for way in range(2):

            @pl.when(holds(way, hop))
            def _(way=way):
                line_copy(way, hop - 1, rows_ref, owner_of(way, hop)).wait_recv()

            if hop < mp_count - 1:

                @pl.when(holds(way, hop) & ends[way])
                def _(way=way):
                    owner = owner_of(way, hop)
                    line_copy(way, hop, columns(owner), owner).start()

    def ring_step(i, hop):
        for way, target in ((0, on), (1, back)):
            piece = 0 if hop < reach else 1 + way
            if empty(i, piece):
                continue
            owner = device_at(pos - hop if way == 0 else pos + hop)
            ring_copy(i, way * reach + hop - 1, None, owner, piece, other).wait_recv()
            if hop < reach:
                ahead = 0 if hop + 1 < reach else 1 + way
                if not empty(i, ahead):
                    copy = ring_copy(i, way * reach + hop, None, owner, ahead, target)
                    copy.start()
                    started.append(copy)
            copy = ring_copy(i, 2 * reach + 1 + way * reach + hop - 1, None, owner, piece, other)
            copy.start()
            started.append(copy)

    line_hops = list(range(1, mp_count)) if has_rows else []
    for hop in range(1, reach + 1):
        for i in range(count):
            ring_step(i, hop)
        if line_hops:
            line_step(line_hops.pop(0))
    for hop in line_hops:
        line_step(hop)

    for i in range(count):
        twin = place + 1 - 2 * core
        ring_copy(i, 2 * reach, parts[i], twin, 0, other).wait_recv()
        for hop in range(1, reach + 1):
            for way in range(2):
                piece = 0 if hop < reach else 1 + way
                if empty(i, piece):
                    continue
                owner = device_at(pos - hop if way == 0 else pos + hop) + 1 - 2 * core
                ring_copy(
                    i, 2 * reach + 1 + way * reach + hop - 1, None, owner, piece, other
                ).wait_recv()
    for copy in started:
        copy.wait_send()
    for copy in kept:
        copy.wait()
    if not has_rows:
        return
    for way in range(2):

        @pl.when(ends[way])
        def _(way=way):
            line_copy(way, 0, rows_ref, line).wait_send()

        for hop in range(1, mp_count - 1):

            @pl.when(holds(way, hop) & ends[way])
            def _(way=way, hop=hop):
                owner = owner_of(way, hop)
                line_copy(way, hop, columns(owner), owner).wait_send()

    keep_rows.wait()


def gather_all(rows, parts, axes, collective_id):
    dp_count, mp_count = lax.axis_size("dp"), lax.axis_size("mp")
    arrays = [part for part in (rows, *parts) if part is not None]
    shapes = [
        jax.ShapeDtypeStruct(
            tuple(s * dp_count if a == axis else s for a, s in enumerate(part.shape)), part.dtype
        )
        for part, axis in zip(parts, axes)
    ]
    semaphores = [
        pltpu.SemaphoreType.DMA((len(parts), 4 * (dp_count // 4) + 1)),
        pltpu.SemaphoreType.DMA((len(parts), 4 * (dp_count // 4) + 1)),
        pltpu.SemaphoreType.DMA((len(parts),)),
        pltpu.SemaphoreType.DMA((2, mp_count)),
        pltpu.SemaphoreType.DMA((2, mp_count)),
        pltpu.SemaphoreType.DMA,
    ]
    if rows is not None:
        shapes.insert(
            0, jax.ShapeDtypeStruct((rows.shape[0], rows.shape[1] * mp_count), rows.dtype)
        )
    moved = 2 * sum(shape.size for shape in shapes)
    return pl.pallas_call(
        functools.partial(gather_kernel, dp_count, mp_count, tuple(axes), rows is not None),
        out_shape=shapes,
        in_specs=[pl.BlockSpec(memory_space=pltpu.VMEM)] * len(arrays),
        out_specs=[pl.BlockSpec(memory_space=pl.ANY)] * len(arrays),
        scratch_shapes=semaphores,
        compiler_params=pltpu.CompilerParams(collective_id=collective_id, has_side_effects=True),
        cost_estimate=pl.CostEstimate(flops=0, bytes_accessed=16 * moved, transcendentals=0),
        name="gather_all",
    )(*arrays)


def ring_move(values, step):
    order = ring_order(lax.axis_size("dp"))
    chips = len(order)
    pairs = [
        (2 * chip + core, 2 * order[(pos + step) % chips] + core)
        for pos, chip in enumerate(order)
        for core in range(2)
    ]
    return lax.ppermute(values, "dp", pairs)


def core_swap(values):
    return lax.ppermute(values, "dp", [(i, i ^ 1) for i in range(lax.axis_size("dp"))])


def direct_move(values, step, swap):
    order = ring_order(lax.axis_size("dp"))
    chips = len(order)
    pairs = [
        (2 * chip + core, 2 * order[(pos + step) % chips] + (core ^ swap))
        for pos, chip in enumerate(order)
        for core in range(2)
    ]
    return lax.ppermute(values, "dp", pairs)


def spread(own):
    chips = lax.axis_size("dp") // 2
    half = own.shape[0] // 2
    same = [None] * chips
    same[0] = ahead = behind = own
    for step in range(1, chips // 2):
        ahead = same[step] = ring_move(ahead, 1)
        behind = same[chips - step] = ring_move(behind, -1)
    same[chips // 2] = jnp.concatenate(
        [ring_move(ahead[:half], 1), ring_move(behind[half:], -1)], axis=0
    )
    return [jnp.concatenate([rows, core_swap(rows)], axis=0) for rows in same]


def add_bf(left, right):
    return (left.astype(jnp.float32) + right.astype(jnp.float32)).astype(jnp.bfloat16)


def collect(pairs):
    chips = len(pairs)
    half = pairs[0][0].shape[0] // 2
    merged = [add_bf(same, core_swap(other)) for same, other in pairs]
    far = merged[chips // 2]
    carry_back, carry_on = ring_move(far[:half], -1), ring_move(far[half:], 1)
    for step in range(chips // 2 - 1, 0, -1):
        back, on = merged[step], merged[chips - step]
        if step == chips // 2 - 1:
            back = jnp.concatenate([add_bf(back[:half], carry_back), back[half:]], axis=0)
            on = jnp.concatenate([on[:half], add_bf(on[half:], carry_on)], axis=0)
        else:
            back, on = add_bf(back, carry_back), add_bf(on, carry_on)
        carry_back, carry_on = ring_move(back, -1), ring_move(on, 1)
    total = merged[0].astype(jnp.float32) + carry_back.astype(jnp.float32)
    return total + carry_on.astype(jnp.float32)


def relative_devices():
    dp_count = lax.axis_size("dp")
    _, pos, core, device_at = ring_neighbours(dp_count)
    places = []
    for k in range(dp_count // 2):
        same = device_at(pos - k)
        places.append((same, same + 1 - 2 * core))
    return places


def weight_grads(rows, cotangents, places):
    width = rows.shape[1] // lax.axis_size("dp")
    pairs = []
    for pair in places:
        pairs.append(
            tuple(
                jnp.dot(
                    lax.dynamic_slice_in_dim(rows, place * width, width, axis=1).T,
                    cotangents,
                    preferred_element_type=jnp.float32,
                ).astype(jnp.bfloat16)
                for place in pair
            )
        )
    return collect(pairs)


def line_total(partial_value):
    count = lax.axis_size("mp")
    total = partial_value
    for shift in range(1, count):
        total = total + lax.ppermute(
            partial_value, "mp", [(i, (i + shift) % count) for i in range(count)]
        )
    return total


def shards(
    block_input,
    segment_ids,
    expert_ids,
    norm_gain,
    query_weight,
    latent_down,
    latent_gain,
    latent_up,
    output_weight,
    moe_gain,
    router_weight,
    shared_gate,
    shared_up,
    shared_down,
    expert_gate,
    expert_up,
    expert_down,
    output_grad,
):
    model_width = norm_gain.shape[0]
    tokens_here = block_input.shape[0]
    share_width = block_input.shape[1]
    mp_count = lax.axis_size("mp")
    mp_place = lax.axis_index("mp")
    dp_count = lax.axis_size("dp")
    heads_here = H // mp_count
    experts_all = router_weight.shape[0]
    experts_group = experts_all // dp_count
    chips = dp_count // 2
    own_expert = lax.axis_index("dp") * experts_group + mp_place // 2
    expert_places = jnp.arange(experts_all, dtype=jnp.int32)
    picked_mask = jnp.max(
        (expert_ids[..., None] == expert_places).astype(jnp.float32), axis=1
    )
    own_gate = expert_gate[0]
    own_up = expert_up[0]
    own_down = expert_down[0]
    cosine, sine_tab = rope_tables(LEN, DR)
    inputs = block_input.astype(jnp.float32)
    gain_one = lax.dynamic_slice_in_dim(norm_gain, mp_place * share_width, share_width)
    gathered = gather_all(
        block_input,
        (query_weight, latent_down, latent_up.T, output_weight, router_weight),
        (1, 1, 0, 1, 1),
        1,
    )
    inputs_full = gathered[0].astype(jnp.float32)
    query_w, down_w, up_wt, out_w, router_w = gathered[1:]
    scale_one = lax.rsqrt(jnp.mean(inputs_full * inputs_full, axis=1, keepdims=True) + epsilon)
    normed = (inputs_full * scale_one * norm_gain).astype(jnp.bfloat16)
    places = relative_devices()
    mask_chunks = spread(picked_mask)
    late_grad, _ = lax.optimization_barrier((output_grad, gathered[0]))
    grad_full = full_rows(late_grad)
    grad_chunks = spread(grad_full)
    query_all = jnp.dot(normed, query_w.T, preferred_element_type=jnp.float32).reshape(
        SEQ_DEV, LEN, heads_here, DN + DR
    )
    latent = full_rows(
        jnp.dot(normed, down_w.T, preferred_element_type=jnp.float32).astype(jnp.bfloat16)
    ).astype(jnp.float32)
    latent_main = latent[:, :KVL]
    scale_lat = lax.rsqrt(jnp.mean(latent_main * latent_main, axis=-1, keepdims=True) + epsilon)
    latent_normed = (latent_main * scale_lat * latent_gain).astype(jnp.bfloat16)
    key_rope = rotate(latent[:, KVL:].reshape(SEQ_DEV, LEN, DR), cosine, sine_tab).astype(
        jnp.bfloat16
    )
    keys_values = jnp.dot(latent_normed, up_wt, preferred_element_type=jnp.float32).reshape(
        SEQ_DEV, LEN, heads_here, DN + DV
    )
    key_nope = keys_values[..., :DN].astype(jnp.bfloat16)
    head_values = keys_values[..., DN:].astype(jnp.bfloat16)
    query_nope = query_all[..., :DN].astype(jnp.bfloat16)
    query_rope = rotate(query_all[..., DN:], cosine[:, None, :], sine_tab[:, None, :]).astype(
        jnp.bfloat16
    )
    attended, log_totals = lax.map(
        attend_forward, (query_nope, query_rope, key_nope, key_rope, head_values, segment_ids)
    )
    attended_flat = attended.reshape(tokens_here, heads_here * DV)
    attended_part = jnp.dot(attended_flat, out_w, preferred_element_type=jnp.float32).astype(
        jnp.bfloat16
    )
    attended_sum = mp_share(attended_part)
    shared_parts, _ = lax.optimization_barrier(
        ((shared_gate, shared_up, shared_down), attended_part)
    )
    sgate_w, sup_w, sdown_w = gather_all(None, shared_parts, (1, 1, 1), 2)
    attended_sum, sgate_w, sup_w, sdown_w = lax.optimization_barrier(
        (attended_sum, sgate_w, sup_w, sdown_w)
    )
    residual = inputs + attended_sum
    gain_two = lax.dynamic_slice_in_dim(moe_gain, mp_place * share_width, share_width)
    residual_full = full_rows(residual.astype(jnp.bfloat16)).astype(jnp.float32)
    scale_two = lax.rsqrt(
        jnp.mean(residual_full * residual_full, axis=1, keepdims=True) + epsilon
    )
    moe_in = (residual_full * scale_two * moe_gain).astype(jnp.bfloat16)
    row_chunks = spread(moe_in)
    router_logits = jnp.dot(moe_in, router_w.T, preferred_element_type=jnp.float32)

    def masked_gates(logits, mask):
        pick_exp = jnp.exp(jnp.where(mask > 0, logits, negative))
        return pick_exp / jnp.sum(pick_exp, axis=-1, keepdims=True)

    gate_prob = masked_gates(router_logits, picked_mask)
    shared_g = jnp.dot(moe_in, sgate_w.T, preferred_element_type=jnp.float32)
    shared_u = jnp.dot(moe_in, sup_w.T, preferred_element_type=jnp.float32)
    shared_act = (jax.nn.silu(shared_g) * shared_u).astype(jnp.bfloat16)
    shared_part = jnp.dot(shared_act, sdown_w, preferred_element_type=jnp.float32)
    up_router = jnp.concatenate([own_up, router_w], axis=0)
    hidden = own_up.shape[0]
    own_column = (expert_places == own_expert).astype(jnp.float32)
    act_all, gate_pre_all, up_pre_all, out_chunks, back_chunks, gate_grads = [], [], [], [], [], []
    for rows_k, grads_k, mask_k in zip(row_chunks, grad_chunks, mask_chunks):
        pre_gate = jnp.dot(rows_k, own_gate.T, preferred_element_type=jnp.float32)
        up_logits = jnp.dot(rows_k, up_router.T, preferred_element_type=jnp.float32)
        pre_up = up_logits[:, :hidden]
        gate_k = jnp.sum(
            masked_gates(up_logits[:, hidden:], mask_k) * own_column, axis=1, keepdims=True
        )
        act_grad = jnp.dot(grads_k, own_down.T, preferred_element_type=jnp.float32)
        activation = jax.nn.silu(pre_gate) * pre_up
        gate_grads.append(jnp.sum(activation * act_grad, axis=1))
        act_grad = act_grad * gate_k
        act_bf = (activation * gate_k).astype(jnp.bfloat16)
        gate_pre = (act_grad * pre_up * silu_grad(pre_gate)).astype(jnp.bfloat16)
        up_pre = (act_grad * jax.nn.silu(pre_gate)).astype(jnp.bfloat16)
        back_chunks.append(
            tuple(
                (
                    jnp.dot(gate_pre[part], own_gate, preferred_element_type=jnp.float32)
                    + jnp.dot(up_pre[part], own_up, preferred_element_type=jnp.float32)
                ).astype(jnp.bfloat16)
                for part in (slice(None, tokens_here), slice(tokens_here, None))
            )
        )
        out_chunks.append(
            tuple(
                jnp.dot(act_bf[part], own_down, preferred_element_type=jnp.float32).astype(
                    jnp.bfloat16
                )
                for part in (slice(None, tokens_here), slice(tokens_here, None))
            )
        )
        act_all.append(act_bf)
        gate_pre_all.append(gate_pre)
        up_pre_all.append(up_pre)
    routed_back = collect(back_chunks)
    rows_all, grads_all = jnp.concatenate(row_chunks), jnp.concatenate(grad_chunks)
    expert_down_grad = jnp.dot(
        jnp.concatenate(act_all).T, grads_all, preferred_element_type=jnp.float32
    )[None]
    expert_gate_grad = jnp.dot(
        jnp.concatenate(gate_pre_all).T, rows_all, preferred_element_type=jnp.float32
    )[None]
    expert_up_grad = jnp.dot(
        jnp.concatenate(up_pre_all).T, rows_all, preferred_element_type=jnp.float32
    )[None]
    order = jnp.array(ring_order(dp_count), jnp.int32)
    dp_place = lax.axis_index("dp")
    ring_place = jnp.argmax((order == dp_place // 2).astype(jnp.int32)).astype(jnp.int32)
    gate_grad = jnp.zeros((tokens_here, experts_all), jnp.float32)
    for k, both in enumerate(gate_grads):
        chip_from = jnp.sum(
            jnp.where(jnp.arange(chips) == (ring_place + k) % chips, order, 0)
        )
        for swap in range(2):
            piece = both[swap * tokens_here : (swap + 1) * tokens_here]
            if k or swap:
                piece = direct_move(piece, -k, swap)
            device_from = 2 * chip_from + (dp_place % 2 if swap == 0 else 1 - dp_place % 2)
            expert_from = device_from * experts_group + mp_place // 2
            gate_grad = gate_grad + piece[:, None] * (expert_places == expert_from).astype(
                jnp.float32
            )
    gate_grad = line_total(gate_grad)
    routed_part = collect(out_chunks)
    moe_total = mp_share(shared_part + routed_part)
    block_output = (residual + moe_total).astype(jnp.bfloat16)
    logit_grad = (
        gate_prob * (gate_grad - jnp.sum(gate_prob * gate_grad, axis=-1, keepdims=True))
    ).astype(jnp.bfloat16)
    router_back = jnp.dot(logit_grad, router_w, preferred_element_type=jnp.float32)
    shared_act_grad = jnp.dot(grad_full, sdown_w.T, preferred_element_type=jnp.float32)
    shared_gate_pre = (shared_act_grad * shared_u * silu_grad(shared_g)).astype(jnp.bfloat16)
    shared_up_pre = (shared_act_grad * jax.nn.silu(shared_g)).astype(jnp.bfloat16)
    sdown_grad = weight_grads(grad_full, shared_act, places)
    hidden_here = shared_gate_pre.shape[1]
    moe_rows_grad = weight_grads(
        moe_in, jnp.concatenate([shared_gate_pre, shared_up_pre, logit_grad], axis=1), places
    )
    shared_back = jnp.dot(shared_gate_pre, sgate_w, preferred_element_type=jnp.float32) + jnp.dot(
        shared_up_pre, sup_w, preferred_element_type=jnp.float32
    )
    router_mine = lax.dynamic_slice_in_dim(router_back, mp_place * share_width, share_width, axis=1)
    moe_in_grad = mp_share(shared_back + routed_back) + router_mine
    back_full = full_rows(moe_in_grad.astype(jnp.bfloat16)).astype(jnp.float32)
    moe_gain_part = jnp.sum(back_full * residual_full * scale_two, axis=0)
    stat_two = jnp.mean(back_full * residual_full * moe_gain, axis=1, keepdims=True)
    residual_grad = (
        output_grad.astype(jnp.float32)
        + scale_two * gain_two * moe_in_grad
        - residual * scale_two**3 * stat_two
    )
    residual_bf = (
        grad_full.astype(jnp.float32)
        + scale_two * moe_gain * back_full
        - residual_full * scale_two**3 * stat_two
    ).astype(jnp.bfloat16)
    out_w_grad = weight_grads(residual_bf, attended_flat, places)
    attended_grad = (
        jnp.dot(residual_bf, out_w.T, preferred_element_type=jnp.float32)
        .astype(jnp.bfloat16)
        .reshape(SEQ_DEV, LEN, heads_here, DV)
    )
    dq_nope, dq_rope, dk_nope, dk_rope, dv_all = lax.map(
        attend_backward,
        (
            query_nope,
            query_rope,
            key_nope,
            key_rope,
            head_values,
            segment_ids,
            log_totals,
            attended_grad,
        ),
    )
    query_grad = (
        jnp.concatenate(
            [dq_nope, unrotate(dq_rope, cosine[:, None, :], sine_tab[:, None, :])], axis=-1
        )
        .reshape(tokens_here, heads_here * (DN + DR))
        .astype(jnp.bfloat16)
    )
    kv_grad = (
        jnp.concatenate([dk_nope, dv_all], axis=-1)
        .reshape(tokens_here, heads_here * (DN + DV))
        .astype(jnp.bfloat16)
    )
    up_w_grad = weight_grads(latent_normed, kv_grad, places)
    normed_lat_grad = jnp.dot(kv_grad, up_wt.T, preferred_element_type=jnp.float32)
    latent_gain_part = jnp.sum(normed_lat_grad * latent_main * scale_lat, axis=0)
    main_grad = scale_lat * latent_gain * normed_lat_grad - latent_main * scale_lat**3 * jnp.mean(
        normed_lat_grad * latent_main * latent_gain, axis=-1, keepdims=True
    )
    rope_grad = unrotate(dk_rope, cosine, sine_tab).reshape(tokens_here, DR)
    latent_grad = mp_share(jnp.concatenate([main_grad, rope_grad], axis=-1)).astype(jnp.bfloat16)
    query_rows_grad = weight_grads(
        normed, jnp.concatenate([query_grad, latent_grad], axis=1), places
    )
    normed_part = jnp.dot(query_grad, query_w, preferred_element_type=jnp.float32) + jnp.dot(
        latent_grad, down_w, preferred_element_type=jnp.float32
    )
    weighted_part = normed_part * inputs_full
    norm_gain_part = jnp.sum(weighted_part * scale_one, axis=0)
    stat_one = line_total(jnp.sum(weighted_part * norm_gain, axis=1))[:, None] / model_width
    moe_gain_part = jnp.where(mp_place == 0, moe_gain_part, 0.0)
    norm_gain_grad, moe_gain_grad, latent_gain_grad = lax.psum(
        (norm_gain_part, moe_gain_part, latent_gain_part), ("dp", "mp")
    )
    normed_grad = mp_share(normed_part)
    input_grad = (
        residual_grad + scale_one * gain_one * normed_grad - inputs * scale_one**3 * stat_one
    )
    query_width = query_grad.shape[1]
    query_weight_grad = query_rows_grad[:, :query_width].T
    latent_down_grad = query_rows_grad[:, query_width:].T
    latent_up_grad = up_w_grad.T
    output_weight_grad = out_w_grad.T
    shared_gate_grad = moe_rows_grad[:, :hidden_here].T
    shared_up_grad = moe_rows_grad[:, hidden_here : 2 * hidden_here].T
    router_grad = moe_rows_grad[:, 2 * hidden_here :].T
    shared_down_grad = sdown_grad.T
    return (
        block_output,
        input_grad,
        norm_gain_grad,
        query_weight_grad,
        latent_down_grad,
        latent_gain_grad,
        latent_up_grad,
        output_weight_grad,
        moe_gain_grad,
        router_grad,
        shared_gate_grad,
        shared_up_grad,
        shared_down_grad,
        expert_gate_grad,
        expert_up_grad,
        expert_down_grad,
    )


def solution(mesh):
    in_specs = (
        P("dp", "mp"),
        P("dp", None),
        P("dp", None),
        P(),
        P("mp", "dp"),
        P("mp", "dp"),
        P(),
        P("mp", "dp"),
        P("mp", "dp"),
        P(),
        P(None, "dp"),
        P("mp", "dp"),
        P("mp", "dp"),
        P("mp", "dp"),
        P(("dp", "mp"), None, None),
        P(("dp", "mp"), None, None),
        P(("dp", "mp"), None, None),
        P("dp", "mp"),
    )
    out_specs = (
        P("dp", "mp"),
        P("dp", "mp"),
        P(),
        P("mp", "dp"),
        P("mp", "dp"),
        P(),
        P("mp", "dp"),
        P("mp", "dp"),
        P(),
        P(None, "dp"),
        P("mp", "dp"),
        P("mp", "dp"),
        P("mp", "dp"),
        P(("dp", "mp"), None, None),
        P(("dp", "mp"), None, None),
        P(("dp", "mp"), None, None),
    )
    return jax.shard_map(shards, mesh=mesh, in_specs=in_specs, out_specs=out_specs, check_vma=False)
```

```python
import functools

import jax
import jax.numpy as jnp
from jax import lax
from jax.experimental import pallas as pl
from jax.experimental.pallas import tpu as pltpu
from jax.sharding import PartitionSpec as P

MESH = pl.DeviceIdType.MESH

H = 16
DN = 128
DR = 64
DV = 128
KVL = 512
TOPK = 6
LEN = 512
SEQ_DEV = 1


epsilon = 1e-06
negative = -1e30


def rope_tables(length, rot_width):
    half_width = rot_width // 2
    frequency = 10000.0 ** (-(2.0 / rot_width) * jnp.arange(half_width, dtype=jnp.float32))
    angles = jnp.arange(length, dtype=jnp.float32)[:, None] * frequency[None, :]
    return (jnp.cos(angles), jnp.sin(angles))


def rotate(values, cosine, sine_tab):
    half_width = values.shape[-1] // 2
    leading = values[..., :half_width]
    trailing = values[..., half_width:]
    return jnp.concatenate(
        [leading * cosine - trailing * sine_tab, trailing * cosine + leading * sine_tab], axis=-1
    )


def unrotate(values, cosine, sine_tab):
    half_width = values.shape[-1] // 2
    leading = values[..., :half_width]
    trailing = values[..., half_width:]
    return jnp.concatenate(
        [leading * cosine + trailing * sine_tab, trailing * cosine - leading * sine_tab], axis=-1
    )


def silu_grad(preact):
    sigmoid_val = jax.nn.sigmoid(preact)
    return sigmoid_val * (1.0 + preact * (1.0 - sigmoid_val))


def head_lanes(shape, heads):
    lane = lax.broadcasted_iota(jnp.int32, shape, 1)
    per_head = shape[1] // (2 * heads)
    mine = lax.rem(lane, heads * per_head) // per_head == pl.program_id(0)
    return mine.astype(jnp.float32)


def attend_forward_kernel(
    heads, scale, q_ref, q_rope_ref, keys_ref, k_rope_ref, seg_row_ref, seg_col_ref, out_ref, probs_ref
):
    width = q_ref.shape[1]
    q_rope = (q_rope_ref[...].astype(jnp.float32) * head_lanes(q_rope_ref.shape, heads)).astype(
        jnp.bfloat16
    )
    nt = (((1,), (1,)), ((), ()))
    logits = lax.dot_general(
        q_ref[...], keys_ref[:, :width], nt, preferred_element_type=jnp.float32
    )
    logits = logits + lax.dot_general(
        q_rope, k_rope_ref[...], nt, preferred_element_type=jnp.float32
    )
    row = lax.broadcasted_iota(jnp.int32, logits.shape, 0)
    column = lax.broadcasted_iota(jnp.int32, logits.shape, 1)
    kept = (seg_col_ref[...] == seg_row_ref[...]) & (column <= row)
    weights = jnp.exp(jnp.where(kept, logits * scale, negative))
    probs = (weights / jnp.sum(weights, axis=1, keepdims=True)).astype(jnp.bfloat16)
    probs_ref[0] = probs
    out_ref[...] = jnp.dot(
        probs, keys_ref[:, width:], preferred_element_type=jnp.float32
    ).astype(jnp.bfloat16)


def attend_forward(q_nope, q_rope, keys_values, k_rope, seg_row, heads, scale):
    length = q_nope.shape[0]
    whole = lambda h: (0, 0)
    mine = lambda h: (0, h)
    return pl.pallas_call(
        functools.partial(attend_forward_kernel, heads, scale),
        grid=(heads,),
        out_shape=(
            jax.ShapeDtypeStruct((length, heads * DV), jnp.bfloat16),
            jax.ShapeDtypeStruct((heads, length, length), jnp.bfloat16),
        ),
        in_specs=[
            pl.BlockSpec((length, DN), mine),
            pl.BlockSpec(q_rope.shape, whole),
            pl.BlockSpec((length, DN + DV), mine),
            pl.BlockSpec(k_rope.shape, whole),
            pl.BlockSpec((1, length), whole),
            pl.BlockSpec((length, 1), whole),
        ],
        out_specs=(
            pl.BlockSpec((length, DV), mine),
            pl.BlockSpec((1, length, length), lambda h: (h, 0, 0)),
        ),
        cost_estimate=pl.CostEstimate(
            flops=2 * heads * length * length * (DN + DV + q_rope.shape[1]),
            bytes_accessed=4 * heads * length * length,
            transcendentals=heads * length * length,
        ),
        name="attend_forward",
    )(q_nope, q_rope, keys_values, k_rope, seg_row, seg_row.T)


def attend_backward_kernel(
    heads,
    scale,
    probs_ref,
    grad_ref,
    q_ref,
    q_rope_ref,
    keys_ref,
    k_rope_ref,
    dq_ref,
    dq_rope_ref,
    dkeys_ref,
    dk_rope_ref,
):
    width = q_ref.shape[1]
    lanes = head_lanes(q_rope_ref.shape, heads)
    q_rope = (q_rope_ref[...].astype(jnp.float32) * lanes).astype(jnp.bfloat16)
    probs, grad = probs_ref[0], grad_ref[...]
    prob_grad = lax.dot_general(
        grad, keys_ref[:, width:], (((1,), (1,)), ((), ())), preferred_element_type=jnp.float32
    )
    wide = probs.astype(jnp.float32)
    row_dot = jnp.sum(wide * prob_grad, axis=1, keepdims=True)
    score_grad = (wide * (prob_grad - row_dot) * scale).astype(jnp.bfloat16)
    tn = (((0,), (0,)), ((), ()))
    dq_ref[...] = jnp.dot(
        score_grad, keys_ref[:, :width], preferred_element_type=jnp.float32
    ).astype(jnp.bfloat16)
    dq_rope = lanes * jnp.dot(score_grad, k_rope_ref[...], preferred_element_type=jnp.float32)
    dk_rope = lax.dot_general(score_grad, q_rope, tn, preferred_element_type=jnp.float32)
    dkeys_ref[:, :width] = lax.dot_general(
        score_grad, q_ref[...], tn, preferred_element_type=jnp.float32
    ).astype(jnp.bfloat16)
    dkeys_ref[:, width:] = lax.dot_general(
        probs, grad, tn, preferred_element_type=jnp.float32
    ).astype(jnp.bfloat16)

    @pl.when(pl.program_id(0) == 0)
    def _():
        dq_rope_ref[...] = dq_rope
        dk_rope_ref[...] = dk_rope

    @pl.when(pl.program_id(0) > 0)
    def _():
        dq_rope_ref[...] += dq_rope
        dk_rope_ref[...] += dk_rope


def attend_backward(probs, grad, q_nope, q_rope, keys_values, k_rope, heads, scale):
    length = q_nope.shape[0]
    whole = lambda h: (0, 0)
    mine = lambda h: (0, h)
    return pl.pallas_call(
        functools.partial(attend_backward_kernel, heads, scale),
        grid=(heads,),
        out_shape=(
            jax.ShapeDtypeStruct(q_nope.shape, jnp.bfloat16),
            jax.ShapeDtypeStruct(q_rope.shape, jnp.float32),
            jax.ShapeDtypeStruct(keys_values.shape, jnp.bfloat16),
            jax.ShapeDtypeStruct(q_rope.shape, jnp.float32),
        ),
        in_specs=[
            pl.BlockSpec((1, length, length), lambda h: (h, 0, 0)),
            pl.BlockSpec((length, DV), mine),
            pl.BlockSpec((length, DN), mine),
            pl.BlockSpec(q_rope.shape, whole),
            pl.BlockSpec((length, DN + DV), mine),
            pl.BlockSpec(k_rope.shape, whole),
        ],
        out_specs=(
            pl.BlockSpec((length, DN), mine),
            pl.BlockSpec(q_rope.shape, whole),
            pl.BlockSpec((length, DN + DV), mine),
            pl.BlockSpec(q_rope.shape, whole),
        ),
        cost_estimate=pl.CostEstimate(
            flops=2 * heads * length * length * 2 * (DN + DV + q_rope.shape[1]),
            bytes_accessed=4 * heads * length * length,
            transcendentals=0,
        ),
        name="attend_backward",
    )(probs, grad, q_nope, q_rope, keys_values, k_rope)


def full_rows(piece_rows):
    return lax.all_gather(piece_rows, "mp", axis=1, tiled=True)


def mp_share(partial_value):
    return lax.psum_scatter(
        partial_value.astype(jnp.bfloat16), "mp", scatter_dimension=1, tiled=True
    ).astype(jnp.float32)


def ring_order(dp_count):
    chips = dp_count // 2
    return list(range(chips // 2)) + list(range(chips - 1, chips // 2 - 1, -1))


def ring_neighbours(dp_count):
    order = ring_order(dp_count)
    chips = len(order)
    place = lax.axis_index("dp")
    chip, core = place // 2, place % 2
    pos = jnp.where(chip < chips // 2, chip, chips // 2 + chips - 1 - chip)

    def device_at(p):
        p = lax.rem(p + 2 * chips, chips)
        c = jnp.where(p < chips // 2, p, chips // 2 + chips - 1 - p)
        return 2 * c + core

    return place, pos, core, device_at


def gather_kernel(dp_count, mp_count, axes, has_rows, *refs):
    count = len(axes)
    if not has_rows:
        refs = (None, *refs[:count], None, *refs[count:])
    rows_ref, parts = refs[0], refs[1 : 1 + count]
    rows_out, wholes = refs[1 + count], refs[2 + count : 2 + 2 * count]
    send, receive, local, line_send, line_receive, line_local = refs[2 + 2 * count :]
    chips = dp_count // 2
    reach = chips // 2
    place, pos, core, device_at = ring_neighbours(dp_count)
    line = lax.axis_index("mp")
    on, back = device_at(pos + 1), device_at(pos - 1)
    other = place + 1 - 2 * core

    barrier = pltpu.get_barrier_semaphore()
    for target in (on, back, other):
        pl.semaphore_signal(barrier, device_id={"dp": target}, device_id_type=MESH)

    waits = 3
    if has_rows:

        @pl.when(line > 0)
        def _():
            pl.semaphore_signal(barrier, device_id={"mp": line - 1}, device_id_type=MESH)

        @pl.when(line < mp_count - 1)
        def _():
            pl.semaphore_signal(barrier, device_id={"mp": line + 1}, device_id_type=MESH)

        waits = 3 + (line > 0).astype(jnp.int32) + (line < mp_count - 1).astype(jnp.int32)
    pl.semaphore_wait(barrier, waits)

    width = rows_ref.shape[1] if has_rows else 0

    def columns(owner):
        return rows_out.at[:, pl.ds(pl.multiple_of(owner * width, width), width)]

    def line_copy(way, hop, source, owner):
        target = line + 1 if way == 0 else line - 1
        return pltpu.make_async_remote_copy(
            source,
            columns(owner),
            line_send.at[way, hop],
            line_receive.at[way, hop],
            device_id={"mp": target},
            device_id_type=MESH,
        )

    ends = (line < mp_count - 1, line > 0)

    def holds(way, hop):
        return line >= hop if way == 0 else line + hop <= mp_count - 1

    def owner_of(way, hop):
        return jnp.clip(line - hop if way == 0 else line + hop, 0, mp_count - 1)

    if has_rows:
        for way in range(2):

            @pl.when(ends[way])
            def _(way=way):
                line_copy(way, 0, rows_ref, line).start()

        keep_rows = pltpu.make_async_copy(rows_ref, columns(line), line_local)
        keep_rows.start()

    def block(i, owner, low, high):
        size = parts[i].shape[axes[i]]
        start = pl.multiple_of(owner * size, size)
        if axes[i] == 1:
            return wholes[i].at[pl.ds(low, high - low), pl.ds(start, size)]
        return wholes[i].at[pl.ds(start + low, high - low), :]

    def split(i, piece):
        rows = parts[i].shape[0]
        middle = rows // 32 * 16
        return ((0, rows), (0, middle), (middle, rows))[piece]

    def ring_copy(i, slot, source, owner, piece, target):
        low, high = split(i, piece)
        if source is None:
            source = block(i, owner, low, high)
        return pltpu.make_async_remote_copy(
            source,
            block(i, owner, low, high),
            send.at[i, slot],
            receive.at[i, slot],
            device_id={"dp": target},
            device_id_type=MESH,
        )

    def empty(i, piece):
        low, high = split(i, piece)
        return low == high

    started, kept = [], []
    for i in range(count):
        for way, target in ((0, on), (1, back)):
            piece = 0 if reach > 1 else 1 + way
            if not empty(i, piece):
                low, high = split(i, piece)
                copy = ring_copy(
                    i, way * reach, parts[i].at[pl.ds(low, high - low), :], place, piece, target
                )
                copy.start()
                started.append(copy)
        copy = ring_copy(i, 2 * reach, parts[i], place, 0, other)
        copy.start()
        started.append(copy)
        copy = pltpu.make_async_copy(
            parts[i], block(i, place, 0, parts[i].shape[0]), local.at[i]
        )
        copy.start()
        kept.append(copy)

    def line_step(hop):
        for way in range(2):

            @pl.when(holds(way, hop))
            def _(way=way):
                line_copy(way, hop - 1, rows_ref, owner_of(way, hop)).wait_recv()

            if hop < mp_count - 1:

                @pl.when(holds(way, hop) & ends[way])
                def _(way=way):
                    owner = owner_of(way, hop)
                    line_copy(way, hop, columns(owner), owner).start()

    def ring_step(i, hop):
        for way, target in ((0, on), (1, back)):
            piece = 0 if hop < reach else 1 + way
            if empty(i, piece):
                continue
            owner = device_at(pos - hop if way == 0 else pos + hop)
            ring_copy(i, way * reach + hop - 1, None, owner, piece, other).wait_recv()
            if hop < reach:
                ahead = 0 if hop + 1 < reach else 1 + way
                if not empty(i, ahead):
                    copy = ring_copy(i, way * reach + hop, None, owner, ahead, target)
                    copy.start()
                    started.append(copy)
            copy = ring_copy(i, 2 * reach + 1 + way * reach + hop - 1, None, owner, piece, other)
            copy.start()
            started.append(copy)

    line_hops = list(range(1, mp_count)) if has_rows else []
    for hop in range(1, reach + 1):
        for i in range(count):
            ring_step(i, hop)
        if line_hops:
            line_step(line_hops.pop(0))
    for hop in line_hops:
        line_step(hop)

    for i in range(count):
        twin = place + 1 - 2 * core
        ring_copy(i, 2 * reach, parts[i], twin, 0, other).wait_recv()
        for hop in range(1, reach + 1):
            for way in range(2):
                piece = 0 if hop < reach else 1 + way
                if empty(i, piece):
                    continue
                owner = device_at(pos - hop if way == 0 else pos + hop) + 1 - 2 * core
                ring_copy(
                    i, 2 * reach + 1 + way * reach + hop - 1, None, owner, piece, other
                ).wait_recv()
    for copy in started:
        copy.wait_send()
    for copy in kept:
        copy.wait()
    if not has_rows:
        return
    for way in range(2):

        @pl.when(ends[way])
        def _(way=way):
            line_copy(way, 0, rows_ref, line).wait_send()

        for hop in range(1, mp_count - 1):

            @pl.when(holds(way, hop) & ends[way])
            def _(way=way, hop=hop):
                owner = owner_of(way, hop)
                line_copy(way, hop, columns(owner), owner).wait_send()

    keep_rows.wait()


def gather_all(rows, parts, axes, collective_id):
    dp_count, mp_count = lax.axis_size("dp"), lax.axis_size("mp")
    arrays = [part for part in (rows, *parts) if part is not None]
    shapes = [
        jax.ShapeDtypeStruct(
            tuple(s * dp_count if a == axis else s for a, s in enumerate(part.shape)), part.dtype
        )
        for part, axis in zip(parts, axes)
    ]
    semaphores = [
        pltpu.SemaphoreType.DMA((len(parts), 4 * (dp_count // 4) + 1)),
        pltpu.SemaphoreType.DMA((len(parts), 4 * (dp_count // 4) + 1)),
        pltpu.SemaphoreType.DMA((len(parts),)),
        pltpu.SemaphoreType.DMA((2, mp_count)),
        pltpu.SemaphoreType.DMA((2, mp_count)),
        pltpu.SemaphoreType.DMA,
    ]
    if rows is not None:
        shapes.insert(
            0, jax.ShapeDtypeStruct((rows.shape[0], rows.shape[1] * mp_count), rows.dtype)
        )
    moved = 2 * sum(shape.size for shape in shapes)
    return pl.pallas_call(
        functools.partial(gather_kernel, dp_count, mp_count, tuple(axes), rows is not None),
        out_shape=shapes,
        in_specs=[pl.BlockSpec(memory_space=pltpu.VMEM)] * len(arrays),
        out_specs=[pl.BlockSpec(memory_space=pl.ANY)] * len(arrays),
        scratch_shapes=semaphores,
        compiler_params=pltpu.CompilerParams(collective_id=collective_id, has_side_effects=True),
        cost_estimate=pl.CostEstimate(flops=0, bytes_accessed=16 * moved, transcendentals=0),
        name="gather_all",
    )(*arrays)


def small_total_kernel(dp_count, mp_count, value_ref, total_ref, ring, line, part, send, receive, line_send, line_receive):
    place, spot = lax.axis_index("dp"), lax.axis_index("mp")
    barrier = pltpu.get_barrier_semaphore()
    ring_targets = [lax.rem(place + shift, dp_count) for shift in range(1, dp_count)]
    line_targets = [lax.rem(spot + shift, mp_count) for shift in range(1, mp_count)]
    for target in ring_targets:
        pl.semaphore_signal(barrier, device_id={"dp": target}, device_id_type=MESH)
    for target in line_targets:
        pl.semaphore_signal(barrier, device_id={"mp": target}, device_id_type=MESH)
    pl.semaphore_wait(barrier, dp_count + mp_count - 2)
    copies = []
    for shift, target in enumerate(ring_targets):
        copies.append(
            pltpu.make_async_remote_copy(
                value_ref,
                ring.at[place],
                send.at[shift],
                receive.at[shift],
                device_id={"dp": target},
                device_id_type=MESH,
            )
        )
    for copy in copies:
        copy.start()
    ring[place] = value_ref[...]
    for copy in copies:
        copy.wait()
    total = ring[0]
    for d in range(1, dp_count):
        total = total + ring[d]
    part[...] = total
    copies = []
    for shift, target in enumerate(line_targets):
        copies.append(
            pltpu.make_async_remote_copy(
                part,
                line.at[spot],
                line_send.at[shift],
                line_receive.at[shift],
                device_id={"mp": target},
                device_id_type=MESH,
            )
        )
    for copy in copies:
        copy.start()
    line[spot] = total
    for copy in copies:
        copy.wait()
    total = line[0]
    for m in range(1, mp_count):
        total = total + line[m]
    total_ref[...] = total


def small_total(value, collective_id):
    dp_count, mp_count = lax.axis_size("dp"), lax.axis_size("mp")
    return pl.pallas_call(
        functools.partial(small_total_kernel, dp_count, mp_count),
        out_shape=jax.ShapeDtypeStruct(value.shape, value.dtype),
        in_specs=[pl.BlockSpec(memory_space=pltpu.VMEM)],
        out_specs=pl.BlockSpec(memory_space=pltpu.VMEM),
        scratch_shapes=[
            pltpu.VMEM((dp_count, *value.shape), value.dtype),
            pltpu.VMEM((mp_count, *value.shape), value.dtype),
            pltpu.VMEM(value.shape, value.dtype),
            pltpu.SemaphoreType.DMA((dp_count - 1,)),
            pltpu.SemaphoreType.DMA((dp_count - 1,)),
            pltpu.SemaphoreType.DMA((mp_count - 1,)),
            pltpu.SemaphoreType.DMA((mp_count - 1,)),
        ],
        compiler_params=pltpu.CompilerParams(collective_id=collective_id, has_side_effects=True),
        cost_estimate=pl.CostEstimate(flops=0, bytes_accessed=1 << 22, transcendentals=0),
        name="small_total",
    )(value)


def ring_move(values, step):
    order = ring_order(lax.axis_size("dp"))
    chips = len(order)
    pairs = [
        (2 * chip + core, 2 * order[(pos + step) % chips] + core)
        for pos, chip in enumerate(order)
        for core in range(2)
    ]
    return lax.ppermute(values, "dp", pairs)


def core_swap(values):
    return lax.ppermute(values, "dp", [(i, i ^ 1) for i in range(lax.axis_size("dp"))])


def direct_move(values, step, swap):
    order = ring_order(lax.axis_size("dp"))
    chips = len(order)
    pairs = [
        (2 * chip + core, 2 * order[(pos + step) % chips] + (core ^ swap))
        for pos, chip in enumerate(order)
        for core in range(2)
    ]
    return lax.ppermute(values, "dp", pairs)


def spread_pairs(own):
    chips = lax.axis_size("dp") // 2
    half = own.shape[0] // 32 * 16
    same = [None] * chips
    same[0] = ahead = behind = own
    for step in range(1, chips // 2):
        ahead = same[step] = ring_move(ahead, 1)
        behind = same[chips - step] = ring_move(behind, -1)
    same[chips // 2] = jnp.concatenate(
        [ring_move(ahead[:half], 1), ring_move(behind[half:], -1)], axis=0
    )
    return [(rows, core_swap(rows)) for rows in same]


def spread(own):
    return [jnp.concatenate(pair, axis=0) for pair in spread_pairs(own)]


def add_bf(left, right):
    return (left.astype(jnp.float32) + right.astype(jnp.float32)).astype(jnp.bfloat16)


def collect(pairs):
    chips = len(pairs)
    half = pairs[0][0].shape[0] // 2
    merged = [add_bf(same, core_swap(other)) for same, other in pairs]
    far = merged[chips // 2]
    carry_back, carry_on = ring_move(far[:half], -1), ring_move(far[half:], 1)
    for step in range(chips // 2 - 1, 0, -1):
        back, on = merged[step], merged[chips - step]
        if step == chips // 2 - 1:
            back = jnp.concatenate([add_bf(back[:half], carry_back), back[half:]], axis=0)
            on = jnp.concatenate([on[:half], add_bf(on[half:], carry_on)], axis=0)
        else:
            back, on = add_bf(back, carry_back), add_bf(on, carry_on)
        carry_back, carry_on = ring_move(back, -1), ring_move(on, 1)
    total = merged[0].astype(jnp.float32) + carry_back.astype(jnp.float32)
    return total + carry_on.astype(jnp.float32)


def relative_devices():
    dp_count = lax.axis_size("dp")
    _, pos, core, device_at = ring_neighbours(dp_count)
    places = []
    for k in range(dp_count // 2):
        same = device_at(pos - k)
        places.append((same, same + 1 - 2 * core))
    return places


def to_relative(values, places):
    width = values.shape[1] // lax.axis_size("dp")
    return jnp.concatenate(
        [
            lax.dynamic_slice_in_dim(values, place * width, width, axis=1)
            for pair in places
            for place in pair
        ],
        axis=1,
    )


def from_relative(values):
    dp_count = lax.axis_size("dp")
    width = values.shape[1] // dp_count
    order = ring_order(dp_count)
    chips = len(order)
    _, pos, core, _ = ring_neighbours(dp_count)
    blocks = []
    for place in range(dp_count):
        back = lax.rem(pos - order.index(place // 2) + chips, chips)
        slot = 2 * back + jnp.where(core == place % 2, 0, 1)
        blocks.append(lax.dynamic_slice_in_dim(values, slot * width, width, axis=1))
    return jnp.concatenate(blocks, axis=1)


def weight_grads(rows, cotangents):
    dp_count = lax.axis_size("dp")
    width = rows.shape[1] // dp_count
    blocks = [
        jnp.dot(
            rows[:, slot * width : (slot + 1) * width].T,
            cotangents,
            preferred_element_type=jnp.float32,
        ).astype(jnp.bfloat16)
        for slot in range(dp_count)
    ]
    return collect(list(zip(blocks[::2], blocks[1::2])))


def line_total(partial_value):
    count = lax.axis_size("mp")
    total = partial_value
    for shift in range(1, count):
        total = total + lax.ppermute(
            partial_value, "mp", [(i, (i + shift) % count) for i in range(count)]
        )
    return total


def shards(
    block_input,
    segment_ids,
    expert_ids,
    norm_gain,
    query_weight,
    latent_down,
    latent_gain,
    latent_up,
    output_weight,
    moe_gain,
    router_weight,
    shared_gate,
    shared_up,
    shared_down,
    expert_gate,
    expert_up,
    expert_down,
    output_grad,
):
    model_width = norm_gain.shape[0]
    tokens_here = block_input.shape[0]
    share_width = block_input.shape[1]
    mp_count = lax.axis_size("mp")
    mp_place = lax.axis_index("mp")
    dp_count = lax.axis_size("dp")
    heads_here = H // mp_count
    experts_all = router_weight.shape[0]
    experts_group = experts_all // dp_count
    chips = dp_count // 2
    own_expert = lax.axis_index("dp") * experts_group + mp_place // 2
    expert_places = jnp.arange(experts_all, dtype=jnp.int32)
    picked_mask = jnp.max(
        (expert_ids[..., None] == expert_places).astype(jnp.float32), axis=1
    )
    own_gate = expert_gate[0]
    own_up = expert_up[0]
    own_down = expert_down[0]
    cosine, sine_tab = rope_tables(LEN, DR)
    inputs = block_input.astype(jnp.float32)
    gain_one = lax.dynamic_slice_in_dim(norm_gain, mp_place * share_width, share_width)
    per_head = query_weight.reshape(heads_here, DN + DR, -1)
    query_rows = jnp.concatenate(
        [
            per_head[:, :DN].reshape(heads_here * DN, -1),
            per_head[:, DN : DN + DR // 2].reshape(heads_here * DR // 2, -1),
            per_head[:, DN + DR // 2 :].reshape(heads_here * DR // 2, -1),
        ],
        axis=0,
    )
    gathered = gather_all(
        block_input,
        (query_rows, latent_down, latent_up.T, output_weight, router_weight),
        (1, 1, 0, 1, 1),
        1,
    )
    inputs_full = gathered[0].astype(jnp.float32)
    query_w, down_w, up_wt, out_w, router_w = gathered[1:]
    scale_one = lax.rsqrt(jnp.mean(inputs_full * inputs_full, axis=1, keepdims=True) + epsilon)
    normed = (inputs_full * scale_one * norm_gain).astype(jnp.bfloat16)
    places = relative_devices()
    mask_chunks = spread(picked_mask)
    shared_parts, _ = lax.optimization_barrier(
        (jnp.concatenate([shared_gate, shared_up, shared_down], axis=0), gathered[0])
    )
    shared_pieces = [piece for pair in spread_pairs(shared_parts) for piece in pair]
    hidden_here = shared_gate.shape[0]
    sgate_w, sup_w, sdown_w = (
        jnp.concatenate(
            [piece[i * hidden_here : (i + 1) * hidden_here] for piece in shared_pieces], axis=1
        )
        for i in range(3)
    )
    nope_width, rope_width = heads_here * DN, heads_here * DR
    query_all = jnp.dot(normed, query_w.T, preferred_element_type=jnp.float32)
    cosines, sines = jnp.tile(cosine, (1, heads_here)), jnp.tile(sine_tab, (1, heads_here))
    query_nope = query_all[:, :nope_width].astype(jnp.bfloat16)
    query_rope = rotate(query_all[:, nope_width:], cosines, sines).astype(jnp.bfloat16)
    score_scale = (DN + DR) ** (-0.5)
    latent = full_rows(
        jnp.dot(normed, down_w.T, preferred_element_type=jnp.float32).astype(jnp.bfloat16)
    ).astype(jnp.float32)
    late_grad, _ = lax.optimization_barrier((output_grad, latent))
    grad_full = full_rows(late_grad)
    grad_chunks = spread(grad_full)
    latent_main = latent[:, :KVL]
    scale_lat = lax.rsqrt(jnp.mean(latent_main * latent_main, axis=-1, keepdims=True) + epsilon)
    latent_normed = (latent_main * scale_lat * latent_gain).astype(jnp.bfloat16)
    key_rope = rotate(latent[:, KVL:], cosine, sine_tab).astype(jnp.bfloat16)
    key_rope = jnp.concatenate(
        [key_rope[:, : DR // 2]] * heads_here + [key_rope[:, DR // 2 :]] * heads_here, axis=1
    )
    keys_values = jnp.dot(latent_normed, up_wt, preferred_element_type=jnp.float32).astype(
        jnp.bfloat16
    )
    attended_flat, probs = attend_forward(
        query_nope, query_rope, keys_values, key_rope, segment_ids, heads_here, score_scale
    )
    attended_part = jnp.dot(attended_flat, out_w, preferred_element_type=jnp.float32).astype(
        jnp.bfloat16
    )
    attended_sum = mp_share(attended_part)
    residual = inputs + attended_sum
    gain_two = lax.dynamic_slice_in_dim(moe_gain, mp_place * share_width, share_width)
    residual_full = full_rows(residual.astype(jnp.bfloat16)).astype(jnp.float32)
    scale_two = lax.rsqrt(
        jnp.mean(residual_full * residual_full, axis=1, keepdims=True) + epsilon
    )
    moe_in = (residual_full * scale_two * moe_gain).astype(jnp.bfloat16)
    row_chunks = spread(moe_in)
    moe_rel, grad_rel = to_relative(moe_in, places), to_relative(grad_full, places)
    router_logits = jnp.dot(moe_in, router_w.T, preferred_element_type=jnp.float32)

    def masked_gates(logits, mask):
        pick_exp = jnp.exp(jnp.where(mask > 0, logits, negative))
        return pick_exp / jnp.sum(pick_exp, axis=-1, keepdims=True)

    gate_prob = masked_gates(router_logits, picked_mask)
    shared_g = jnp.dot(moe_rel, sgate_w.T, preferred_element_type=jnp.float32)
    shared_u = jnp.dot(moe_rel, sup_w.T, preferred_element_type=jnp.float32)
    shared_act = (jax.nn.silu(shared_g) * shared_u).astype(jnp.bfloat16)
    shared_part = from_relative(
        jnp.dot(shared_act, sdown_w, preferred_element_type=jnp.float32)
    )
    up_router = jnp.concatenate([own_up, router_w], axis=0)
    hidden = own_up.shape[0]
    own_column = (expert_places == own_expert).astype(jnp.float32)
    act_all, gate_pre_all, up_pre_all, out_chunks, back_chunks, gate_grads = [], [], [], [], [], []
    for rows_k, grads_k, mask_k in zip(row_chunks, grad_chunks, mask_chunks):
        pre_gate = jnp.dot(rows_k, own_gate.T, preferred_element_type=jnp.float32)
        up_logits = jnp.dot(rows_k, up_router.T, preferred_element_type=jnp.float32)
        pre_up = up_logits[:, :hidden]
        gate_k = jnp.sum(
            masked_gates(up_logits[:, hidden:], mask_k) * own_column, axis=1, keepdims=True
        )
        act_grad = jnp.dot(grads_k, own_down.T, preferred_element_type=jnp.float32)
        activation = jax.nn.silu(pre_gate) * pre_up
        gate_grads.append(jnp.sum(activation * act_grad, axis=1))
        act_grad = act_grad * gate_k
        act_bf = (activation * gate_k).astype(jnp.bfloat16)
        gate_pre = (act_grad * pre_up * silu_grad(pre_gate)).astype(jnp.bfloat16)
        up_pre = (act_grad * jax.nn.silu(pre_gate)).astype(jnp.bfloat16)
        back_chunks.append(
            tuple(
                (
                    jnp.dot(gate_pre[part], own_gate, preferred_element_type=jnp.float32)
                    + jnp.dot(up_pre[part], own_up, preferred_element_type=jnp.float32)
                ).astype(jnp.bfloat16)
                for part in (slice(None, tokens_here), slice(tokens_here, None))
            )
        )
        act_all.append(act_bf)
        gate_pre_all.append(gate_pre)
        up_pre_all.append(up_pre)
    routed_back = collect(back_chunks)
    act_late, _ = lax.optimization_barrier((act_all, routed_back))
    act_all, gate_pre_all, up_pre_all, _ = lax.optimization_barrier(
        (act_all, gate_pre_all, up_pre_all, back_chunks)
    )
    for act_bf in act_late:
        out_chunks.append(
            tuple(
                jnp.dot(act_bf[part], own_down, preferred_element_type=jnp.float32).astype(
                    jnp.bfloat16
                )
                for part in (slice(None, tokens_here), slice(tokens_here, None))
            )
        )
    rows_all, grads_all = jnp.concatenate(row_chunks), jnp.concatenate(grad_chunks)
    expert_down_grad = jnp.dot(
        jnp.concatenate(act_all).T, grads_all, preferred_element_type=jnp.float32
    )[None]
    expert_gate_grad = jnp.dot(
        jnp.concatenate(gate_pre_all).T, rows_all, preferred_element_type=jnp.float32
    )[None]
    expert_up_grad = jnp.dot(
        jnp.concatenate(up_pre_all).T, rows_all, preferred_element_type=jnp.float32
    )[None]
    order = jnp.array(ring_order(dp_count), jnp.int32)
    dp_place = lax.axis_index("dp")
    ring_place = jnp.argmax((order == dp_place // 2).astype(jnp.int32)).astype(jnp.int32)
    gate_grad = jnp.zeros((tokens_here, experts_all), jnp.float32)
    for k, both in enumerate(gate_grads):
        chip_from = jnp.sum(
            jnp.where(jnp.arange(chips) == (ring_place + k) % chips, order, 0)
        )
        for swap in range(2):
            piece = both[swap * tokens_here : (swap + 1) * tokens_here]
            if k or swap:
                piece = direct_move(piece, -k, swap)
            device_from = 2 * chip_from + (dp_place % 2 if swap == 0 else 1 - dp_place % 2)
            expert_from = device_from * experts_group + mp_place // 2
            gate_grad = gate_grad + piece[:, None] * (expert_places == expert_from).astype(
                jnp.float32
            )
    gate_grad = line_total(gate_grad)
    routed_part = collect(out_chunks)
    moe_total = mp_share(shared_part + routed_part)
    block_output = (residual + moe_total).astype(jnp.bfloat16)
    logit_grad = (
        gate_prob * (gate_grad - jnp.sum(gate_prob * gate_grad, axis=-1, keepdims=True))
    ).astype(jnp.bfloat16)
    router_back = jnp.dot(logit_grad, router_w, preferred_element_type=jnp.float32)
    shared_act_grad = jnp.dot(grad_rel, sdown_w.T, preferred_element_type=jnp.float32)
    shared_gate_pre = (shared_act_grad * shared_u * silu_grad(shared_g)).astype(jnp.bfloat16)
    shared_up_pre = (shared_act_grad * jax.nn.silu(shared_g)).astype(jnp.bfloat16)
    moe_late, grad_late, shared_late, _ = lax.optimization_barrier(
        (
            moe_rel,
            grad_rel,
            (shared_act, shared_gate_pre, shared_up_pre, logit_grad),
            routed_back,
        )
    )
    sdown_grad = weight_grads(grad_late, shared_late[0])
    moe_rows_grad = weight_grads(moe_late, jnp.concatenate(shared_late[1:], axis=1))
    shared_back = from_relative(
        jnp.dot(shared_gate_pre, sgate_w, preferred_element_type=jnp.float32)
        + jnp.dot(shared_up_pre, sup_w, preferred_element_type=jnp.float32)
    )
    router_mine = lax.dynamic_slice_in_dim(router_back, mp_place * share_width, share_width, axis=1)
    moe_in_grad = mp_share(shared_back + routed_back) + router_mine
    back_full = full_rows(moe_in_grad.astype(jnp.bfloat16)).astype(jnp.float32)
    moe_gain_part = jnp.sum(back_full * residual_full * scale_two, axis=0)
    stat_two = jnp.mean(back_full * residual_full * moe_gain, axis=1, keepdims=True)
    residual_grad = (
        output_grad.astype(jnp.float32)
        + scale_two * gain_two * moe_in_grad
        - residual * scale_two**3 * stat_two
    )
    residual_bf = (
        grad_full.astype(jnp.float32)
        + scale_two * moe_gain * back_full
        - residual_full * scale_two**3 * stat_two
    ).astype(jnp.bfloat16)
    out_w_grad = weight_grads(to_relative(residual_bf, places), attended_flat)
    attended_grad = jnp.dot(residual_bf, out_w.T, preferred_element_type=jnp.float32).astype(
        jnp.bfloat16
    )
    dq_nope, dq_rope, kv_grad, dk_ropes = attend_backward(
        probs,
        attended_grad,
        query_nope,
        query_rope,
        keys_values,
        key_rope,
        heads_here,
        score_scale,
    )
    query_grad = jnp.concatenate(
        [dq_nope, unrotate(dq_rope, cosines, sines).astype(jnp.bfloat16)], axis=1
    )
    dk_rope = jnp.sum(dk_ropes.reshape(-1, 2, heads_here, DR // 2), axis=2).reshape(-1, DR)
    up_w_grad = weight_grads(to_relative(latent_normed, places), kv_grad)
    normed_lat_grad = jnp.dot(kv_grad, up_wt.T, preferred_element_type=jnp.float32)
    latent_gain_part = jnp.sum(normed_lat_grad * latent_main * scale_lat, axis=0)
    main_grad = scale_lat * latent_gain * normed_lat_grad - latent_main * scale_lat**3 * jnp.mean(
        normed_lat_grad * latent_main * latent_gain, axis=-1, keepdims=True
    )
    rope_grad = unrotate(dk_rope, cosine, sine_tab)
    latent_grad = mp_share(jnp.concatenate([main_grad, rope_grad], axis=-1)).astype(jnp.bfloat16)
    query_rows_grad = weight_grads(
        to_relative(normed, places), jnp.concatenate([query_grad, latent_grad], axis=1)
    )
    normed_part = jnp.dot(query_grad, query_w, preferred_element_type=jnp.float32) + jnp.dot(
        latent_grad, down_w, preferred_element_type=jnp.float32
    )
    weighted_part = normed_part * inputs_full
    norm_gain_part = jnp.sum(weighted_part * scale_one, axis=0)
    stat_one = line_total(jnp.sum(weighted_part * norm_gain, axis=1))[:, None] / model_width
    moe_gain_part = jnp.where(mp_place == 0, moe_gain_part, 0.0)
    gain_total = small_total(
        jnp.concatenate([norm_gain_part, moe_gain_part, latent_gain_part]).reshape(-1, 128), 2
    ).reshape(-1)
    norm_gain_grad = gain_total[:model_width]
    moe_gain_grad = gain_total[model_width : 2 * model_width]
    latent_gain_grad = gain_total[2 * model_width :]
    normed_grad = mp_share(normed_part)
    input_grad = (
        residual_grad + scale_one * gain_one * normed_grad - inputs * scale_one**3 * stat_one
    )
    query_width = query_grad.shape[1]
    query_rows_grad, down_rows_grad = (
        query_rows_grad[:, :query_width].T,
        query_rows_grad[:, query_width:].T,
    )
    parts = [query_rows_grad[:nope_width].reshape(heads_here, DN, -1)]
    for half in range(2):
        low = nope_width + half * rope_width // 2
        parts.append(
            query_rows_grad[low : low + rope_width // 2].reshape(heads_here, DR // 2, -1)
        )
    query_weight_grad = jnp.concatenate(parts, axis=1).reshape(query_width, -1)
    latent_down_grad = down_rows_grad
    latent_up_grad = up_w_grad.T
    output_weight_grad = out_w_grad.T
    shared_gate_grad = moe_rows_grad[:, :hidden_here].T
    shared_up_grad = moe_rows_grad[:, hidden_here : 2 * hidden_here].T
    router_grad = moe_rows_grad[:, 2 * hidden_here :].T
    shared_down_grad = sdown_grad.T
    return (
        block_output,
        input_grad,
        norm_gain_grad,
        query_weight_grad,
        latent_down_grad,
        latent_gain_grad,
        latent_up_grad,
        output_weight_grad,
        moe_gain_grad,
        router_grad,
        shared_gate_grad,
        shared_up_grad,
        shared_down_grad,
        expert_gate_grad,
        expert_up_grad,
        expert_down_grad,
    )


def solution(mesh):
    in_specs = (
        P("dp", "mp"),
        P("dp", None),
        P("dp", None),
        P(),
        P("mp", "dp"),
        P("mp", "dp"),
        P(),
        P("mp", "dp"),
        P("mp", "dp"),
        P(),
        P(None, "dp"),
        P("mp", "dp"),
        P("mp", "dp"),
        P("mp", "dp"),
        P(("dp", "mp"), None, None),
        P(("dp", "mp"), None, None),
        P(("dp", "mp"), None, None),
        P("dp", "mp"),
    )
    out_specs = (
        P("dp", "mp"),
        P("dp", "mp"),
        P(),
        P("mp", "dp"),
        P("mp", "dp"),
        P(),
        P("mp", "dp"),
        P("mp", "dp"),
        P(),
        P(None, "dp"),
        P("mp", "dp"),
        P("mp", "dp"),
        P("mp", "dp"),
        P(("dp", "mp"), None, None),
        P(("dp", "mp"), None, None),
        P(("dp", "mp"), None, None),
    )
    return jax.shard_map(shards, mesh=mesh, in_specs=in_specs, out_specs=out_specs, check_vma=False)
```

```python
import functools

import jax
import jax.numpy as jnp
from jax import lax
from jax.experimental import pallas as pl
from jax.experimental.pallas import tpu as pltpu
from jax.sharding import PartitionSpec as P

MESH = pl.DeviceIdType.MESH

H = 16
DN = 128
DR = 64
DV = 128
KVL = 512
LEN = 512


epsilon = 1e-06
negative = -1e30


def rope_tables(length, rot_width):
    half_width = rot_width // 2
    frequency = 10000.0 ** (-(2.0 / rot_width) * jnp.arange(half_width, dtype=jnp.float32))
    angles = jnp.arange(length, dtype=jnp.float32)[:, None] * frequency[None, :]
    return (jnp.cos(angles), jnp.sin(angles))


def rotate(values, cosine, sine_tab):
    half_width = values.shape[-1] // 2
    leading = values[..., :half_width]
    trailing = values[..., half_width:]
    return jnp.concatenate(
        [leading * cosine - trailing * sine_tab, trailing * cosine + leading * sine_tab], axis=-1
    )


def unrotate(values, cosine, sine_tab):
    half_width = values.shape[-1] // 2
    leading = values[..., :half_width]
    trailing = values[..., half_width:]
    return jnp.concatenate(
        [leading * cosine + trailing * sine_tab, trailing * cosine - leading * sine_tab], axis=-1
    )


def silu_grad(preact):
    sigmoid_val = jax.nn.sigmoid(preact)
    return sigmoid_val * (1.0 + preact * (1.0 - sigmoid_val))


def head_lanes(shape, heads):
    lane = lax.broadcasted_iota(jnp.int32, shape, 1)
    per_head = shape[1] // (2 * heads)
    mine = lax.rem(lane, heads * per_head) // per_head == pl.program_id(0)
    return mine.astype(jnp.float32)


def attend_forward_kernel(
    heads, scale, q_ref, q_rope_ref, keys_ref, k_rope_ref, seg_row_ref, seg_col_ref, out_ref, probs_ref
):
    width = q_ref.shape[1]
    q_rope = (q_rope_ref[...].astype(jnp.float32) * head_lanes(q_rope_ref.shape, heads)).astype(
        jnp.bfloat16
    )
    nt = (((1,), (1,)), ((), ()))
    logits = lax.dot_general(
        q_ref[...], keys_ref[:, :width], nt, preferred_element_type=jnp.float32
    )
    logits = logits + lax.dot_general(
        q_rope, k_rope_ref[...], nt, preferred_element_type=jnp.float32
    )
    row = lax.broadcasted_iota(jnp.int32, logits.shape, 0)
    column = lax.broadcasted_iota(jnp.int32, logits.shape, 1)
    kept = (seg_col_ref[...] == seg_row_ref[...]) & (column <= row)
    weights = jnp.exp(jnp.where(kept, logits * scale, negative))
    probs = (weights / jnp.sum(weights, axis=1, keepdims=True)).astype(jnp.bfloat16)
    probs_ref[0] = probs
    out_ref[...] = jnp.dot(
        probs, keys_ref[:, width:], preferred_element_type=jnp.float32
    ).astype(jnp.bfloat16)


def attend_forward(q_nope, q_rope, keys_values, k_rope, seg_row, heads, scale):
    length = q_nope.shape[0]
    whole = lambda h: (0, 0)
    mine = lambda h: (0, h)
    return pl.pallas_call(
        functools.partial(attend_forward_kernel, heads, scale),
        grid=(heads,),
        out_shape=(
            jax.ShapeDtypeStruct((length, heads * DV), jnp.bfloat16),
            jax.ShapeDtypeStruct((heads, length, length), jnp.bfloat16),
        ),
        in_specs=[
            pl.BlockSpec((length, DN), mine),
            pl.BlockSpec(q_rope.shape, whole),
            pl.BlockSpec((length, DN + DV), mine),
            pl.BlockSpec(k_rope.shape, whole),
            pl.BlockSpec((1, length), whole),
            pl.BlockSpec((length, 1), whole),
        ],
        out_specs=(
            pl.BlockSpec((length, DV), mine),
            pl.BlockSpec((1, length, length), lambda h: (h, 0, 0)),
        ),
        cost_estimate=pl.CostEstimate(
            flops=2 * heads * length * length * (DN + DV + q_rope.shape[1]),
            bytes_accessed=4 * heads * length * length,
            transcendentals=heads * length * length,
        ),
        name="attend_forward",
    )(q_nope, q_rope, keys_values, k_rope, seg_row, seg_row.T)


def attend_backward_kernel(
    heads,
    scale,
    probs_ref,
    grad_ref,
    q_ref,
    q_rope_ref,
    keys_ref,
    k_rope_ref,
    dq_ref,
    dq_rope_ref,
    dkeys_ref,
    dk_rope_ref,
):
    width = q_ref.shape[1]
    lanes = head_lanes(q_rope_ref.shape, heads)
    q_rope = (q_rope_ref[...].astype(jnp.float32) * lanes).astype(jnp.bfloat16)
    probs, grad = probs_ref[0], grad_ref[...]
    prob_grad = lax.dot_general(
        grad, keys_ref[:, width:], (((1,), (1,)), ((), ())), preferred_element_type=jnp.float32
    )
    wide = probs.astype(jnp.float32)
    row_dot = jnp.sum(wide * prob_grad, axis=1, keepdims=True)
    score_grad = (wide * (prob_grad - row_dot) * scale).astype(jnp.bfloat16)
    tn = (((0,), (0,)), ((), ()))
    dq_ref[...] = jnp.dot(
        score_grad, keys_ref[:, :width], preferred_element_type=jnp.float32
    ).astype(jnp.bfloat16)
    dq_rope = lanes * jnp.dot(score_grad, k_rope_ref[...], preferred_element_type=jnp.float32)
    dk_rope = lax.dot_general(score_grad, q_rope, tn, preferred_element_type=jnp.float32)
    dkeys_ref[:, :width] = lax.dot_general(
        score_grad, q_ref[...], tn, preferred_element_type=jnp.float32
    ).astype(jnp.bfloat16)
    dkeys_ref[:, width:] = lax.dot_general(
        probs, grad, tn, preferred_element_type=jnp.float32
    ).astype(jnp.bfloat16)

    @pl.when(pl.program_id(0) == 0)
    def _():
        dq_rope_ref[...] = dq_rope
        dk_rope_ref[...] = dk_rope

    @pl.when(pl.program_id(0) > 0)
    def _():
        dq_rope_ref[...] += dq_rope
        dk_rope_ref[...] += dk_rope


def attend_backward(probs, grad, q_nope, q_rope, keys_values, k_rope, heads, scale):
    length = q_nope.shape[0]
    whole = lambda h: (0, 0)
    mine = lambda h: (0, h)
    return pl.pallas_call(
        functools.partial(attend_backward_kernel, heads, scale),
        grid=(heads,),
        out_shape=(
            jax.ShapeDtypeStruct(q_nope.shape, jnp.bfloat16),
            jax.ShapeDtypeStruct(q_rope.shape, jnp.float32),
            jax.ShapeDtypeStruct(keys_values.shape, jnp.bfloat16),
            jax.ShapeDtypeStruct(q_rope.shape, jnp.float32),
        ),
        in_specs=[
            pl.BlockSpec((1, length, length), lambda h: (h, 0, 0)),
            pl.BlockSpec((length, DV), mine),
            pl.BlockSpec((length, DN), mine),
            pl.BlockSpec(q_rope.shape, whole),
            pl.BlockSpec((length, DN + DV), mine),
            pl.BlockSpec(k_rope.shape, whole),
        ],
        out_specs=(
            pl.BlockSpec((length, DN), mine),
            pl.BlockSpec(q_rope.shape, whole),
            pl.BlockSpec((length, DN + DV), mine),
            pl.BlockSpec(q_rope.shape, whole),
        ),
        cost_estimate=pl.CostEstimate(
            flops=2 * heads * length * length * 2 * (DN + DV + q_rope.shape[1]),
            bytes_accessed=4 * heads * length * length,
            transcendentals=0,
        ),
        name="attend_backward",
    )(probs, grad, q_nope, q_rope, keys_values, k_rope)


def expert_kernel(held, *refs):
    xs, gs = refs[:4], refs[4:8]
    mask_ref, own_ref, *weights = refs[8:13]
    refs = refs[13 + held :]
    back_same, back_other, score_ref, act_ref, gate_pre_ref, up_pre_ref, x_all, g_all = refs[:8]
    pre_gate, pre_up, grads, gate_ref, up_ref, down_ref, arrived = refs[8:]
    hidden = gate_ref.shape[0]
    nt = (((1,), (1,)), ((), ()))
    tn = (((0,), (0,)), ((), ()))
    first = pl.program_id(0) == 0
    copies = [
        pltpu.make_async_copy(weight, kept, arrived.at[i])
        for i, (weight, kept) in enumerate(zip(weights, (gate_ref, up_ref, down_ref)))
    ]

    @pl.when(first)
    def _():
        for copy in copies:
            copy.start()

    half = xs[0].shape[0]
    for part in range(2):
        rows = slice(part * half, (part + 1) * half)
        x_all[rows, :] = jnp.where(first, xs[part][...], xs[part + 2][...])
        g_all[rows, :] = jnp.where(first, gs[part][...], gs[part + 2][...])

    def arrive(i):
        @pl.when(first)
        def _():
            copies[i].wait()

    arrive(0)
    pre_gate[...] = lax.dot_general(
        gate_ref[...], x_all[...], nt, preferred_element_type=jnp.float32
    )
    arrive(1)
    pre_up[...] = lax.dot_general(up_ref[...], x_all[...], nt, preferred_element_type=jnp.float32)
    arrive(2)
    grads[...] = lax.dot_general(
        down_ref[...], g_all[...], nt, preferred_element_type=jnp.float32
    )
    mask = mask_ref[...]
    pick_exp = jnp.exp(jnp.where(mask > 0, pre_up[hidden:, :], negative))
    share = jnp.sum(pick_exp * own_ref[...], axis=0, keepdims=True) / jnp.sum(
        pick_exp, axis=0, keepdims=True
    )
    step = 32 if hidden % 32 == 0 else 16

    def body(i, score):
        rows = pl.ds(pl.multiple_of(i * step, step), step)
        gate_in, up_in, grad = pre_gate[rows, :], pre_up[rows, :], grads[rows, :]
        sig = jax.nn.sigmoid(gate_in)
        silu = gate_in * sig
        activation = silu * up_in
        scaled = grad * share
        act_ref[rows, :] = (activation * share).astype(jnp.bfloat16)
        gate_pre_ref[rows, :] = (scaled * up_in * (sig * (1.0 + gate_in * (1.0 - sig)))).astype(
            jnp.bfloat16
        )
        up_pre_ref[rows, :] = (scaled * silu).astype(jnp.bfloat16)
        return score + jnp.sum(activation * grad, axis=0, keepdims=True)

    score_ref[...] = lax.fori_loop(
        0, hidden // step, body, jnp.zeros((1, x_all.shape[0]), jnp.float32)
    )
    width = 512
    for low in range(0, gate_ref.shape[1], width):
        columns = slice(low, low + width)
        back = lax.dot_general(
            gate_pre_ref[...], gate_ref[:, columns], tn, preferred_element_type=jnp.float32
        ) + lax.dot_general(
            up_pre_ref[...], up_ref[:hidden, columns], tn, preferred_element_type=jnp.float32
        )
        back = back.astype(jnp.bfloat16)

        @pl.when(first)
        def _(back=back, columns=columns):
            back_same[:, columns] = back

        @pl.when(jnp.logical_not(first))
        def _(back=back, columns=columns):
            back_other[:, columns] = back


def expert_rows(k, chips, rows, grads, mask, own, gate, up_router, down, held):
    half, width = rows[0].shape
    tokens = 2 * half
    hidden = gate.shape[0]
    whole = lambda shape: pl.BlockSpec(shape, lambda i: (0, 0), pipeline_mode=pl.Buffered(1))
    bf = jnp.bfloat16
    total = 2 * chips * tokens
    slab = pl.BlockSpec((hidden, tokens), lambda i: (0, 2 * k + i))
    lines = pl.BlockSpec((tokens, width), lambda i: (2 * k + i, 0))
    return pl.pallas_call(
        functools.partial(expert_kernel, len(held)),
        grid=(2,),
        out_shape=(
            jax.ShapeDtypeStruct((tokens, width), bf),
            jax.ShapeDtypeStruct((tokens, width), bf),
            jax.ShapeDtypeStruct((1, 2 * tokens), jnp.float32),
            jax.ShapeDtypeStruct((hidden, total), bf),
            jax.ShapeDtypeStruct((hidden, total), bf),
            jax.ShapeDtypeStruct((hidden, total), bf),
            jax.ShapeDtypeStruct((total, width), bf),
            jax.ShapeDtypeStruct((total, width), bf),
        ),
        in_specs=[
            *[whole((half, width))] * 8,
            pl.BlockSpec((mask.shape[0], tokens), lambda i: (0, i)),
            whole(own.shape),
            *[pl.BlockSpec(memory_space=pl.ANY)] * (3 + len(held)),
        ],
        out_specs=(
            whole((tokens, width)),
            whole((tokens, width)),
            pl.BlockSpec((1, tokens), lambda i: (0, i)),
            slab,
            slab,
            slab,
            lines,
            lines,
        ),
        scratch_shapes=[
            pltpu.VMEM((hidden, tokens), jnp.float32),
            pltpu.VMEM((up_router.shape[0], tokens), jnp.float32),
            pltpu.VMEM((hidden, tokens), jnp.float32),
            pltpu.VMEM(gate.shape, bf),
            pltpu.VMEM(up_router.shape, bf),
            pltpu.VMEM(down.shape, bf),
            pltpu.SemaphoreType.DMA((3,)),
        ],
        input_output_aliases={13 + i: 3 + i for i in range(len(held))},
        cost_estimate=pl.CostEstimate(
            flops=2 * 2 * tokens * hidden * width * 5,
            bytes_accessed=2 * (3 * hidden * width + 10 * tokens * width),
            transcendentals=2 * tokens * hidden,
        ),
        name="expert_rows",
    )(*rows, *grads, mask, own, gate, up_router, down, *held)


def full_rows(piece_rows):
    return lax.all_gather(piece_rows, "mp", axis=1, tiled=True)


def mp_share(partial_value):
    return lax.psum_scatter(
        partial_value.astype(jnp.bfloat16), "mp", scatter_dimension=1, tiled=True
    ).astype(jnp.float32)


def ring_order(dp_count):
    chips = dp_count // 2
    return list(range(chips // 2)) + list(range(chips - 1, chips // 2 - 1, -1))


def ring_neighbours(dp_count):
    order = ring_order(dp_count)
    chips = len(order)
    place = lax.axis_index("dp")
    chip, core = place // 2, place % 2
    pos = jnp.where(chip < chips // 2, chip, chips // 2 + chips - 1 - chip)

    def device_at(p):
        p = lax.rem(p + 2 * chips, chips)
        c = jnp.where(p < chips // 2, p, chips // 2 + chips - 1 - p)
        return 2 * c + core

    return place, pos, core, device_at


def gather_kernel(dp_count, mp_count, axes, has_rows, *refs):
    count = len(axes)
    if not has_rows:
        refs = (None, *refs[:count], None, *refs[count:])
    rows_ref, parts = refs[0], refs[1 : 1 + count]
    rows_out, wholes = refs[1 + count], refs[2 + count : 2 + 2 * count]
    send, receive, local, line_send, line_receive, line_local = refs[2 + 2 * count :]
    chips = dp_count // 2
    reach = chips // 2
    place, pos, core, device_at = ring_neighbours(dp_count)
    line = lax.axis_index("mp")
    on, back = device_at(pos + 1), device_at(pos - 1)
    other = place + 1 - 2 * core

    barrier = pltpu.get_barrier_semaphore()
    for target in (on, back, other):
        pl.semaphore_signal(barrier, device_id={"dp": target}, device_id_type=MESH)

    waits = 3
    if has_rows:

        @pl.when(line > 0)
        def _():
            pl.semaphore_signal(barrier, device_id={"mp": line - 1}, device_id_type=MESH)

        @pl.when(line < mp_count - 1)
        def _():
            pl.semaphore_signal(barrier, device_id={"mp": line + 1}, device_id_type=MESH)

        waits = 3 + (line > 0).astype(jnp.int32) + (line < mp_count - 1).astype(jnp.int32)
    pl.semaphore_wait(barrier, waits)

    width = rows_ref.shape[1] if has_rows else 0

    def columns(owner):
        return rows_out.at[:, pl.ds(pl.multiple_of(owner * width, width), width)]

    def line_copy(way, hop, source, owner):
        target = line + 1 if way == 0 else line - 1
        return pltpu.make_async_remote_copy(
            source,
            columns(owner),
            line_send.at[way, hop],
            line_receive.at[way, hop],
            device_id={"mp": target},
            device_id_type=MESH,
        )

    ends = (line < mp_count - 1, line > 0)

    def holds(way, hop):
        return line >= hop if way == 0 else line + hop <= mp_count - 1

    def owner_of(way, hop):
        return jnp.clip(line - hop if way == 0 else line + hop, 0, mp_count - 1)

    if has_rows:
        for way in range(2):

            @pl.when(ends[way])
            def _(way=way):
                line_copy(way, 0, rows_ref, line).start()

        keep_rows = pltpu.make_async_copy(rows_ref, columns(line), line_local)
        keep_rows.start()

    def block(i, owner, low, high):
        size = parts[i].shape[axes[i]]
        start = pl.multiple_of(owner * size, size)
        if axes[i] == 1:
            return wholes[i].at[pl.ds(low, high - low), pl.ds(start, size)]
        return wholes[i].at[pl.ds(start + low, high - low), :]

    def split(i, piece):
        rows = parts[i].shape[0]
        middle = rows // 32 * 16
        return ((0, rows), (0, middle), (middle, rows))[piece]

    def ring_copy(i, slot, source, owner, piece, target):
        low, high = split(i, piece)
        if source is None:
            source = block(i, owner, low, high)
        return pltpu.make_async_remote_copy(
            source,
            block(i, owner, low, high),
            send.at[i, slot],
            receive.at[i, slot],
            device_id={"dp": target},
            device_id_type=MESH,
        )

    def empty(i, piece):
        low, high = split(i, piece)
        return low == high

    started, kept = [], []
    for i in range(count):
        for way, target in ((0, on), (1, back)):
            piece = 0 if reach > 1 else 1 + way
            if not empty(i, piece):
                low, high = split(i, piece)
                copy = ring_copy(
                    i, way * reach, parts[i].at[pl.ds(low, high - low), :], place, piece, target
                )
                copy.start()
                started.append(copy)
        copy = ring_copy(i, 2 * reach, parts[i], place, 0, other)
        copy.start()
        started.append(copy)
        copy = pltpu.make_async_copy(
            parts[i], block(i, place, 0, parts[i].shape[0]), local.at[i]
        )
        copy.start()
        kept.append(copy)

    def line_step(hop):
        for way in range(2):

            @pl.when(holds(way, hop))
            def _(way=way):
                line_copy(way, hop - 1, rows_ref, owner_of(way, hop)).wait_recv()

            if hop < mp_count - 1:

                @pl.when(holds(way, hop) & ends[way])
                def _(way=way):
                    owner = owner_of(way, hop)
                    line_copy(way, hop, columns(owner), owner).start()

    def ring_step(i, hop):
        for way, target in ((0, on), (1, back)):
            piece = 0 if hop < reach else 1 + way
            if empty(i, piece):
                continue
            owner = device_at(pos - hop if way == 0 else pos + hop)
            ring_copy(i, way * reach + hop - 1, None, owner, piece, other).wait_recv()
            if hop < reach:
                ahead = 0 if hop + 1 < reach else 1 + way
                if not empty(i, ahead):
                    copy = ring_copy(i, way * reach + hop, None, owner, ahead, target)
                    copy.start()
                    started.append(copy)
            copy = ring_copy(i, 2 * reach + 1 + way * reach + hop - 1, None, owner, piece, other)
            copy.start()
            started.append(copy)

    line_hops = list(range(1, mp_count)) if has_rows else []
    for hop in range(1, reach + 1):
        for i in range(count):
            ring_step(i, hop)
        if line_hops:
            line_step(line_hops.pop(0))
    for hop in line_hops:
        line_step(hop)

    for i in range(count):
        twin = place + 1 - 2 * core
        ring_copy(i, 2 * reach, parts[i], twin, 0, other).wait_recv()
        for hop in range(1, reach + 1):
            for way in range(2):
                piece = 0 if hop < reach else 1 + way
                if empty(i, piece):
                    continue
                owner = device_at(pos - hop if way == 0 else pos + hop) + 1 - 2 * core
                ring_copy(
                    i, 2 * reach + 1 + way * reach + hop - 1, None, owner, piece, other
                ).wait_recv()
    for copy in started:
        copy.wait_send()
    for copy in kept:
        copy.wait()
    if not has_rows:
        return
    for way in range(2):

        @pl.when(ends[way])
        def _(way=way):
            line_copy(way, 0, rows_ref, line).wait_send()

        for hop in range(1, mp_count - 1):

            @pl.when(holds(way, hop) & ends[way])
            def _(way=way, hop=hop):
                owner = owner_of(way, hop)
                line_copy(way, hop, columns(owner), owner).wait_send()

    keep_rows.wait()


def gather_all(rows, parts, axes, collective_id):
    dp_count, mp_count = lax.axis_size("dp"), lax.axis_size("mp")
    arrays = [part for part in (rows, *parts) if part is not None]
    shapes = [
        jax.ShapeDtypeStruct(
            tuple(s * dp_count if a == axis else s for a, s in enumerate(part.shape)), part.dtype
        )
        for part, axis in zip(parts, axes)
    ]
    semaphores = [
        pltpu.SemaphoreType.DMA((len(parts), 4 * (dp_count // 4) + 1)),
        pltpu.SemaphoreType.DMA((len(parts), 4 * (dp_count // 4) + 1)),
        pltpu.SemaphoreType.DMA((len(parts),)),
        pltpu.SemaphoreType.DMA((2, mp_count)),
        pltpu.SemaphoreType.DMA((2, mp_count)),
        pltpu.SemaphoreType.DMA,
    ]
    if rows is not None:
        shapes.insert(
            0, jax.ShapeDtypeStruct((rows.shape[0], rows.shape[1] * mp_count), rows.dtype)
        )
    moved = 2 * sum(shape.size for shape in shapes)
    return pl.pallas_call(
        functools.partial(gather_kernel, dp_count, mp_count, tuple(axes), rows is not None),
        out_shape=shapes,
        in_specs=[pl.BlockSpec(memory_space=pltpu.VMEM)] * len(arrays),
        out_specs=[pl.BlockSpec(memory_space=pl.ANY)] * len(arrays),
        scratch_shapes=semaphores,
        compiler_params=pltpu.CompilerParams(collective_id=collective_id, has_side_effects=True),
        cost_estimate=pl.CostEstimate(flops=0, bytes_accessed=16 * moved, transcendentals=0),
        name="gather_all",
    )(*arrays)


def small_total_kernel(dp_count, mp_count, value_ref, total_ref, ring, line, part, send, receive, line_send, line_receive):
    place, spot = lax.axis_index("dp"), lax.axis_index("mp")
    barrier = pltpu.get_barrier_semaphore()
    ring_targets = [lax.rem(place + shift, dp_count) for shift in range(1, dp_count)]
    line_targets = [lax.rem(spot + shift, mp_count) for shift in range(1, mp_count)]
    for target in ring_targets:
        pl.semaphore_signal(barrier, device_id={"dp": target}, device_id_type=MESH)
    for target in line_targets:
        pl.semaphore_signal(barrier, device_id={"mp": target}, device_id_type=MESH)
    pl.semaphore_wait(barrier, dp_count + mp_count - 2)
    copies = []
    for shift, target in enumerate(ring_targets):
        copies.append(
            pltpu.make_async_remote_copy(
                value_ref,
                ring.at[place],
                send.at[shift],
                receive.at[shift],
                device_id={"dp": target},
                device_id_type=MESH,
            )
        )
    for copy in copies:
        copy.start()
    ring[place] = value_ref[...]
    for copy in copies:
        copy.wait()
    total = ring[0]
    for d in range(1, dp_count):
        total = total + ring[d]
    part[...] = total
    copies = []
    for shift, target in enumerate(line_targets):
        copies.append(
            pltpu.make_async_remote_copy(
                part,
                line.at[spot],
                line_send.at[shift],
                line_receive.at[shift],
                device_id={"mp": target},
                device_id_type=MESH,
            )
        )
    for copy in copies:
        copy.start()
    line[spot] = total
    for copy in copies:
        copy.wait()
    total = line[0]
    for m in range(1, mp_count):
        total = total + line[m]
    total_ref[...] = total


def small_total(value, collective_id):
    dp_count, mp_count = lax.axis_size("dp"), lax.axis_size("mp")
    return pl.pallas_call(
        functools.partial(small_total_kernel, dp_count, mp_count),
        out_shape=jax.ShapeDtypeStruct(value.shape, value.dtype),
        in_specs=[pl.BlockSpec(memory_space=pltpu.VMEM)],
        out_specs=pl.BlockSpec(memory_space=pltpu.VMEM),
        scratch_shapes=[
            pltpu.VMEM((dp_count, *value.shape), value.dtype),
            pltpu.VMEM((mp_count, *value.shape), value.dtype),
            pltpu.VMEM(value.shape, value.dtype),
            pltpu.SemaphoreType.DMA((dp_count - 1,)),
            pltpu.SemaphoreType.DMA((dp_count - 1,)),
            pltpu.SemaphoreType.DMA((mp_count - 1,)),
            pltpu.SemaphoreType.DMA((mp_count - 1,)),
        ],
        compiler_params=pltpu.CompilerParams(collective_id=collective_id, has_side_effects=True),
        cost_estimate=pl.CostEstimate(flops=0, bytes_accessed=1 << 22, transcendentals=0),
        name="small_total",
    )(value)


def ring_move(values, step):
    order = ring_order(lax.axis_size("dp"))
    chips = len(order)
    pairs = [
        (2 * chip + core, 2 * order[(pos + step) % chips] + core)
        for pos, chip in enumerate(order)
        for core in range(2)
    ]
    return lax.ppermute(values, "dp", pairs)


def core_swap(values):
    return lax.ppermute(values, "dp", [(i, i ^ 1) for i in range(lax.axis_size("dp"))])


def direct_move(values, step, swap):
    order = ring_order(lax.axis_size("dp"))
    chips = len(order)
    pairs = [
        (2 * chip + core, 2 * order[(pos + step) % chips] + (core ^ swap))
        for pos, chip in enumerate(order)
        for core in range(2)
    ]
    return lax.ppermute(values, "dp", pairs)


def spread_pairs(own):
    chips = lax.axis_size("dp") // 2
    half = own.shape[0] // 32 * 16
    same = [None] * chips
    same[0] = ahead = behind = own
    for step in range(1, chips // 2):
        ahead = same[step] = ring_move(ahead, 1)
        behind = same[chips - step] = ring_move(behind, -1)
    ends = [ring_move(ahead[:half], 1), ring_move(behind[half:], -1)]
    same[chips // 2] = jnp.concatenate(ends, axis=0)
    return [(rows, core_swap(rows)) for rows in same]


def spread_halves(own):
    chips = lax.axis_size("dp") // 2
    half = own.shape[0] // 2
    same = [None] * chips
    same[0] = ahead = behind = [own[:half], own[half:]]
    for step in range(1, chips // 2):
        ahead = same[step] = [ring_move(part, 1) for part in ahead]
        behind = same[chips - step] = [ring_move(part, -1) for part in behind[::-1]][::-1]
    same[chips // 2] = [ring_move(ahead[0], 1), ring_move(behind[1], -1)]
    return [parts + [core_swap(part) for part in parts] for parts in same]


def add_bf(left, right):
    return (left.astype(jnp.float32) + right.astype(jnp.float32)).astype(jnp.bfloat16)


def collect(pairs):
    chips = len(pairs)
    half = pairs[0][0].shape[0] // 2
    far = add_bf(pairs[chips // 2][0], core_swap(pairs[chips // 2][1]))
    merged = [add_bf(same, core_swap(other)) for same, other in pairs]
    carry_back, carry_on = ring_move(far[:half], -1), ring_move(far[half:], 1)
    for step in range(chips // 2 - 1, 0, -1):
        back, on = merged[step], merged[chips - step]
        if step == chips // 2 - 1:
            back = jnp.concatenate([add_bf(back[:half], carry_back), back[half:]], axis=0)
            on = jnp.concatenate([on[:half], add_bf(on[half:], carry_on)], axis=0)
        else:
            back, on = add_bf(back, carry_back), add_bf(on, carry_on)
        carry_back, carry_on = ring_move(back, -1), ring_move(on, 1)
    total = merged[0].astype(jnp.float32) + carry_back.astype(jnp.float32)
    return total + carry_on.astype(jnp.float32)


def relative_devices():
    dp_count = lax.axis_size("dp")
    _, pos, core, device_at = ring_neighbours(dp_count)
    places = []
    for k in range(dp_count // 2):
        same = device_at(pos - k)
        places.append((same, same + 1 - 2 * core))
    return places


def assemble_kernel(parts, places_ref, *refs):
    pieces, wholes = refs[: len(refs) - parts], refs[len(refs) - parts :]
    width = pieces[0].shape[1]
    for part in range(parts):

        @pl.when(pl.program_id(0) == part)
        def _(part=part):
            for i, piece in enumerate(pieces):
                start = pl.multiple_of(places_ref[i] * width, width)
                wholes[part][:, pl.ds(start, width)] = piece[...]


def assemble(pieces, places, parts):
    rows, width = pieces[0].shape[0] // parts, pieces[0].shape[1]
    whole = (rows, width * len(pieces))
    return pl.pallas_call(
        functools.partial(assemble_kernel, parts),
        grid_spec=pltpu.PrefetchScalarGridSpec(
            num_scalar_prefetch=1,
            grid=(parts,),
            in_specs=[pl.BlockSpec((rows, width), lambda i, p: (i, 0))] * len(pieces),
            out_specs=[pl.BlockSpec(whole, lambda i, p: (0, 0), pipeline_mode=pl.Buffered(1))]
            * parts,
        ),
        out_shape=[jax.ShapeDtypeStruct(whole, pieces[0].dtype)] * parts,
        cost_estimate=pl.CostEstimate(
            flops=0, bytes_accessed=8 * parts * whole[0] * whole[1], transcendentals=0
        ),
        name="assemble",
    )(places, *pieces)


def weight_grads(rows, cotangents, places):
    whole = jnp.dot(rows.T, cotangents, preferred_element_type=jnp.float32).astype(
        jnp.bfloat16
    )
    width = whole.shape[0] // lax.axis_size("dp")
    pairs = [
        tuple(lax.dynamic_slice_in_dim(whole, place * width, width) for place in pair)
        for pair in places
    ]
    return collect(pairs)


def line_share(partial_value):
    count = lax.axis_size("mp")
    spot = lax.axis_index("mp")
    width = partial_value.shape[1] // count
    rounded = partial_value.astype(jnp.bfloat16)
    total = lax.dynamic_slice_in_dim(partial_value, spot * width, width, axis=1)
    for shift in range(1, count):
        target = lax.rem(spot + shift, count)
        piece = lax.ppermute(
            lax.dynamic_slice_in_dim(rounded, target * width, width, axis=1),
            "mp",
            [(i, (i + shift) % count) for i in range(count)],
        )
        total = total + piece.astype(jnp.float32)
    return total


def line_total(partial_value):
    count = lax.axis_size("mp")
    total = partial_value
    for shift in range(1, count):
        total = total + lax.ppermute(
            partial_value, "mp", [(i, (i + shift) % count) for i in range(count)]
        )
    return total


def shards(
    block_input,
    segment_ids,
    expert_ids,
    norm_gain,
    query_weight,
    latent_down,
    latent_gain,
    latent_up,
    output_weight,
    moe_gain,
    router_weight,
    shared_gate,
    shared_up,
    shared_down,
    expert_gate,
    expert_up,
    expert_down,
    output_grad,
):
    model_width = norm_gain.shape[0]
    tokens_here = block_input.shape[0]
    share_width = block_input.shape[1]
    mp_count = lax.axis_size("mp")
    mp_place = lax.axis_index("mp")
    dp_count = lax.axis_size("dp")
    heads_here = H // mp_count
    experts_all = router_weight.shape[0]
    experts_group = experts_all // dp_count
    chips = dp_count // 2
    own_expert = lax.axis_index("dp") * experts_group + mp_place // 2
    expert_places = jnp.arange(experts_all, dtype=jnp.int32)
    own_gate = expert_gate[0]
    own_up = expert_up[0]
    own_down = expert_down[0]
    cosine, sine_tab = rope_tables(LEN, DR)
    inputs = block_input.astype(jnp.float32)
    gain_one = lax.dynamic_slice_in_dim(norm_gain, mp_place * share_width, share_width)
    per_head = query_weight.reshape(heads_here, DN + DR, -1)
    query_rows = jnp.concatenate(
        [
            per_head[:, :DN].reshape(heads_here * DN, -1),
            per_head[:, DN : DN + DR // 2].reshape(heads_here * DR // 2, -1),
            per_head[:, DN + DR // 2 :].reshape(heads_here * DR // 2, -1),
        ],
        axis=0,
    )
    gathered = gather_all(
        block_input,
        (query_rows, latent_down, latent_up.T, output_weight, router_weight),
        (1, 1, 0, 1, 1),
        1,
    )
    inputs_full = gathered[0].astype(jnp.float32)
    query_w, down_w, up_wt, out_w, router_w = gathered[1:]
    scale_one = lax.rsqrt(jnp.mean(inputs_full * inputs_full, axis=1, keepdims=True) + epsilon)
    normed = (inputs_full * scale_one * norm_gain).astype(jnp.bfloat16)
    places = relative_devices()
    late_ids, _ = lax.optimization_barrier((expert_ids, gathered[0]))
    picked_mask = jnp.max((late_ids[..., None] == expert_places).astype(jnp.float32), axis=1)
    mask_pairs = spread_pairs(picked_mask)
    shared_parts, _ = lax.optimization_barrier(
        (jnp.concatenate([shared_gate, shared_up, shared_down], axis=0), gathered[0])
    )
    shared_pieces = [piece for pair in spread_pairs(shared_parts) for piece in pair]
    hidden_here = shared_gate.shape[0]
    places_flat = jnp.stack([place for pair in places for place in pair]).astype(jnp.int32)
    sgate_w, sup_w, sdown_w = assemble(shared_pieces, places_flat, 3)
    late_grad, _ = lax.optimization_barrier((output_grad, gathered[0]))
    grad_full = full_rows(late_grad)
    grad_pairs = spread_halves(grad_full)
    nope_width, rope_width = heads_here * DN, heads_here * DR
    query_all = jnp.dot(normed, query_w.T, preferred_element_type=jnp.float32)
    cosines, sines = jnp.tile(cosine, (1, heads_here)), jnp.tile(sine_tab, (1, heads_here))
    query_nope = query_all[:, :nope_width].astype(jnp.bfloat16)
    query_rope = rotate(query_all[:, nope_width:], cosines, sines).astype(jnp.bfloat16)
    score_scale = (DN + DR) ** (-0.5)
    latent_part = jnp.dot(normed, down_w.T, preferred_element_type=jnp.float32).astype(
        jnp.bfloat16
    )
    latent = full_rows(latent_part).astype(jnp.float32)
    latent_main = latent[:, :KVL]
    scale_lat = lax.rsqrt(jnp.mean(latent_main * latent_main, axis=-1, keepdims=True) + epsilon)
    latent_normed = (latent_main * scale_lat * latent_gain).astype(jnp.bfloat16)
    key_rope = rotate(latent[:, KVL:], cosine, sine_tab).astype(jnp.bfloat16)
    key_rope = jnp.concatenate(
        [key_rope[:, : DR // 2]] * heads_here + [key_rope[:, DR // 2 :]] * heads_here, axis=1
    )
    keys_values = jnp.dot(latent_normed, up_wt, preferred_element_type=jnp.float32).astype(
        jnp.bfloat16
    )
    attended_flat, probs = attend_forward(
        query_nope, query_rope, keys_values, key_rope, segment_ids, heads_here, score_scale
    )
    attended_part = jnp.dot(attended_flat, out_w, preferred_element_type=jnp.float32).astype(
        jnp.bfloat16
    )
    attended_sum = mp_share(attended_part)
    residual = inputs + attended_sum
    residual_rounded = residual.astype(jnp.bfloat16)
    gain_two = lax.dynamic_slice_in_dim(moe_gain, mp_place * share_width, share_width)
    residual_full = full_rows(residual_rounded)
    residual_full = residual_full.astype(jnp.float32)
    scale_two = lax.rsqrt(
        jnp.mean(residual_full * residual_full, axis=1, keepdims=True) + epsilon
    )
    moe_in = (residual_full * scale_two * moe_gain).astype(jnp.bfloat16)
    row_pairs = spread_halves(moe_in)
    router_logits = jnp.dot(moe_in, router_w.T, preferred_element_type=jnp.float32)

    def masked_gates(logits, mask):
        pick_exp = jnp.exp(jnp.where(mask > 0, logits, negative))
        return pick_exp / jnp.sum(pick_exp, axis=-1, keepdims=True)

    gate_prob = masked_gates(router_logits, picked_mask)
    shared_g = jnp.dot(moe_in, sgate_w.T, preferred_element_type=jnp.float32)
    shared_u = jnp.dot(moe_in, sup_w.T, preferred_element_type=jnp.float32)
    shared_act = (jax.nn.silu(shared_g) * shared_u).astype(jnp.bfloat16)
    shared_part = jnp.dot(shared_act, sdown_w, preferred_element_type=jnp.float32)
    up_router = jnp.concatenate([own_up, router_w], axis=0)
    own_column = (expert_places == own_expert).astype(jnp.float32)[:, None]
    backs, gate_grads, held = [None] * chips, [None] * chips, ()
    visits = [0]
    for hop in range(1, chips // 2):
        visits += [hop, chips - hop]
    visits.insert(len(visits) - 1, chips // 2)
    for k in visits:
        done = expert_rows(
            k,
            chips,
            row_pairs[k],
            grad_pairs[k],
            jnp.concatenate(mask_pairs[k]).T,
            own_column,
            own_gate,
            up_router,
            own_down,
            held,
        )
        *back, gate_grads[k] = done[:3]
        backs[k], held = tuple(back), done[3:]
    routed_back = collect(backs)
    act_late, _ = lax.optimization_barrier((held[0], routed_back))
    tokens_pair = 2 * tokens_here

    def out_rows(low):
        return jnp.dot(
            act_late[:, low : low + tokens_here].T,
            own_down,
            preferred_element_type=jnp.float32,
        ).astype(jnp.bfloat16)

    out_pairs = [
        (out_rows(k * tokens_pair), out_rows(k * tokens_pair + tokens_here))
        for k in range(chips)
    ]
    act_all, gate_pre_all, up_pre_all, rows_all, grads_all = held
    expert_down_grad = jnp.dot(act_all, grads_all, preferred_element_type=jnp.float32)[None]
    expert_gate_grad = jnp.dot(
        gate_pre_all, rows_all, preferred_element_type=jnp.float32
    )[None]
    expert_up_grad = jnp.dot(up_pre_all, rows_all, preferred_element_type=jnp.float32)[None]
    gate_grads, _ = lax.optimization_barrier((gate_grads, routed_back))
    order = jnp.array(ring_order(dp_count), jnp.int32)
    dp_place = lax.axis_index("dp")
    ring_place = jnp.argmax((order == dp_place // 2).astype(jnp.int32)).astype(jnp.int32)
    gate_grad = jnp.zeros((tokens_here, experts_all), jnp.float32)
    for k, both in enumerate(gate_grads):
        chip_from = jnp.sum(
            jnp.where(jnp.arange(chips) == (ring_place + k) % chips, order, 0)
        )
        for swap in range(2):
            piece = both[0, swap * tokens_here : (swap + 1) * tokens_here]
            if k or swap:
                piece = direct_move(piece, -k, swap)
            device_from = 2 * chip_from + (dp_place % 2 if swap == 0 else 1 - dp_place % 2)
            expert_from = device_from * experts_group + mp_place // 2
            gate_grad = gate_grad + piece[:, None] * (expert_places == expert_from).astype(
                jnp.float32
            )
    gate_grad = line_total(gate_grad)
    routed_part = collect(out_pairs)
    moe_total = mp_share(shared_part + routed_part)
    block_output = (residual + moe_total).astype(jnp.bfloat16)
    logit_grad = (
        gate_prob * (gate_grad - jnp.sum(gate_prob * gate_grad, axis=-1, keepdims=True))
    ).astype(jnp.bfloat16)
    router_back = jnp.dot(logit_grad, router_w, preferred_element_type=jnp.float32)
    shared_act_grad = jnp.dot(grad_full, sdown_w.T, preferred_element_type=jnp.float32)
    shared_gate_pre = (shared_act_grad * shared_u * silu_grad(shared_g)).astype(jnp.bfloat16)
    shared_up_pre = (shared_act_grad * jax.nn.silu(shared_g)).astype(jnp.bfloat16)
    moe_late, grad_late, shared_late, _ = lax.optimization_barrier(
        (
            moe_in,
            grad_full,
            (shared_act, shared_gate_pre, shared_up_pre, logit_grad),
            routed_back,
        )
    )
    sdown_grad = weight_grads(grad_late, shared_late[0], places)
    moe_rows_grad = weight_grads(moe_late, jnp.concatenate(shared_late[1:], axis=1), places)
    shared_back = jnp.dot(
        shared_gate_pre, sgate_w, preferred_element_type=jnp.float32
    ) + jnp.dot(shared_up_pre, sup_w, preferred_element_type=jnp.float32)
    router_mine = lax.dynamic_slice_in_dim(router_back, mp_place * share_width, share_width, axis=1)
    back_share = mp_share(shared_back + routed_back)
    moe_in_grad = back_share + router_mine
    moe_in_grad_bf = moe_in_grad.astype(jnp.bfloat16)
    back_full = full_rows(moe_in_grad_bf)
    back_full = back_full.astype(jnp.float32)
    moe_gain_part = jnp.sum(back_full * residual_full * scale_two, axis=0)
    stat_two = jnp.mean(back_full * residual_full * moe_gain, axis=1, keepdims=True)
    residual_grad = (
        output_grad.astype(jnp.float32)
        + scale_two * gain_two * moe_in_grad
        - residual * scale_two**3 * stat_two
    )
    residual_bf = (
        grad_full.astype(jnp.float32)
        + scale_two * moe_gain * back_full
        - residual_full * scale_two**3 * stat_two
    ).astype(jnp.bfloat16)
    out_w_grad = weight_grads(residual_bf, attended_flat, places)
    attended_grad = jnp.dot(residual_bf, out_w.T, preferred_element_type=jnp.float32).astype(
        jnp.bfloat16
    )
    dq_nope, dq_rope, kv_grad, dk_ropes = attend_backward(
        probs,
        attended_grad,
        query_nope,
        query_rope,
        keys_values,
        key_rope,
        heads_here,
        score_scale,
    )
    query_grad = jnp.concatenate(
        [dq_nope, unrotate(dq_rope, cosines, sines).astype(jnp.bfloat16)], axis=1
    )
    dk_rope = jnp.sum(dk_ropes.reshape(-1, 2, heads_here, DR // 2), axis=2).reshape(-1, DR)
    up_w_grad = weight_grads(latent_normed, kv_grad, places)
    normed_lat_grad = jnp.dot(kv_grad, up_wt.T, preferred_element_type=jnp.float32)
    latent_gain_part = jnp.sum(normed_lat_grad * latent_main * scale_lat, axis=0)
    main_grad = scale_lat * latent_gain * normed_lat_grad - latent_main * scale_lat**3 * jnp.mean(
        normed_lat_grad * latent_main * latent_gain, axis=-1, keepdims=True
    )
    rope_grad = unrotate(dk_rope, cosine, sine_tab)
    latent_grad = line_share(jnp.concatenate([main_grad, rope_grad], axis=-1)).astype(jnp.bfloat16)
    query_rows_grad = weight_grads(
        normed, jnp.concatenate([query_grad, latent_grad], axis=1), places
    )
    normed_part = jnp.dot(query_grad, query_w, preferred_element_type=jnp.float32) + jnp.dot(
        latent_grad, down_w, preferred_element_type=jnp.float32
    )
    weighted_part = normed_part * inputs_full
    norm_gain_part = jnp.sum(weighted_part * scale_one, axis=0)
    stat_one = line_total(jnp.sum(weighted_part * norm_gain, axis=1))[:, None] / model_width
    moe_gain_part = jnp.where(mp_place == 0, moe_gain_part, 0.0)
    gain_total = small_total(
        jnp.concatenate([norm_gain_part, moe_gain_part, latent_gain_part]).reshape(-1, 128), 2
    ).reshape(-1)
    norm_gain_grad = gain_total[:model_width]
    moe_gain_grad = gain_total[model_width : 2 * model_width]
    latent_gain_grad = gain_total[2 * model_width :]
    normed_grad = mp_share(normed_part)
    input_grad = (
        residual_grad + scale_one * gain_one * normed_grad - inputs * scale_one**3 * stat_one
    )
    query_width = query_grad.shape[1]
    query_rows_grad, down_rows_grad = (
        query_rows_grad[:, :query_width].T,
        query_rows_grad[:, query_width:].T,
    )
    parts = [query_rows_grad[:nope_width].reshape(heads_here, DN, -1)]
    for half in range(2):
        low = nope_width + half * rope_width // 2
        parts.append(
            query_rows_grad[low : low + rope_width // 2].reshape(heads_here, DR // 2, -1)
        )
    query_weight_grad = jnp.concatenate(parts, axis=1).reshape(query_width, -1)
    latent_down_grad = down_rows_grad
    latent_up_grad = up_w_grad.T
    output_weight_grad = out_w_grad.T
    shared_gate_grad = moe_rows_grad[:, :hidden_here].T
    shared_up_grad = moe_rows_grad[:, hidden_here : 2 * hidden_here].T
    router_grad = moe_rows_grad[:, 2 * hidden_here :].T
    shared_down_grad = sdown_grad.T
    return (
        block_output,
        input_grad,
        norm_gain_grad,
        query_weight_grad,
        latent_down_grad,
        latent_gain_grad,
        latent_up_grad,
        output_weight_grad,
        moe_gain_grad,
        router_grad,
        shared_gate_grad,
        shared_up_grad,
        shared_down_grad,
        expert_gate_grad,
        expert_up_grad,
        expert_down_grad,
    )


def solution(mesh):
    in_specs = (
        P("dp", "mp"),
        P("dp", None),
        P("dp", None),
        P(),
        P("mp", "dp"),
        P("mp", "dp"),
        P(),
        P("mp", "dp"),
        P("mp", "dp"),
        P(),
        P(None, "dp"),
        P("mp", "dp"),
        P("mp", "dp"),
        P("mp", "dp"),
        P(("dp", "mp"), None, None),
        P(("dp", "mp"), None, None),
        P(("dp", "mp"), None, None),
        P("dp", "mp"),
    )
    out_specs = (
        P("dp", "mp"),
        P("dp", "mp"),
        P(),
        P("mp", "dp"),
        P("mp", "dp"),
        P(),
        P("mp", "dp"),
        P("mp", "dp"),
        P(),
        P(None, "dp"),
        P("mp", "dp"),
        P("mp", "dp"),
        P("mp", "dp"),
        P(("dp", "mp"), None, None),
        P(("dp", "mp"), None, None),
        P(("dp", "mp"), None, None),
    )

    return jax.shard_map(shards, mesh=mesh, in_specs=in_specs, out_specs=out_specs, check_vma=False)
```

```python
import functools

import jax
import jax.numpy as jnp
from jax import lax
from jax.experimental import pallas as pl
from jax.experimental.pallas import tpu as pltpu
from jax.sharding import PartitionSpec as P

MESH = pl.DeviceIdType.MESH

H = 16
DN = 128
DR = 64
DV = 128
KVL = 512
LEN = 512


epsilon = 1e-06
negative = -1e30


def rope_tables(length, rot_width):
    half_width = rot_width // 2
    frequency = 10000.0 ** (-(2.0 / rot_width) * jnp.arange(half_width, dtype=jnp.float32))
    angles = jnp.arange(length, dtype=jnp.float32)[:, None] * frequency[None, :]
    return (jnp.cos(angles), jnp.sin(angles))


def rotate(values, cosine, sine_tab):
    half_width = values.shape[-1] // 2
    leading = values[..., :half_width]
    trailing = values[..., half_width:]
    return jnp.concatenate(
        [leading * cosine - trailing * sine_tab, trailing * cosine + leading * sine_tab], axis=-1
    )


def unrotate(values, cosine, sine_tab):
    half_width = values.shape[-1] // 2
    leading = values[..., :half_width]
    trailing = values[..., half_width:]
    return jnp.concatenate(
        [leading * cosine + trailing * sine_tab, trailing * cosine - leading * sine_tab], axis=-1
    )


def silu_grad(preact):
    sigmoid_val = jax.nn.sigmoid(preact)
    return sigmoid_val * (1.0 + preact * (1.0 - sigmoid_val))


def head_lanes(shape, heads):
    lane = lax.broadcasted_iota(jnp.int32, shape, 1)
    per_head = shape[1] // (2 * heads)
    mine = lax.rem(lane, heads * per_head) // per_head == pl.program_id(0)
    return mine.astype(jnp.float32)


def attend_forward_kernel(
    heads, scale, q_ref, q_rope_ref, keys_ref, k_rope_ref, seg_row_ref, seg_col_ref, out_ref, probs_ref
):
    width = q_ref.shape[1]
    q_rope = (q_rope_ref[...].astype(jnp.float32) * head_lanes(q_rope_ref.shape, heads)).astype(
        jnp.bfloat16
    )
    nt = (((1,), (1,)), ((), ()))
    logits = lax.dot_general(
        q_ref[...], keys_ref[:, :width], nt, preferred_element_type=jnp.float32
    )
    logits = logits + lax.dot_general(
        q_rope, k_rope_ref[...], nt, preferred_element_type=jnp.float32
    )
    row = lax.broadcasted_iota(jnp.int32, logits.shape, 0)
    column = lax.broadcasted_iota(jnp.int32, logits.shape, 1)
    kept = (seg_col_ref[...] == seg_row_ref[...]) & (column <= row)
    weights = jnp.exp(jnp.where(kept, logits * scale, negative))
    probs = (weights / jnp.sum(weights, axis=1, keepdims=True)).astype(jnp.bfloat16)
    probs_ref[0] = probs
    out_ref[...] = jnp.dot(
        probs, keys_ref[:, width:], preferred_element_type=jnp.float32
    ).astype(jnp.bfloat16)


def attend_forward(q_nope, q_rope, keys_values, k_rope, seg_row, heads, scale):
    length = q_nope.shape[0]
    whole = lambda h: (0, 0)
    mine = lambda h: (0, h)
    return pl.pallas_call(
        functools.partial(attend_forward_kernel, heads, scale),
        grid=(heads,),
        out_shape=(
            jax.ShapeDtypeStruct((length, heads * DV), jnp.bfloat16),
            jax.ShapeDtypeStruct((heads, length, length), jnp.bfloat16),
        ),
        in_specs=[
            pl.BlockSpec((length, DN), mine),
            pl.BlockSpec(q_rope.shape, whole),
            pl.BlockSpec((length, DN + DV), mine),
            pl.BlockSpec(k_rope.shape, whole),
            pl.BlockSpec((1, length), whole),
            pl.BlockSpec((length, 1), whole),
        ],
        out_specs=(
            pl.BlockSpec((length, DV), mine),
            pl.BlockSpec((1, length, length), lambda h: (h, 0, 0)),
        ),
        cost_estimate=pl.CostEstimate(
            flops=2 * heads * length * length * (DN + DV + q_rope.shape[1]),
            bytes_accessed=4 * heads * length * length,
            transcendentals=heads * length * length,
        ),
        name="attend_forward",
    )(q_nope, q_rope, keys_values, k_rope, seg_row, seg_row.T)


def attend_backward_kernel(
    heads,
    scale,
    probs_ref,
    grad_ref,
    q_ref,
    q_rope_ref,
    keys_ref,
    k_rope_ref,
    dq_ref,
    dq_rope_ref,
    dkeys_ref,
    dk_rope_ref,
):
    width = q_ref.shape[1]
    lanes = head_lanes(q_rope_ref.shape, heads)
    q_rope = (q_rope_ref[...].astype(jnp.float32) * lanes).astype(jnp.bfloat16)
    probs, grad = probs_ref[0], grad_ref[...]
    prob_grad = lax.dot_general(
        grad, keys_ref[:, width:], (((1,), (1,)), ((), ())), preferred_element_type=jnp.float32
    )
    wide = probs.astype(jnp.float32)
    row_dot = jnp.sum(wide * prob_grad, axis=1, keepdims=True)
    score_grad = (wide * (prob_grad - row_dot) * scale).astype(jnp.bfloat16)
    tn = (((0,), (0,)), ((), ()))
    dq_ref[...] = jnp.dot(
        score_grad, keys_ref[:, :width], preferred_element_type=jnp.float32
    ).astype(jnp.bfloat16)
    dq_rope = lanes * jnp.dot(score_grad, k_rope_ref[...], preferred_element_type=jnp.float32)
    dk_rope = lax.dot_general(score_grad, q_rope, tn, preferred_element_type=jnp.float32)
    dkeys_ref[:, :width] = lax.dot_general(
        score_grad, q_ref[...], tn, preferred_element_type=jnp.float32
    ).astype(jnp.bfloat16)
    dkeys_ref[:, width:] = lax.dot_general(
        probs, grad, tn, preferred_element_type=jnp.float32
    ).astype(jnp.bfloat16)

    @pl.when(pl.program_id(0) == 0)
    def _():
        dq_rope_ref[...] = dq_rope
        dk_rope_ref[...] = dk_rope

    @pl.when(pl.program_id(0) > 0)
    def _():
        dq_rope_ref[...] += dq_rope
        dk_rope_ref[...] += dk_rope


def attend_backward(probs, grad, q_nope, q_rope, keys_values, k_rope, heads, scale):
    length = q_nope.shape[0]
    whole = lambda h: (0, 0)
    mine = lambda h: (0, h)
    return pl.pallas_call(
        functools.partial(attend_backward_kernel, heads, scale),
        grid=(heads,),
        out_shape=(
            jax.ShapeDtypeStruct(q_nope.shape, jnp.bfloat16),
            jax.ShapeDtypeStruct(q_rope.shape, jnp.float32),
            jax.ShapeDtypeStruct(keys_values.shape, jnp.bfloat16),
            jax.ShapeDtypeStruct(q_rope.shape, jnp.float32),
        ),
        in_specs=[
            pl.BlockSpec((1, length, length), lambda h: (h, 0, 0)),
            pl.BlockSpec((length, DV), mine),
            pl.BlockSpec((length, DN), mine),
            pl.BlockSpec(q_rope.shape, whole),
            pl.BlockSpec((length, DN + DV), mine),
            pl.BlockSpec(k_rope.shape, whole),
        ],
        out_specs=(
            pl.BlockSpec((length, DN), mine),
            pl.BlockSpec(q_rope.shape, whole),
            pl.BlockSpec((length, DN + DV), mine),
            pl.BlockSpec(q_rope.shape, whole),
        ),
        cost_estimate=pl.CostEstimate(
            flops=2 * heads * length * length * 2 * (DN + DV + q_rope.shape[1]),
            bytes_accessed=4 * heads * length * length,
            transcendentals=0,
        ),
        name="attend_backward",
    )(probs, grad, q_nope, q_rope, keys_values, k_rope)


def expert_kernel(held, k, *refs):
    xs, gs = refs[:4], refs[4:8]
    mask_ref, own_ref, *weights = refs[8:13]
    refs = refs[13 + held :]
    back_same, back_other, score_ref, act_ref, gate_pre_ref, up_pre_ref, x_all, g_all = refs[:8]
    x_kept, g_kept, pre_gate, pre_up, grads, gate_ref, up_ref, down_ref = refs[8:16]
    arrived, landed, stored = refs[16:]
    hidden = gate_ref.shape[0]
    half, tokens = xs[0].shape[0], 2 * xs[0].shape[0]
    nt = (((1,), (1,)), ((), ()))
    tn = (((0,), (0,)), ((), ()))
    slot = pl.program_id(0)
    first = slot == 0
    into = [
        pltpu.make_async_copy(weight, kept, arrived.at[i])
        for i, (weight, kept) in enumerate(zip(weights, (gate_ref, up_ref, down_ref)))
    ]

    def take(sources, kept, i, part):
        return pltpu.make_async_copy(
            sources[part],
            kept.at[part // 2, pl.ds(part % 2 * half, half), :],
            landed.at[i, part],
        )

    def store(kept, whole, i, part):
        rows = pl.ds((2 * k + part) * tokens, tokens)
        return pltpu.make_async_copy(kept.at[part], whole.at[rows, :], stored.at[i, part])

    @pl.when(first)
    def _():
        for part in range(2):
            take(xs, x_kept, 0, part).start()
        for copy in into:
            copy.start()
        for part in range(2):
            take(gs, g_kept, 1, part).start()
        for part in range(2, 4):
            take(xs, x_kept, 0, part).start()
            take(gs, g_kept, 1, part).start()

    def arrive(sources, kept, whole, i):
        for core in range(2):

            @pl.when(slot == core)
            def _(core=core):
                take(sources, kept, i, 2 * core).wait()
                take(sources, kept, i, 2 * core + 1).wait()
                store(kept, whole, i, core).start()

    def arrive_weight(i):
        @pl.when(first)
        def _():
            into[i].wait()

    arrive(xs, x_kept, x_all, 0)
    arrive_weight(0)
    pre_gate[...] = lax.dot_general(
        gate_ref[...], x_kept[slot], nt, preferred_element_type=jnp.float32
    )
    arrive_weight(1)
    pre_up[...] = lax.dot_general(
        up_ref[...], x_kept[slot], nt, preferred_element_type=jnp.float32
    )
    arrive(gs, g_kept, g_all, 1)
    arrive_weight(2)
    grads[...] = lax.dot_general(
        down_ref[...], g_kept[slot], nt, preferred_element_type=jnp.float32
    )
    mask = mask_ref[...]
    pick_exp = jnp.exp(jnp.where(mask > 0, pre_up[hidden:, :], negative))
    share = jnp.sum(pick_exp * own_ref[...], axis=0, keepdims=True) / jnp.sum(
        pick_exp, axis=0, keepdims=True
    )
    step = 32 if hidden % 32 == 0 else 16

    def body(i, score):
        rows = pl.ds(pl.multiple_of(i * step, step), step)
        gate_in, up_in, grad = pre_gate[rows, :], pre_up[rows, :], grads[rows, :]
        sig = jax.nn.sigmoid(gate_in)
        silu = gate_in * sig
        activation = silu * up_in
        scaled = grad * share
        act_ref[rows, :] = (activation * share).astype(jnp.bfloat16)
        gate_pre_ref[rows, :] = (scaled * up_in * (sig * (1.0 + gate_in * (1.0 - sig)))).astype(
            jnp.bfloat16
        )
        up_pre_ref[rows, :] = (scaled * silu).astype(jnp.bfloat16)
        return score + jnp.sum(activation * grad, axis=0, keepdims=True)

    score_ref[...] = lax.fori_loop(
        0, hidden // step, body, jnp.zeros((1, tokens), jnp.float32)
    )
    width = 512
    for low in range(0, gate_ref.shape[1], width):
        columns = slice(low, low + width)
        back = lax.dot_general(
            gate_pre_ref[...], gate_ref[:, columns], tn, preferred_element_type=jnp.float32
        ) + lax.dot_general(
            up_pre_ref[...], up_ref[:hidden, columns], tn, preferred_element_type=jnp.float32
        )
        back = back.astype(jnp.bfloat16)

        @pl.when(first)
        def _(back=back, columns=columns):
            back_same[:, columns] = back

        @pl.when(jnp.logical_not(first))
        def _(back=back, columns=columns):
            back_other[:, columns] = back

    @pl.when(jnp.logical_not(first))
    def _():
        for part in range(2):
            store(x_kept, x_all, 0, part).wait()
            store(g_kept, g_all, 1, part).wait()


def expert_rows(k, chips, rows, grads, mask, own, gate, up_router, down, held):
    half, width = rows[0].shape
    tokens = 2 * half
    hidden = gate.shape[0]
    whole = lambda shape: pl.BlockSpec(shape, lambda i: (0, 0), pipeline_mode=pl.Buffered(1))
    bf = jnp.bfloat16
    total = 2 * chips * tokens
    slab = pl.BlockSpec((hidden, tokens), lambda i: (0, 2 * k + i))
    anywhere = pl.BlockSpec(memory_space=pl.ANY)
    return pl.pallas_call(
        functools.partial(expert_kernel, len(held), k),
        grid=(2,),
        out_shape=(
            jax.ShapeDtypeStruct((tokens, width), bf),
            jax.ShapeDtypeStruct((tokens, width), bf),
            jax.ShapeDtypeStruct((1, 2 * tokens), jnp.float32),
            jax.ShapeDtypeStruct((hidden, total), bf),
            jax.ShapeDtypeStruct((hidden, total), bf),
            jax.ShapeDtypeStruct((hidden, total), bf),
            jax.ShapeDtypeStruct((total, width), bf),
            jax.ShapeDtypeStruct((total, width), bf),
        ),
        in_specs=[
            *[anywhere] * 8,
            pl.BlockSpec((mask.shape[0], tokens), lambda i: (0, i)),
            whole(own.shape),
            *[anywhere] * (3 + len(held)),
        ],
        out_specs=(
            whole((tokens, width)),
            whole((tokens, width)),
            pl.BlockSpec((1, tokens), lambda i: (0, i)),
            slab,
            slab,
            slab,
            anywhere,
            anywhere,
        ),
        scratch_shapes=[
            pltpu.VMEM((2, tokens, width), bf),
            pltpu.VMEM((2, tokens, width), bf),
            pltpu.VMEM((hidden, tokens), jnp.float32),
            pltpu.VMEM((up_router.shape[0], tokens), jnp.float32),
            pltpu.VMEM((hidden, tokens), jnp.float32),
            pltpu.VMEM(gate.shape, bf),
            pltpu.VMEM(up_router.shape, bf),
            pltpu.VMEM(down.shape, bf),
            pltpu.SemaphoreType.DMA((3,)),
            pltpu.SemaphoreType.DMA((2, 4)),
            pltpu.SemaphoreType.DMA((2, 2)),
        ],
        input_output_aliases={13 + i: 3 + i for i in range(len(held))},
        cost_estimate=pl.CostEstimate(
            flops=2 * 2 * tokens * hidden * width * 5,
            bytes_accessed=2 * (3 * hidden * width + 10 * tokens * width),
            transcendentals=2 * tokens * hidden,
        ),
        name="expert_rows",
    )(*rows, *grads, mask, own, gate, up_router, down, *held)


def full_rows(piece_rows):
    return lax.all_gather(piece_rows, "mp", axis=1, tiled=True)


def mp_share(partial_value):
    return lax.psum_scatter(
        partial_value.astype(jnp.bfloat16), "mp", scatter_dimension=1, tiled=True
    ).astype(jnp.float32)


def ring_order(dp_count):
    chips = dp_count // 2
    return list(range(chips // 2)) + list(range(chips - 1, chips // 2 - 1, -1))


def ring_neighbours(dp_count):
    order = ring_order(dp_count)
    chips = len(order)
    place = lax.axis_index("dp")
    chip, core = place // 2, place % 2
    pos = jnp.where(chip < chips // 2, chip, chips // 2 + chips - 1 - chip)

    def device_at(p):
        p = lax.rem(p + 2 * chips, chips)
        c = jnp.where(p < chips // 2, p, chips // 2 + chips - 1 - p)
        return 2 * c + core

    return place, pos, core, device_at


def gather_kernel(dp_count, mp_count, axes, has_rows, *refs):
    count = len(axes)
    if not has_rows:
        refs = (None, *refs[:count], None, *refs[count:])
    rows_ref, parts = refs[0], refs[1 : 1 + count]
    rows_out, wholes = refs[1 + count], refs[2 + count : 2 + 2 * count]
    send, receive, local, line_send, line_receive, line_local = refs[2 + 2 * count :]
    chips = dp_count // 2
    reach = chips // 2
    place, pos, core, device_at = ring_neighbours(dp_count)
    line = lax.axis_index("mp")
    on, back = device_at(pos + 1), device_at(pos - 1)
    other = place + 1 - 2 * core

    barrier = pltpu.get_barrier_semaphore()
    for target in (on, back, other):
        pl.semaphore_signal(barrier, device_id={"dp": target}, device_id_type=MESH)

    waits = 3
    if has_rows:

        @pl.when(line > 0)
        def _():
            pl.semaphore_signal(barrier, device_id={"mp": line - 1}, device_id_type=MESH)

        @pl.when(line < mp_count - 1)
        def _():
            pl.semaphore_signal(barrier, device_id={"mp": line + 1}, device_id_type=MESH)

        waits = 3 + (line > 0).astype(jnp.int32) + (line < mp_count - 1).astype(jnp.int32)
    pl.semaphore_wait(barrier, waits)

    width = rows_ref.shape[1] if has_rows else 0

    def columns(owner):
        return rows_out.at[:, pl.ds(pl.multiple_of(owner * width, width), width)]

    def line_copy(way, hop, source, owner):
        target = line + 1 if way == 0 else line - 1
        return pltpu.make_async_remote_copy(
            source,
            columns(owner),
            line_send.at[way, hop],
            line_receive.at[way, hop],
            device_id={"mp": target},
            device_id_type=MESH,
        )

    ends = (line < mp_count - 1, line > 0)

    def holds(way, hop):
        return line >= hop if way == 0 else line + hop <= mp_count - 1

    def owner_of(way, hop):
        return jnp.clip(line - hop if way == 0 else line + hop, 0, mp_count - 1)

    if has_rows:
        for way in range(2):

            @pl.when(ends[way])
            def _(way=way):
                line_copy(way, 0, rows_ref, line).start()

        keep_rows = pltpu.make_async_copy(rows_ref, columns(line), line_local)
        keep_rows.start()

    def block(i, owner, low, high):
        size = parts[i].shape[axes[i]]
        start = pl.multiple_of(owner * size, size)
        if axes[i] == 1:
            return wholes[i].at[pl.ds(low, high - low), pl.ds(start, size)]
        return wholes[i].at[pl.ds(start + low, high - low), :]

    def split(i, piece):
        rows = parts[i].shape[0]
        middle = rows // 32 * 16
        return ((0, rows), (0, middle), (middle, rows))[piece]

    def ring_copy(i, slot, source, owner, piece, target):
        low, high = split(i, piece)
        if source is None:
            source = block(i, owner, low, high)
        return pltpu.make_async_remote_copy(
            source,
            block(i, owner, low, high),
            send.at[i, slot],
            receive.at[i, slot],
            device_id={"dp": target},
            device_id_type=MESH,
        )

    def empty(i, piece):
        low, high = split(i, piece)
        return low == high

    started, kept = [], []
    for i in range(count):
        for way, target in ((0, on), (1, back)):
            piece = 0 if reach > 1 else 1 + way
            if not empty(i, piece):
                low, high = split(i, piece)
                copy = ring_copy(
                    i, way * reach, parts[i].at[pl.ds(low, high - low), :], place, piece, target
                )
                copy.start()
                started.append(copy)
        copy = ring_copy(i, 2 * reach, parts[i], place, 0, other)
        copy.start()
        started.append(copy)
        copy = pltpu.make_async_copy(
            parts[i], block(i, place, 0, parts[i].shape[0]), local.at[i]
        )
        copy.start()
        kept.append(copy)

    def line_step(hop):
        for way in range(2):

            @pl.when(holds(way, hop))
            def _(way=way):
                line_copy(way, hop - 1, rows_ref, owner_of(way, hop)).wait_recv()

            if hop < mp_count - 1:

                @pl.when(holds(way, hop) & ends[way])
                def _(way=way):
                    owner = owner_of(way, hop)
                    line_copy(way, hop, columns(owner), owner).start()

    def ring_step(i, hop):
        for way, target in ((0, on), (1, back)):
            piece = 0 if hop < reach else 1 + way
            if empty(i, piece):
                continue
            owner = device_at(pos - hop if way == 0 else pos + hop)
            ring_copy(i, way * reach + hop - 1, None, owner, piece, other).wait_recv()
            if hop < reach:
                ahead = 0 if hop + 1 < reach else 1 + way
                if not empty(i, ahead):
                    copy = ring_copy(i, way * reach + hop, None, owner, ahead, target)
                    copy.start()
                    started.append(copy)
            copy = ring_copy(i, 2 * reach + 1 + way * reach + hop - 1, None, owner, piece, other)
            copy.start()
            started.append(copy)

    line_hops = list(range(1, mp_count)) if has_rows else []
    for hop in range(1, reach + 1):
        for i in range(count):
            ring_step(i, hop)
        if line_hops:
            line_step(line_hops.pop(0))
    for hop in line_hops:
        line_step(hop)

    for i in range(count):
        twin = place + 1 - 2 * core
        ring_copy(i, 2 * reach, parts[i], twin, 0, other).wait_recv()
        for hop in range(1, reach + 1):
            for way in range(2):
                piece = 0 if hop < reach else 1 + way
                if empty(i, piece):
                    continue
                owner = device_at(pos - hop if way == 0 else pos + hop) + 1 - 2 * core
                ring_copy(
                    i, 2 * reach + 1 + way * reach + hop - 1, None, owner, piece, other
                ).wait_recv()
    for copy in started:
        copy.wait_send()
    for copy in kept:
        copy.wait()
    if not has_rows:
        return
    for way in range(2):

        @pl.when(ends[way])
        def _(way=way):
            line_copy(way, 0, rows_ref, line).wait_send()

        for hop in range(1, mp_count - 1):

            @pl.when(holds(way, hop) & ends[way])
            def _(way=way, hop=hop):
                owner = owner_of(way, hop)
                line_copy(way, hop, columns(owner), owner).wait_send()

    keep_rows.wait()


def gather_all(rows, parts, axes, collective_id):
    dp_count, mp_count = lax.axis_size("dp"), lax.axis_size("mp")
    arrays = [part for part in (rows, *parts) if part is not None]
    shapes = [
        jax.ShapeDtypeStruct(
            tuple(s * dp_count if a == axis else s for a, s in enumerate(part.shape)), part.dtype
        )
        for part, axis in zip(parts, axes)
    ]
    semaphores = [
        pltpu.SemaphoreType.DMA((len(parts), 4 * (dp_count // 4) + 1)),
        pltpu.SemaphoreType.DMA((len(parts), 4 * (dp_count // 4) + 1)),
        pltpu.SemaphoreType.DMA((len(parts),)),
        pltpu.SemaphoreType.DMA((2, mp_count)),
        pltpu.SemaphoreType.DMA((2, mp_count)),
        pltpu.SemaphoreType.DMA,
    ]
    if rows is not None:
        shapes.insert(
            0, jax.ShapeDtypeStruct((rows.shape[0], rows.shape[1] * mp_count), rows.dtype)
        )
    moved = 2 * sum(shape.size for shape in shapes)
    return pl.pallas_call(
        functools.partial(gather_kernel, dp_count, mp_count, tuple(axes), rows is not None),
        out_shape=shapes,
        in_specs=[pl.BlockSpec(memory_space=pltpu.VMEM)] * len(arrays),
        out_specs=[pl.BlockSpec(memory_space=pl.ANY)] * len(arrays),
        scratch_shapes=semaphores,
        compiler_params=pltpu.CompilerParams(collective_id=collective_id, has_side_effects=True),
        cost_estimate=pl.CostEstimate(flops=0, bytes_accessed=16 * moved, transcendentals=0),
        name="gather_all",
    )(*arrays)


def small_total_kernel(dp_count, mp_count, value_ref, total_ref, ring, line, part, send, receive, line_send, line_receive):
    place, spot = lax.axis_index("dp"), lax.axis_index("mp")
    barrier = pltpu.get_barrier_semaphore()
    ring_targets = [lax.rem(place + shift, dp_count) for shift in range(1, dp_count)]
    line_targets = [lax.rem(spot + shift, mp_count) for shift in range(1, mp_count)]
    for target in ring_targets:
        pl.semaphore_signal(barrier, device_id={"dp": target}, device_id_type=MESH)
    for target in line_targets:
        pl.semaphore_signal(barrier, device_id={"mp": target}, device_id_type=MESH)
    pl.semaphore_wait(barrier, dp_count + mp_count - 2)
    copies = []
    for shift, target in enumerate(ring_targets):
        copies.append(
            pltpu.make_async_remote_copy(
                value_ref,
                ring.at[place],
                send.at[shift],
                receive.at[shift],
                device_id={"dp": target},
                device_id_type=MESH,
            )
        )
    for copy in copies:
        copy.start()
    ring[place] = value_ref[...]
    for copy in copies:
        copy.wait()
    total = ring[0]
    for d in range(1, dp_count):
        total = total + ring[d]
    part[...] = total
    copies = []
    for shift, target in enumerate(line_targets):
        copies.append(
            pltpu.make_async_remote_copy(
                part,
                line.at[spot],
                line_send.at[shift],
                line_receive.at[shift],
                device_id={"mp": target},
                device_id_type=MESH,
            )
        )
    for copy in copies:
        copy.start()
    line[spot] = total
    for copy in copies:
        copy.wait()
    total = line[0]
    for m in range(1, mp_count):
        total = total + line[m]
    total_ref[...] = total


def small_total(value, collective_id):
    dp_count, mp_count = lax.axis_size("dp"), lax.axis_size("mp")
    return pl.pallas_call(
        functools.partial(small_total_kernel, dp_count, mp_count),
        out_shape=jax.ShapeDtypeStruct(value.shape, value.dtype),
        in_specs=[pl.BlockSpec(memory_space=pltpu.VMEM)],
        out_specs=pl.BlockSpec(memory_space=pltpu.VMEM),
        scratch_shapes=[
            pltpu.VMEM((dp_count, *value.shape), value.dtype),
            pltpu.VMEM((mp_count, *value.shape), value.dtype),
            pltpu.VMEM(value.shape, value.dtype),
            pltpu.SemaphoreType.DMA((dp_count - 1,)),
            pltpu.SemaphoreType.DMA((dp_count - 1,)),
            pltpu.SemaphoreType.DMA((mp_count - 1,)),
            pltpu.SemaphoreType.DMA((mp_count - 1,)),
        ],
        compiler_params=pltpu.CompilerParams(collective_id=collective_id, has_side_effects=True),
        cost_estimate=pl.CostEstimate(flops=0, bytes_accessed=1 << 22, transcendentals=0),
        name="small_total",
    )(value)


def ring_move(values, step):
    order = ring_order(lax.axis_size("dp"))
    chips = len(order)
    pairs = [
        (2 * chip + core, 2 * order[(pos + step) % chips] + core)
        for pos, chip in enumerate(order)
        for core in range(2)
    ]
    return lax.ppermute(values, "dp", pairs)


def core_swap(values):
    return lax.ppermute(values, "dp", [(i, i ^ 1) for i in range(lax.axis_size("dp"))])


def direct_move(values, step, swap):
    order = ring_order(lax.axis_size("dp"))
    chips = len(order)
    pairs = [
        (2 * chip + core, 2 * order[(pos + step) % chips] + (core ^ swap))
        for pos, chip in enumerate(order)
        for core in range(2)
    ]
    return lax.ppermute(values, "dp", pairs)


def spread_pairs(own):
    chips = lax.axis_size("dp") // 2
    half = own.shape[0] // 32 * 16
    same = [None] * chips
    same[0] = ahead = behind = own
    for step in range(1, chips // 2):
        ahead = same[step] = ring_move(ahead, 1)
        behind = same[chips - step] = ring_move(behind, -1)
    ends = [ring_move(ahead[:half], 1), ring_move(behind[half:], -1)]
    same[chips // 2] = jnp.concatenate(ends, axis=0)
    return [(rows, core_swap(rows)) for rows in same]


def spread_halves(own):
    chips = lax.axis_size("dp") // 2
    half = own.shape[0] // 2
    same = [None] * chips
    same[0] = ahead = behind = [own[:half], own[half:]]
    for step in range(1, chips // 2):
        ahead = same[step] = [ring_move(part, 1) for part in ahead]
        behind = same[chips - step] = [ring_move(part, -1) for part in behind[::-1]][::-1]
    same[chips // 2] = [ring_move(ahead[0], 1), ring_move(behind[1], -1)]
    return [parts + [core_swap(part) for part in parts] for parts in same]


def add_bf(left, right):
    return (left.astype(jnp.float32) + right.astype(jnp.float32)).astype(jnp.bfloat16)


def collect(pairs):
    chips = len(pairs)
    half = pairs[0][0].shape[0] // 2
    far = add_bf(pairs[chips // 2][0], core_swap(pairs[chips // 2][1]))
    merged = [add_bf(same, core_swap(other)) for same, other in pairs]
    carry_back, carry_on = ring_move(far[:half], -1), ring_move(far[half:], 1)
    for step in range(chips // 2 - 1, 0, -1):
        back, on = merged[step], merged[chips - step]
        if step == chips // 2 - 1:
            back = jnp.concatenate([add_bf(back[:half], carry_back), back[half:]], axis=0)
            on = jnp.concatenate([on[:half], add_bf(on[half:], carry_on)], axis=0)
        else:
            back, on = add_bf(back, carry_back), add_bf(on, carry_on)
        carry_back, carry_on = ring_move(back, -1), ring_move(on, 1)
    total = merged[0].astype(jnp.float32) + carry_back.astype(jnp.float32)
    return total + carry_on.astype(jnp.float32)


def relative_devices():
    dp_count = lax.axis_size("dp")
    _, pos, core, device_at = ring_neighbours(dp_count)
    places = []
    for k in range(dp_count // 2):
        same = device_at(pos - k)
        places.append((same, same + 1 - 2 * core))
    return places


def assemble_kernel(parts, places_ref, *refs):
    pieces, wholes = refs[: len(refs) - parts], refs[len(refs) - parts :]
    width = pieces[0].shape[1]
    for part in range(parts):

        @pl.when(pl.program_id(0) == part)
        def _(part=part):
            for i, piece in enumerate(pieces):
                start = pl.multiple_of(places_ref[i] * width, width)
                wholes[part][:, pl.ds(start, width)] = piece[...]


def assemble(pieces, places, parts):
    rows, width = pieces[0].shape[0] // parts, pieces[0].shape[1]
    whole = (rows, width * len(pieces))
    return pl.pallas_call(
        functools.partial(assemble_kernel, parts),
        grid_spec=pltpu.PrefetchScalarGridSpec(
            num_scalar_prefetch=1,
            grid=(parts,),
            in_specs=[pl.BlockSpec((rows, width), lambda i, p: (i, 0))] * len(pieces),
            out_specs=[pl.BlockSpec(whole, lambda i, p: (0, 0), pipeline_mode=pl.Buffered(1))]
            * parts,
        ),
        out_shape=[jax.ShapeDtypeStruct(whole, pieces[0].dtype)] * parts,
        cost_estimate=pl.CostEstimate(
            flops=0, bytes_accessed=8 * parts * whole[0] * whole[1], transcendentals=0
        ),
        name="assemble",
    )(places, *pieces)


def weight_grads(rows, cotangents, places):
    whole = jnp.dot(rows.T, cotangents, preferred_element_type=jnp.float32).astype(
        jnp.bfloat16
    )
    width = whole.shape[0] // lax.axis_size("dp")
    pairs = [
        tuple(lax.dynamic_slice_in_dim(whole, place * width, width) for place in pair)
        for pair in places
    ]
    return collect(pairs)


def line_share(partial_value):
    count = lax.axis_size("mp")
    spot = lax.axis_index("mp")
    width = partial_value.shape[1] // count
    rounded = partial_value.astype(jnp.bfloat16)
    total = lax.dynamic_slice_in_dim(partial_value, spot * width, width, axis=1)
    for shift in range(1, count):
        target = lax.rem(spot + shift, count)
        piece = lax.ppermute(
            lax.dynamic_slice_in_dim(rounded, target * width, width, axis=1),
            "mp",
            [(i, (i + shift) % count) for i in range(count)],
        )
        total = total + piece.astype(jnp.float32)
    return total


def line_total(partial_value):
    count = lax.axis_size("mp")
    total = partial_value
    for shift in range(1, count):
        total = total + lax.ppermute(
            partial_value, "mp", [(i, (i + shift) % count) for i in range(count)]
        )
    return total


def shards(
    block_input,
    segment_ids,
    expert_ids,
    norm_gain,
    query_weight,
    latent_down,
    latent_gain,
    latent_up,
    output_weight,
    moe_gain,
    router_weight,
    shared_gate,
    shared_up,
    shared_down,
    expert_gate,
    expert_up,
    expert_down,
    output_grad,
):
    model_width = norm_gain.shape[0]
    tokens_here = block_input.shape[0]
    share_width = block_input.shape[1]
    mp_count = lax.axis_size("mp")
    mp_place = lax.axis_index("mp")
    dp_count = lax.axis_size("dp")
    heads_here = H // mp_count
    experts_all = router_weight.shape[0]
    experts_group = experts_all // dp_count
    chips = dp_count // 2
    own_expert = lax.axis_index("dp") * experts_group + mp_place // 2
    expert_places = jnp.arange(experts_all, dtype=jnp.int32)
    own_gate = expert_gate[0]
    own_up = expert_up[0]
    own_down = expert_down[0]
    cosine, sine_tab = rope_tables(LEN, DR)
    inputs = block_input.astype(jnp.float32)
    gain_one = lax.dynamic_slice_in_dim(norm_gain, mp_place * share_width, share_width)
    per_head = query_weight.reshape(heads_here, DN + DR, -1)
    query_rows = jnp.concatenate(
        [
            per_head[:, :DN].reshape(heads_here * DN, -1),
            per_head[:, DN : DN + DR // 2].reshape(heads_here * DR // 2, -1),
            per_head[:, DN + DR // 2 :].reshape(heads_here * DR // 2, -1),
        ],
        axis=0,
    )
    gathered = gather_all(
        block_input,
        (query_rows, latent_down, latent_up.T, output_weight, router_weight),
        (1, 1, 0, 1, 1),
        1,
    )
    inputs_full = gathered[0].astype(jnp.float32)
    query_w, down_w, up_wt, out_w, router_w = gathered[1:]
    scale_one = lax.rsqrt(jnp.mean(inputs_full * inputs_full, axis=1, keepdims=True) + epsilon)
    normed = (inputs_full * scale_one * norm_gain).astype(jnp.bfloat16)
    places = relative_devices()
    late_ids, _ = lax.optimization_barrier((expert_ids, gathered[0]))
    picked_mask = jnp.max((late_ids[..., None] == expert_places).astype(jnp.float32), axis=1)
    mask_pairs = spread_pairs(picked_mask)
    shared_parts, _ = lax.optimization_barrier(
        (jnp.concatenate([shared_gate, shared_up, shared_down], axis=0), gathered[0])
    )
    shared_pieces = [piece for pair in spread_pairs(shared_parts) for piece in pair]
    hidden_here = shared_gate.shape[0]
    places_flat = jnp.stack([place for pair in places for place in pair]).astype(jnp.int32)
    sgate_w, sup_w, sdown_w = assemble(shared_pieces, places_flat, 3)
    late_grad, _ = lax.optimization_barrier((output_grad, gathered[0]))
    grad_full = full_rows(late_grad)
    grad_pairs = spread_halves(grad_full)
    nope_width, rope_width = heads_here * DN, heads_here * DR
    query_all = jnp.dot(normed, query_w.T, preferred_element_type=jnp.float32)
    cosines, sines = jnp.tile(cosine, (1, heads_here)), jnp.tile(sine_tab, (1, heads_here))
    query_nope = query_all[:, :nope_width].astype(jnp.bfloat16)
    query_rope = rotate(query_all[:, nope_width:], cosines, sines).astype(jnp.bfloat16)
    score_scale = (DN + DR) ** (-0.5)
    latent_part = jnp.dot(normed, down_w.T, preferred_element_type=jnp.float32).astype(
        jnp.bfloat16
    )
    latent = full_rows(latent_part).astype(jnp.float32)
    latent_main = latent[:, :KVL]
    scale_lat = lax.rsqrt(jnp.mean(latent_main * latent_main, axis=-1, keepdims=True) + epsilon)
    latent_normed = (latent_main * scale_lat * latent_gain).astype(jnp.bfloat16)
    key_rope = rotate(latent[:, KVL:], cosine, sine_tab).astype(jnp.bfloat16)
    key_rope = jnp.concatenate(
        [key_rope[:, : DR // 2]] * heads_here + [key_rope[:, DR // 2 :]] * heads_here, axis=1
    )
    keys_values = jnp.dot(latent_normed, up_wt, preferred_element_type=jnp.float32).astype(
        jnp.bfloat16
    )
    attended_flat, probs = attend_forward(
        query_nope, query_rope, keys_values, key_rope, segment_ids, heads_here, score_scale
    )
    attended_part = jnp.dot(attended_flat, out_w, preferred_element_type=jnp.float32).astype(
        jnp.bfloat16
    )
    attended_sum = mp_share(attended_part)
    residual = inputs + attended_sum
    residual_rounded = residual.astype(jnp.bfloat16)
    gain_two = lax.dynamic_slice_in_dim(moe_gain, mp_place * share_width, share_width)
    residual_full = full_rows(residual_rounded)
    residual_full = residual_full.astype(jnp.float32)
    scale_two = lax.rsqrt(
        jnp.mean(residual_full * residual_full, axis=1, keepdims=True) + epsilon
    )
    moe_in = (residual_full * scale_two * moe_gain).astype(jnp.bfloat16)
    row_pairs = spread_halves(moe_in)
    router_logits = jnp.dot(moe_in, router_w.T, preferred_element_type=jnp.float32)

    def masked_gates(logits, mask):
        pick_exp = jnp.exp(jnp.where(mask > 0, logits, negative))
        return pick_exp / jnp.sum(pick_exp, axis=-1, keepdims=True)

    gate_prob = masked_gates(router_logits, picked_mask)
    shared_g = jnp.dot(moe_in, sgate_w.T, preferred_element_type=jnp.float32)
    shared_u = jnp.dot(moe_in, sup_w.T, preferred_element_type=jnp.float32)
    shared_act = (jax.nn.silu(shared_g) * shared_u).astype(jnp.bfloat16)
    shared_part = jnp.dot(shared_act, sdown_w, preferred_element_type=jnp.float32)
    up_router = jnp.concatenate([own_up, router_w], axis=0)
    own_column = (expert_places == own_expert).astype(jnp.float32)[:, None]
    backs, gate_grads, held = [None] * chips, [None] * chips, ()
    visits = [0]
    for hop in range(1, chips // 2):
        visits += [hop, chips - hop]
    visits.insert(len(visits) - 1, chips // 2)
    for k in visits:
        done = expert_rows(
            k,
            chips,
            row_pairs[k],
            grad_pairs[k],
            jnp.concatenate(mask_pairs[k]).T,
            own_column,
            own_gate,
            up_router,
            own_down,
            held,
        )
        *back, gate_grads[k] = done[:3]
        backs[k], held = tuple(back), done[3:]
    routed_back = collect(backs)
    act_late, _ = lax.optimization_barrier((held[0], routed_back))
    tokens_pair = 2 * tokens_here

    def out_rows(low):
        return jnp.dot(
            act_late[:, low : low + tokens_here].T,
            own_down,
            preferred_element_type=jnp.float32,
        ).astype(jnp.bfloat16)

    out_pairs = [
        (out_rows(k * tokens_pair), out_rows(k * tokens_pair + tokens_here))
        for k in range(chips)
    ]
    act_all, gate_pre_all, up_pre_all, rows_all, grads_all = held
    expert_down_grad = jnp.dot(act_all, grads_all, preferred_element_type=jnp.float32)[None]
    expert_gate_grad = jnp.dot(
        gate_pre_all, rows_all, preferred_element_type=jnp.float32
    )[None]
    expert_up_grad = jnp.dot(up_pre_all, rows_all, preferred_element_type=jnp.float32)[None]
    gate_grads, _ = lax.optimization_barrier((gate_grads, routed_back))
    order = jnp.array(ring_order(dp_count), jnp.int32)
    dp_place = lax.axis_index("dp")
    ring_place = jnp.argmax((order == dp_place // 2).astype(jnp.int32)).astype(jnp.int32)
    gate_grad = jnp.zeros((tokens_here, experts_all), jnp.float32)
    for k, both in enumerate(gate_grads):
        chip_from = jnp.sum(
            jnp.where(jnp.arange(chips) == (ring_place + k) % chips, order, 0)
        )
        for swap in range(2):
            piece = both[0, swap * tokens_here : (swap + 1) * tokens_here]
            if k or swap:
                piece = direct_move(piece, -k, swap)
            device_from = 2 * chip_from + (dp_place % 2 if swap == 0 else 1 - dp_place % 2)
            expert_from = device_from * experts_group + mp_place // 2
            gate_grad = gate_grad + piece[:, None] * (expert_places == expert_from).astype(
                jnp.float32
            )
    gate_grad = line_total(gate_grad)
    routed_part = collect(out_pairs)
    moe_total = mp_share(shared_part + routed_part)
    block_output = (residual + moe_total).astype(jnp.bfloat16)
    logit_grad = (
        gate_prob * (gate_grad - jnp.sum(gate_prob * gate_grad, axis=-1, keepdims=True))
    ).astype(jnp.bfloat16)
    router_back = jnp.dot(logit_grad, router_w, preferred_element_type=jnp.float32)
    shared_act_grad = jnp.dot(grad_full, sdown_w.T, preferred_element_type=jnp.float32)
    shared_gate_pre = (shared_act_grad * shared_u * silu_grad(shared_g)).astype(jnp.bfloat16)
    shared_up_pre = (shared_act_grad * jax.nn.silu(shared_g)).astype(jnp.bfloat16)
    moe_late, grad_late, shared_late, _ = lax.optimization_barrier(
        (
            moe_in,
            grad_full,
            (shared_act, shared_gate_pre, shared_up_pre, logit_grad),
            routed_back,
        )
    )
    sdown_grad = weight_grads(grad_late, shared_late[0], places)
    moe_rows_grad = weight_grads(moe_late, jnp.concatenate(shared_late[1:], axis=1), places)
    shared_back = jnp.dot(
        shared_gate_pre, sgate_w, preferred_element_type=jnp.float32
    ) + jnp.dot(shared_up_pre, sup_w, preferred_element_type=jnp.float32)
    router_mine = lax.dynamic_slice_in_dim(router_back, mp_place * share_width, share_width, axis=1)
    back_share = mp_share(shared_back + routed_back)
    moe_in_grad = back_share + router_mine
    moe_in_grad_bf = moe_in_grad.astype(jnp.bfloat16)
    back_full = full_rows(moe_in_grad_bf)
    back_full = back_full.astype(jnp.float32)
    moe_gain_part = jnp.sum(back_full * residual_full * scale_two, axis=0)
    stat_two = jnp.mean(back_full * residual_full * moe_gain, axis=1, keepdims=True)
    residual_grad = (
        output_grad.astype(jnp.float32)
        + scale_two * gain_two * moe_in_grad
        - residual * scale_two**3 * stat_two
    )
    residual_bf = (
        grad_full.astype(jnp.float32)
        + scale_two * moe_gain * back_full
        - residual_full * scale_two**3 * stat_two
    ).astype(jnp.bfloat16)
    out_w_grad = weight_grads(residual_bf, attended_flat, places)
    attended_grad = jnp.dot(residual_bf, out_w.T, preferred_element_type=jnp.float32).astype(
        jnp.bfloat16
    )
    dq_nope, dq_rope, kv_grad, dk_ropes = attend_backward(
        probs,
        attended_grad,
        query_nope,
        query_rope,
        keys_values,
        key_rope,
        heads_here,
        score_scale,
    )
    query_grad = jnp.concatenate(
        [dq_nope, unrotate(dq_rope, cosines, sines).astype(jnp.bfloat16)], axis=1
    )
    dk_rope = jnp.sum(dk_ropes.reshape(-1, 2, heads_here, DR // 2), axis=2).reshape(-1, DR)
    up_w_grad = weight_grads(latent_normed, kv_grad, places)
    normed_lat_grad = jnp.dot(kv_grad, up_wt.T, preferred_element_type=jnp.float32)
    latent_gain_part = jnp.sum(normed_lat_grad * latent_main * scale_lat, axis=0)
    main_grad = scale_lat * latent_gain * normed_lat_grad - latent_main * scale_lat**3 * jnp.mean(
        normed_lat_grad * latent_main * latent_gain, axis=-1, keepdims=True
    )
    rope_grad = unrotate(dk_rope, cosine, sine_tab)
    latent_grad = line_share(jnp.concatenate([main_grad, rope_grad], axis=-1)).astype(jnp.bfloat16)
    query_rows_grad = weight_grads(
        normed, jnp.concatenate([query_grad, latent_grad], axis=1), places
    )
    normed_part = jnp.dot(query_grad, query_w, preferred_element_type=jnp.float32) + jnp.dot(
        latent_grad, down_w, preferred_element_type=jnp.float32
    )
    weighted_part = normed_part * inputs_full
    norm_gain_part = jnp.sum(weighted_part * scale_one, axis=0)
    stat_one = line_total(jnp.sum(weighted_part * norm_gain, axis=1))[:, None] / model_width
    moe_gain_part = jnp.where(mp_place == 0, moe_gain_part, 0.0)
    gain_total = small_total(
        jnp.concatenate([norm_gain_part, moe_gain_part, latent_gain_part]).reshape(-1, 128), 2
    ).reshape(-1)
    norm_gain_grad = gain_total[:model_width]
    moe_gain_grad = gain_total[model_width : 2 * model_width]
    latent_gain_grad = gain_total[2 * model_width :]
    normed_grad = mp_share(normed_part)
    input_grad = (
        residual_grad + scale_one * gain_one * normed_grad - inputs * scale_one**3 * stat_one
    )
    query_width = query_grad.shape[1]
    query_rows_grad, down_rows_grad = (
        query_rows_grad[:, :query_width].T,
        query_rows_grad[:, query_width:].T,
    )
    parts = [query_rows_grad[:nope_width].reshape(heads_here, DN, -1)]
    for half in range(2):
        low = nope_width + half * rope_width // 2
        parts.append(
            query_rows_grad[low : low + rope_width // 2].reshape(heads_here, DR // 2, -1)
        )
    query_weight_grad = jnp.concatenate(parts, axis=1).reshape(query_width, -1)
    latent_down_grad = down_rows_grad
    latent_up_grad = up_w_grad.T
    output_weight_grad = out_w_grad.T
    shared_gate_grad = moe_rows_grad[:, :hidden_here].T
    shared_up_grad = moe_rows_grad[:, hidden_here : 2 * hidden_here].T
    router_grad = moe_rows_grad[:, 2 * hidden_here :].T
    shared_down_grad = sdown_grad.T
    return (
        block_output,
        input_grad,
        norm_gain_grad,
        query_weight_grad,
        latent_down_grad,
        latent_gain_grad,
        latent_up_grad,
        output_weight_grad,
        moe_gain_grad,
        router_grad,
        shared_gate_grad,
        shared_up_grad,
        shared_down_grad,
        expert_gate_grad,
        expert_up_grad,
        expert_down_grad,
    )


def solution(mesh):
    in_specs = (
        P("dp", "mp"),
        P("dp", None),
        P("dp", None),
        P(),
        P("mp", "dp"),
        P("mp", "dp"),
        P(),
        P("mp", "dp"),
        P("mp", "dp"),
        P(),
        P(None, "dp"),
        P("mp", "dp"),
        P("mp", "dp"),
        P("mp", "dp"),
        P(("dp", "mp"), None, None),
        P(("dp", "mp"), None, None),
        P(("dp", "mp"), None, None),
        P("dp", "mp"),
    )
    out_specs = (
        P("dp", "mp"),
        P("dp", "mp"),
        P(),
        P("mp", "dp"),
        P("mp", "dp"),
        P(),
        P("mp", "dp"),
        P("mp", "dp"),
        P(),
        P(None, "dp"),
        P("mp", "dp"),
        P("mp", "dp"),
        P("mp", "dp"),
        P(("dp", "mp"), None, None),
        P(("dp", "mp"), None, None),
        P(("dp", "mp"), None, None),
    )

    return jax.shard_map(shards, mesh=mesh, in_specs=in_specs, out_specs=out_specs, check_vma=False)
```

```python
import functools

import jax
import jax.numpy as jnp
from jax import lax
from jax.experimental import pallas as pl
from jax.experimental.pallas import tpu as pltpu
from jax.sharding import PartitionSpec as P

MESH = pl.DeviceIdType.MESH

H = 16
DN = 128
DR = 64
DV = 128
KVL = 512
LEN = 512


epsilon = 1e-06
negative = -1e30


def rope_tables(length, rot_width):
    half_width = rot_width // 2
    frequency = 10000.0 ** (-(2.0 / rot_width) * jnp.arange(half_width, dtype=jnp.float32))
    angles = jnp.arange(length, dtype=jnp.float32)[:, None] * frequency[None, :]
    return (jnp.cos(angles), jnp.sin(angles))


def rotate(values, cosine, sine_tab):
    half_width = values.shape[-1] // 2
    leading = values[..., :half_width]
    trailing = values[..., half_width:]
    return jnp.concatenate(
        [leading * cosine - trailing * sine_tab, trailing * cosine + leading * sine_tab], axis=-1
    )


def unrotate(values, cosine, sine_tab):
    half_width = values.shape[-1] // 2
    leading = values[..., :half_width]
    trailing = values[..., half_width:]
    return jnp.concatenate(
        [leading * cosine + trailing * sine_tab, trailing * cosine - leading * sine_tab], axis=-1
    )


def silu_grad(preact):
    sigmoid_val = jax.nn.sigmoid(preact)
    return sigmoid_val * (1.0 + preact * (1.0 - sigmoid_val))


def head_lanes(shape, heads):
    lane = lax.broadcasted_iota(jnp.int32, shape, 1)
    per_head = shape[1] // (2 * heads)
    mine = lax.rem(lane, heads * per_head) // per_head == pl.program_id(0)
    return mine.astype(jnp.float32)


def attend_forward_kernel(
    heads, scale, q_ref, q_rope_ref, keys_ref, k_rope_ref, seg_row_ref, seg_col_ref, out_ref, probs_ref
):
    width = q_ref.shape[1]
    q_rope = (q_rope_ref[...].astype(jnp.float32) * head_lanes(q_rope_ref.shape, heads)).astype(
        jnp.bfloat16
    )
    nt = (((1,), (1,)), ((), ()))
    logits = lax.dot_general(
        q_ref[...], keys_ref[:, :width], nt, preferred_element_type=jnp.float32
    )
    logits = logits + lax.dot_general(
        q_rope, k_rope_ref[...], nt, preferred_element_type=jnp.float32
    )
    row = lax.broadcasted_iota(jnp.int32, logits.shape, 0)
    column = lax.broadcasted_iota(jnp.int32, logits.shape, 1)
    kept = (seg_col_ref[...] == seg_row_ref[...]) & (column <= row)
    weights = jnp.exp(jnp.where(kept, logits * scale, negative))
    probs = (weights / jnp.sum(weights, axis=1, keepdims=True)).astype(jnp.bfloat16)
    probs_ref[0] = probs
    out_ref[...] = jnp.dot(
        probs, keys_ref[:, width:], preferred_element_type=jnp.float32
    ).astype(jnp.bfloat16)


def attend_forward(q_nope, q_rope, keys_values, k_rope, seg_row, heads, scale):
    length = q_nope.shape[0]
    whole = lambda h: (0, 0)
    mine = lambda h: (0, h)
    return pl.pallas_call(
        functools.partial(attend_forward_kernel, heads, scale),
        grid=(heads,),
        out_shape=(
            jax.ShapeDtypeStruct((length, heads * DV), jnp.bfloat16),
            jax.ShapeDtypeStruct((heads, length, length), jnp.bfloat16),
        ),
        in_specs=[
            pl.BlockSpec((length, DN), mine),
            pl.BlockSpec(q_rope.shape, whole),
            pl.BlockSpec((length, DN + DV), mine),
            pl.BlockSpec(k_rope.shape, whole),
            pl.BlockSpec((1, length), whole),
            pl.BlockSpec((length, 1), whole),
        ],
        out_specs=(
            pl.BlockSpec((length, DV), mine),
            pl.BlockSpec((1, length, length), lambda h: (h, 0, 0)),
        ),
        cost_estimate=pl.CostEstimate(
            flops=2 * heads * length * length * (DN + DV + q_rope.shape[1]),
            bytes_accessed=4 * heads * length * length,
            transcendentals=heads * length * length,
        ),
        name="attend_forward",
    )(q_nope, q_rope, keys_values, k_rope, seg_row, seg_row.T)


def attend_backward_kernel(
    heads,
    scale,
    probs_ref,
    grad_ref,
    q_ref,
    q_rope_ref,
    keys_ref,
    k_rope_ref,
    dq_ref,
    dq_rope_ref,
    dkeys_ref,
    dk_rope_ref,
):
    width = q_ref.shape[1]
    lanes = head_lanes(q_rope_ref.shape, heads)
    q_rope = (q_rope_ref[...].astype(jnp.float32) * lanes).astype(jnp.bfloat16)
    probs, grad = probs_ref[0], grad_ref[...]
    prob_grad = lax.dot_general(
        grad, keys_ref[:, width:], (((1,), (1,)), ((), ())), preferred_element_type=jnp.float32
    )
    wide = probs.astype(jnp.float32)
    row_dot = jnp.sum(wide * prob_grad, axis=1, keepdims=True)
    score_grad = (wide * (prob_grad - row_dot) * scale).astype(jnp.bfloat16)
    tn = (((0,), (0,)), ((), ()))
    dq_ref[...] = jnp.dot(
        score_grad, keys_ref[:, :width], preferred_element_type=jnp.float32
    ).astype(jnp.bfloat16)
    dq_rope = lanes * jnp.dot(score_grad, k_rope_ref[...], preferred_element_type=jnp.float32)
    dk_rope = lax.dot_general(score_grad, q_rope, tn, preferred_element_type=jnp.float32)
    dkeys_ref[:, :width] = lax.dot_general(
        score_grad, q_ref[...], tn, preferred_element_type=jnp.float32
    ).astype(jnp.bfloat16)
    dkeys_ref[:, width:] = lax.dot_general(
        probs, grad, tn, preferred_element_type=jnp.float32
    ).astype(jnp.bfloat16)

    @pl.when(pl.program_id(0) == 0)
    def _():
        dq_rope_ref[...] = dq_rope
        dk_rope_ref[...] = dk_rope

    @pl.when(pl.program_id(0) > 0)
    def _():
        dq_rope_ref[...] += dq_rope
        dk_rope_ref[...] += dk_rope


def attend_backward(probs, grad, q_nope, q_rope, keys_values, k_rope, heads, scale):
    length = q_nope.shape[0]
    whole = lambda h: (0, 0)
    mine = lambda h: (0, h)
    return pl.pallas_call(
        functools.partial(attend_backward_kernel, heads, scale),
        grid=(heads,),
        out_shape=(
            jax.ShapeDtypeStruct(q_nope.shape, jnp.bfloat16),
            jax.ShapeDtypeStruct(q_rope.shape, jnp.float32),
            jax.ShapeDtypeStruct(keys_values.shape, jnp.bfloat16),
            jax.ShapeDtypeStruct(q_rope.shape, jnp.float32),
        ),
        in_specs=[
            pl.BlockSpec((1, length, length), lambda h: (h, 0, 0)),
            pl.BlockSpec((length, DV), mine),
            pl.BlockSpec((length, DN), mine),
            pl.BlockSpec(q_rope.shape, whole),
            pl.BlockSpec((length, DN + DV), mine),
            pl.BlockSpec(k_rope.shape, whole),
        ],
        out_specs=(
            pl.BlockSpec((length, DN), mine),
            pl.BlockSpec(q_rope.shape, whole),
            pl.BlockSpec((length, DN + DV), mine),
            pl.BlockSpec(q_rope.shape, whole),
        ),
        cost_estimate=pl.CostEstimate(
            flops=2 * heads * length * length * 2 * (DN + DV + q_rope.shape[1]),
            bytes_accessed=4 * heads * length * length,
            transcendentals=0,
        ),
        name="attend_backward",
    )(probs, grad, q_nope, q_rope, keys_values, k_rope)


def expert_kernel(held, k, *refs):
    xs, gs = refs[:4], refs[4:8]
    mask_ref, own_ref, *weights = refs[8:13]
    refs = refs[13 + held :]
    back_same, back_other, score_ref, act_ref, gate_pre_ref, up_pre_ref, x_all, g_all = refs[:8]
    x_kept, g_kept, pre_gate, pre_up, grads, gate_ref, up_ref, down_ref = refs[8:16]
    arrived, landed, stored = refs[16:]
    hidden = gate_ref.shape[0]
    half, tokens = xs[0].shape[0], 2 * xs[0].shape[0]
    nt = (((1,), (1,)), ((), ()))
    tn = (((0,), (0,)), ((), ()))
    slot = pl.program_id(0)
    first = slot == 0
    into = [
        pltpu.make_async_copy(weight, kept, arrived.at[i])
        for i, (weight, kept) in enumerate(zip(weights, (gate_ref, up_ref, down_ref)))
    ]

    def take(sources, kept, i, part):
        return pltpu.make_async_copy(
            sources[part],
            kept.at[part // 2, pl.ds(part % 2 * half, half), :],
            landed.at[i, part],
        )

    def store(kept, whole, i, part):
        rows = pl.ds((2 * k + part) * tokens, tokens)
        return pltpu.make_async_copy(kept.at[part], whole.at[rows, :], stored.at[i, part])

    @pl.when(first)
    def _():
        for part in range(2):
            take(xs, x_kept, 0, part).start()
        for copy in into:
            copy.start()
        for part in range(2):
            take(gs, g_kept, 1, part).start()
        for part in range(2, 4):
            take(xs, x_kept, 0, part).start()
            take(gs, g_kept, 1, part).start()

    def arrive(sources, kept, whole, i):
        for core in range(2):

            @pl.when(slot == core)
            def _(core=core):
                take(sources, kept, i, 2 * core).wait()
                take(sources, kept, i, 2 * core + 1).wait()
                store(kept, whole, i, core).start()

    def arrive_weight(i):
        @pl.when(first)
        def _():
            into[i].wait()

    arrive(xs, x_kept, x_all, 0)
    arrive_weight(0)
    pre_gate[...] = lax.dot_general(
        gate_ref[...], x_kept[slot], nt, preferred_element_type=jnp.float32
    )
    arrive_weight(1)
    pre_up[...] = lax.dot_general(
        up_ref[...], x_kept[slot], nt, preferred_element_type=jnp.float32
    )
    arrive(gs, g_kept, g_all, 1)
    arrive_weight(2)
    grads[...] = lax.dot_general(
        down_ref[...], g_kept[slot], nt, preferred_element_type=jnp.float32
    )
    mask = mask_ref[...]
    pick_exp = jnp.exp(jnp.where(mask > 0, pre_up[hidden:, :], negative))
    share = jnp.sum(pick_exp * own_ref[...], axis=0, keepdims=True) / jnp.sum(
        pick_exp, axis=0, keepdims=True
    )
    step = 64 if hidden % 64 == 0 else 16

    def body(i, score):
        rows = pl.ds(pl.multiple_of(i * step, step), step)
        gate_in, up_in, grad = pre_gate[rows, :], pre_up[rows, :], grads[rows, :]
        sig = jax.nn.sigmoid(gate_in)
        silu = gate_in * sig
        activation = silu * up_in
        scaled = grad * share
        act_ref[rows, :] = (activation * share).astype(jnp.bfloat16)
        gate_pre_ref[rows, :] = (scaled * up_in * (sig * (1.0 + gate_in * (1.0 - sig)))).astype(
            jnp.bfloat16
        )
        up_pre_ref[rows, :] = (scaled * silu).astype(jnp.bfloat16)
        return score + jnp.sum(activation * grad, axis=0, keepdims=True)

    score_ref[...] = lax.fori_loop(
        0, hidden // step, body, jnp.zeros((1, tokens), jnp.float32)
    )
    width = 512
    for low in range(0, gate_ref.shape[1], width):
        columns = slice(low, low + width)
        back = lax.dot_general(
            gate_pre_ref[...], gate_ref[:, columns], tn, preferred_element_type=jnp.float32
        ) + lax.dot_general(
            up_pre_ref[...], up_ref[:hidden, columns], tn, preferred_element_type=jnp.float32
        )
        back = back.astype(jnp.bfloat16)

        @pl.when(first)
        def _(back=back, columns=columns):
            back_same[:, columns] = back

        @pl.when(jnp.logical_not(first))
        def _(back=back, columns=columns):
            back_other[:, columns] = back

    @pl.when(jnp.logical_not(first))
    def _():
        for part in range(2):
            store(x_kept, x_all, 0, part).wait()
            store(g_kept, g_all, 1, part).wait()


def expert_rows(k, chips, rows, grads, mask, own, gate, up_router, down, held):
    half, width = rows[0].shape
    tokens = 2 * half
    hidden = gate.shape[0]
    whole = lambda shape: pl.BlockSpec(shape, lambda i: (0, 0), pipeline_mode=pl.Buffered(1))
    bf = jnp.bfloat16
    total = 2 * chips * tokens
    slab = pl.BlockSpec((hidden, tokens), lambda i: (0, 2 * k + i))
    anywhere = pl.BlockSpec(memory_space=pl.ANY)
    return pl.pallas_call(
        functools.partial(expert_kernel, len(held), k),
        grid=(2,),
        out_shape=(
            jax.ShapeDtypeStruct((tokens, width), bf),
            jax.ShapeDtypeStruct((tokens, width), bf),
            jax.ShapeDtypeStruct((1, 2 * tokens), jnp.float32),
            jax.ShapeDtypeStruct((hidden, total), bf),
            jax.ShapeDtypeStruct((hidden, total), bf),
            jax.ShapeDtypeStruct((hidden, total), bf),
            jax.ShapeDtypeStruct((total, width), bf),
            jax.ShapeDtypeStruct((total, width), bf),
        ),
        in_specs=[
            *[anywhere] * 8,
            pl.BlockSpec((mask.shape[0], tokens), lambda i: (0, i)),
            whole(own.shape),
            *[anywhere] * (3 + len(held)),
        ],
        out_specs=(
            whole((tokens, width)),
            whole((tokens, width)),
            pl.BlockSpec((1, tokens), lambda i: (0, i)),
            slab,
            slab,
            slab,
            anywhere,
            anywhere,
        ),
        scratch_shapes=[
            pltpu.VMEM((2, tokens, width), bf),
            pltpu.VMEM((2, tokens, width), bf),
            pltpu.VMEM((hidden, tokens), jnp.float32),
            pltpu.VMEM((up_router.shape[0], tokens), jnp.float32),
            pltpu.VMEM((hidden, tokens), jnp.float32),
            pltpu.VMEM(gate.shape, bf),
            pltpu.VMEM(up_router.shape, bf),
            pltpu.VMEM(down.shape, bf),
            pltpu.SemaphoreType.DMA((3,)),
            pltpu.SemaphoreType.DMA((2, 4)),
            pltpu.SemaphoreType.DMA((2, 2)),
        ],
        input_output_aliases={13 + i: 3 + i for i in range(len(held))},
        cost_estimate=pl.CostEstimate(
            flops=2 * 2 * tokens * hidden * width * 5,
            bytes_accessed=2 * (3 * hidden * width + 10 * tokens * width),
            transcendentals=2 * tokens * hidden,
        ),
        name="expert_rows",
    )(*rows, *grads, mask, own, gate, up_router, down, *held)


def full_rows(piece_rows):
    return lax.all_gather(piece_rows, "mp", axis=1, tiled=True)


def mp_share(partial_value):
    return lax.psum_scatter(
        partial_value.astype(jnp.bfloat16), "mp", scatter_dimension=1, tiled=True
    ).astype(jnp.float32)


def ring_order(dp_count):
    chips = dp_count // 2
    return list(range(chips // 2)) + list(range(chips - 1, chips // 2 - 1, -1))


def ring_neighbours(dp_count):
    order = ring_order(dp_count)
    chips = len(order)
    place = lax.axis_index("dp")
    chip, core = place // 2, place % 2
    pos = jnp.where(chip < chips // 2, chip, chips // 2 + chips - 1 - chip)

    def device_at(p):
        p = lax.rem(p + 2 * chips, chips)
        c = jnp.where(p < chips // 2, p, chips // 2 + chips - 1 - p)
        return 2 * c + core

    return place, pos, core, device_at


def gather_kernel(dp_count, mp_count, axes, has_rows, *refs):
    count = len(axes)
    if not has_rows:
        refs = (None, *refs[:count], None, *refs[count:])
    rows_ref, parts = refs[0], refs[1 : 1 + count]
    rows_out, wholes = refs[1 + count], refs[2 + count : 2 + 2 * count]
    send, receive, local, line_send, line_receive, line_local = refs[2 + 2 * count :]
    chips = dp_count // 2
    reach = chips // 2
    place, pos, core, device_at = ring_neighbours(dp_count)
    line = lax.axis_index("mp")
    on, back = device_at(pos + 1), device_at(pos - 1)
    other = place + 1 - 2 * core

    barrier = pltpu.get_barrier_semaphore()
    for target in (on, back, other):
        pl.semaphore_signal(barrier, device_id={"dp": target}, device_id_type=MESH)

    waits = 3
    if has_rows:

        @pl.when(line > 0)
        def _():
            pl.semaphore_signal(barrier, device_id={"mp": line - 1}, device_id_type=MESH)

        @pl.when(line < mp_count - 1)
        def _():
            pl.semaphore_signal(barrier, device_id={"mp": line + 1}, device_id_type=MESH)

        waits = 3 + (line > 0).astype(jnp.int32) + (line < mp_count - 1).astype(jnp.int32)
    pl.semaphore_wait(barrier, waits)

    width = rows_ref.shape[1] if has_rows else 0

    def columns(owner):
        return rows_out.at[:, pl.ds(pl.multiple_of(owner * width, width), width)]

    def line_copy(way, hop, source, owner):
        target = line + 1 if way == 0 else line - 1
        return pltpu.make_async_remote_copy(
            source,
            columns(owner),
            line_send.at[way, hop],
            line_receive.at[way, hop],
            device_id={"mp": target},
            device_id_type=MESH,
        )

    ends = (line < mp_count - 1, line > 0)

    def holds(way, hop):
        return line >= hop if way == 0 else line + hop <= mp_count - 1

    def owner_of(way, hop):
        return jnp.clip(line - hop if way == 0 else line + hop, 0, mp_count - 1)

    if has_rows:
        for way in range(2):

            @pl.when(ends[way])
            def _(way=way):
                line_copy(way, 0, rows_ref, line).start()

        keep_rows = pltpu.make_async_copy(rows_ref, columns(line), line_local)
        keep_rows.start()

    def block(i, owner, low, high):
        size = parts[i].shape[axes[i]]
        start = pl.multiple_of(owner * size, size)
        if axes[i] == 1:
            return wholes[i].at[pl.ds(low, high - low), pl.ds(start, size)]
        return wholes[i].at[pl.ds(start + low, high - low), :]

    def split(i, piece):
        rows = parts[i].shape[0]
        middle = rows // 32 * 16
        return ((0, rows), (0, middle), (middle, rows))[piece]

    def ring_copy(i, slot, source, owner, piece, target):
        low, high = split(i, piece)
        if source is None:
            source = block(i, owner, low, high)
        return pltpu.make_async_remote_copy(
            source,
            block(i, owner, low, high),
            send.at[i, slot],
            receive.at[i, slot],
            device_id={"dp": target},
            device_id_type=MESH,
        )

    def empty(i, piece):
        low, high = split(i, piece)
        return low == high

    started, kept = [], []
    for i in range(count):
        for way, target in ((0, on), (1, back)):
            piece = 0 if reach > 1 else 1 + way
            if not empty(i, piece):
                low, high = split(i, piece)
                copy = ring_copy(
                    i, way * reach, parts[i].at[pl.ds(low, high - low), :], place, piece, target
                )
                copy.start()
                started.append(copy)
        copy = ring_copy(i, 2 * reach, parts[i], place, 0, other)
        copy.start()
        started.append(copy)
        copy = pltpu.make_async_copy(
            parts[i], block(i, place, 0, parts[i].shape[0]), local.at[i]
        )
        copy.start()
        kept.append(copy)

    def line_step(hop):
        for way in range(2):

            @pl.when(holds(way, hop))
            def _(way=way):
                line_copy(way, hop - 1, rows_ref, owner_of(way, hop)).wait_recv()

            if hop < mp_count - 1:

                @pl.when(holds(way, hop) & ends[way])
                def _(way=way):
                    owner = owner_of(way, hop)
                    line_copy(way, hop, columns(owner), owner).start()

    def ring_step(i, hop):
        for way, target in ((0, on), (1, back)):
            piece = 0 if hop < reach else 1 + way
            if empty(i, piece):
                continue
            owner = device_at(pos - hop if way == 0 else pos + hop)
            ring_copy(i, way * reach + hop - 1, None, owner, piece, other).wait_recv()
            if hop < reach:
                ahead = 0 if hop + 1 < reach else 1 + way
                if not empty(i, ahead):
                    copy = ring_copy(i, way * reach + hop, None, owner, ahead, target)
                    copy.start()
                    started.append(copy)
            copy = ring_copy(i, 2 * reach + 1 + way * reach + hop - 1, None, owner, piece, other)
            copy.start()
            started.append(copy)

    line_hops = list(range(1, mp_count)) if has_rows else []
    for hop in range(1, reach + 1):
        for i in range(count):
            ring_step(i, hop)
        if line_hops:
            line_step(line_hops.pop(0))
    for hop in line_hops:
        line_step(hop)

    for i in range(count):
        twin = place + 1 - 2 * core
        ring_copy(i, 2 * reach, parts[i], twin, 0, other).wait_recv()
        for hop in range(1, reach + 1):
            for way in range(2):
                piece = 0 if hop < reach else 1 + way
                if empty(i, piece):
                    continue
                owner = device_at(pos - hop if way == 0 else pos + hop) + 1 - 2 * core
                ring_copy(
                    i, 2 * reach + 1 + way * reach + hop - 1, None, owner, piece, other
                ).wait_recv()
    for copy in started:
        copy.wait_send()
    for copy in kept:
        copy.wait()
    if not has_rows:
        return
    for way in range(2):

        @pl.when(ends[way])
        def _(way=way):
            line_copy(way, 0, rows_ref, line).wait_send()

        for hop in range(1, mp_count - 1):

            @pl.when(holds(way, hop) & ends[way])
            def _(way=way, hop=hop):
                owner = owner_of(way, hop)
                line_copy(way, hop, columns(owner), owner).wait_send()

    keep_rows.wait()


def gather_all(rows, parts, axes, collective_id):
    dp_count, mp_count = lax.axis_size("dp"), lax.axis_size("mp")
    arrays = [part for part in (rows, *parts) if part is not None]
    shapes = [
        jax.ShapeDtypeStruct(
            tuple(s * dp_count if a == axis else s for a, s in enumerate(part.shape)), part.dtype
        )
        for part, axis in zip(parts, axes)
    ]
    semaphores = [
        pltpu.SemaphoreType.DMA((len(parts), 4 * (dp_count // 4) + 1)),
        pltpu.SemaphoreType.DMA((len(parts), 4 * (dp_count // 4) + 1)),
        pltpu.SemaphoreType.DMA((len(parts),)),
        pltpu.SemaphoreType.DMA((2, mp_count)),
        pltpu.SemaphoreType.DMA((2, mp_count)),
        pltpu.SemaphoreType.DMA,
    ]
    if rows is not None:
        shapes.insert(
            0, jax.ShapeDtypeStruct((rows.shape[0], rows.shape[1] * mp_count), rows.dtype)
        )
    moved = 2 * sum(shape.size for shape in shapes)
    return pl.pallas_call(
        functools.partial(gather_kernel, dp_count, mp_count, tuple(axes), rows is not None),
        out_shape=shapes,
        in_specs=[pl.BlockSpec(memory_space=pltpu.VMEM)] * len(arrays),
        out_specs=[pl.BlockSpec(memory_space=pl.ANY)] * len(arrays),
        scratch_shapes=semaphores,
        compiler_params=pltpu.CompilerParams(collective_id=collective_id, has_side_effects=True),
        cost_estimate=pl.CostEstimate(flops=0, bytes_accessed=16 * moved, transcendentals=0),
        name="gather_all",
    )(*arrays)


def small_total_kernel(dp_count, mp_count, value_ref, total_ref, ring, line, part, send, receive, line_send, line_receive):
    place, spot = lax.axis_index("dp"), lax.axis_index("mp")
    barrier = pltpu.get_barrier_semaphore()
    ring_targets = [lax.rem(place + shift, dp_count) for shift in range(1, dp_count)]
    line_targets = [lax.rem(spot + shift, mp_count) for shift in range(1, mp_count)]
    for target in ring_targets:
        pl.semaphore_signal(barrier, device_id={"dp": target}, device_id_type=MESH)
    for target in line_targets:
        pl.semaphore_signal(barrier, device_id={"mp": target}, device_id_type=MESH)
    pl.semaphore_wait(barrier, dp_count + mp_count - 2)
    copies = []
    for shift, target in enumerate(ring_targets):
        copies.append(
            pltpu.make_async_remote_copy(
                value_ref,
                ring.at[place],
                send.at[shift],
                receive.at[shift],
                device_id={"dp": target},
                device_id_type=MESH,
            )
        )
    for copy in copies:
        copy.start()
    ring[place] = value_ref[...]
    for copy in copies:
        copy.wait()
    total = ring[0]
    for d in range(1, dp_count):
        total = total + ring[d]
    part[...] = total
    copies = []
    for shift, target in enumerate(line_targets):
        copies.append(
            pltpu.make_async_remote_copy(
                part,
                line.at[spot],
                line_send.at[shift],
                line_receive.at[shift],
                device_id={"mp": target},
                device_id_type=MESH,
            )
        )
    for copy in copies:
        copy.start()
    line[spot] = total
    for copy in copies:
        copy.wait()
    total = line[0]
    for m in range(1, mp_count):
        total = total + line[m]
    total_ref[...] = total


def small_total(value, collective_id):
    dp_count, mp_count = lax.axis_size("dp"), lax.axis_size("mp")
    return pl.pallas_call(
        functools.partial(small_total_kernel, dp_count, mp_count),
        out_shape=jax.ShapeDtypeStruct(value.shape, value.dtype),
        in_specs=[pl.BlockSpec(memory_space=pltpu.VMEM)],
        out_specs=pl.BlockSpec(memory_space=pltpu.VMEM),
        scratch_shapes=[
            pltpu.VMEM((dp_count, *value.shape), value.dtype),
            pltpu.VMEM((mp_count, *value.shape), value.dtype),
            pltpu.VMEM(value.shape, value.dtype),
            pltpu.SemaphoreType.DMA((dp_count - 1,)),
            pltpu.SemaphoreType.DMA((dp_count - 1,)),
            pltpu.SemaphoreType.DMA((mp_count - 1,)),
            pltpu.SemaphoreType.DMA((mp_count - 1,)),
        ],
        compiler_params=pltpu.CompilerParams(collective_id=collective_id, has_side_effects=True),
        cost_estimate=pl.CostEstimate(flops=0, bytes_accessed=1 << 22, transcendentals=0),
        name="small_total",
    )(value)


def ring_move(values, step):
    order = ring_order(lax.axis_size("dp"))
    chips = len(order)
    pairs = [
        (2 * chip + core, 2 * order[(pos + step) % chips] + core)
        for pos, chip in enumerate(order)
        for core in range(2)
    ]
    return lax.ppermute(values, "dp", pairs)


def core_swap(values):
    return lax.ppermute(values, "dp", [(i, i ^ 1) for i in range(lax.axis_size("dp"))])


def direct_move(values, step, swap):
    order = ring_order(lax.axis_size("dp"))
    chips = len(order)
    pairs = [
        (2 * chip + core, 2 * order[(pos + step) % chips] + (core ^ swap))
        for pos, chip in enumerate(order)
        for core in range(2)
    ]
    return lax.ppermute(values, "dp", pairs)


def spread_pairs(own):
    chips = lax.axis_size("dp") // 2
    half = own.shape[0] // 32 * 16
    same = [None] * chips
    same[0] = ahead = behind = own
    for step in range(1, chips // 2):
        ahead = same[step] = ring_move(ahead, 1)
        behind = same[chips - step] = ring_move(behind, -1)
    ends = [ring_move(ahead[:half], 1), ring_move(behind[half:], -1)]
    same[chips // 2] = jnp.concatenate(ends, axis=0)
    return [(rows, core_swap(rows)) for rows in same]


def spread_halves(own):
    chips = lax.axis_size("dp") // 2
    half = own.shape[0] // 2
    same = [None] * chips
    same[0] = ahead = behind = [own[:half], own[half:]]
    for step in range(1, chips // 2):
        ahead = same[step] = [ring_move(part, 1) for part in ahead]
        behind = same[chips - step] = [ring_move(part, -1) for part in behind[::-1]][::-1]
    same[chips // 2] = [ring_move(ahead[0], 1), ring_move(behind[1], -1)]
    return [parts + [core_swap(part) for part in parts] for parts in same]


def add_bf(left, right):
    return (left.astype(jnp.float32) + right.astype(jnp.float32)).astype(jnp.bfloat16)


def collect(pairs):
    chips = len(pairs)
    half = pairs[0][0].shape[0] // 2
    others = []
    for pair in pairs:
        others.append(core_swap(pair[1]))
    far = add_bf(pairs[chips // 2][0], others[chips // 2])
    merged = [add_bf(pair[0], other) for pair, other in zip(pairs, others)]
    carry_back, carry_on = ring_move(far[:half], -1), ring_move(far[half:], 1)
    for step in range(chips // 2 - 1, 0, -1):
        back, on = merged[step], merged[chips - step]
        if step == chips // 2 - 1:
            back = jnp.concatenate([add_bf(back[:half], carry_back), back[half:]], axis=0)
            on = jnp.concatenate([on[:half], add_bf(on[half:], carry_on)], axis=0)
        else:
            back, on = add_bf(back, carry_back), add_bf(on, carry_on)
        carry_back, carry_on = ring_move(back, -1), ring_move(on, 1)
    total = merged[0].astype(jnp.float32) + carry_back.astype(jnp.float32)
    return total + carry_on.astype(jnp.float32)


def relative_devices():
    dp_count = lax.axis_size("dp")
    _, pos, core, device_at = ring_neighbours(dp_count)
    places = []
    for k in range(dp_count // 2):
        same = device_at(pos - k)
        places.append((same, same + 1 - 2 * core))
    return places


def assemble_kernel(parts, places_ref, *refs):
    pieces, wholes = refs[: len(refs) - parts], refs[len(refs) - parts :]
    width = pieces[0].shape[1]
    for part in range(parts):

        @pl.when(pl.program_id(0) == part)
        def _(part=part):
            for i, piece in enumerate(pieces):
                start = pl.multiple_of(places_ref[i] * width, width)
                wholes[part][:, pl.ds(start, width)] = piece[...]


def assemble(pieces, places, parts):
    rows, width = pieces[0].shape[0] // parts, pieces[0].shape[1]
    whole = (rows, width * len(pieces))
    return pl.pallas_call(
        functools.partial(assemble_kernel, parts),
        grid_spec=pltpu.PrefetchScalarGridSpec(
            num_scalar_prefetch=1,
            grid=(parts,),
            in_specs=[pl.BlockSpec((rows, width), lambda i, p: (i, 0))] * len(pieces),
            out_specs=[pl.BlockSpec(whole, lambda i, p: (0, 0), pipeline_mode=pl.Buffered(1))]
            * parts,
        ),
        out_shape=[jax.ShapeDtypeStruct(whole, pieces[0].dtype)] * parts,
        cost_estimate=pl.CostEstimate(
            flops=0, bytes_accessed=8 * parts * whole[0] * whole[1], transcendentals=0
        ),
        name="assemble",
    )(places, *pieces)


def weight_grads(rows, cotangents, places):
    whole = jnp.dot(rows.T, cotangents, preferred_element_type=jnp.float32).astype(
        jnp.bfloat16
    )
    width = whole.shape[0] // lax.axis_size("dp")
    pairs = [
        tuple(lax.dynamic_slice_in_dim(whole, place * width, width) for place in pair)
        for pair in places
    ]
    return collect(pairs)


def line_share(partial_value):
    count = lax.axis_size("mp")
    spot = lax.axis_index("mp")
    width = partial_value.shape[1] // count
    rounded = partial_value.astype(jnp.bfloat16)
    total = lax.dynamic_slice_in_dim(partial_value, spot * width, width, axis=1)
    for shift in range(1, count):
        target = lax.rem(spot + shift, count)
        piece = lax.ppermute(
            lax.dynamic_slice_in_dim(rounded, target * width, width, axis=1),
            "mp",
            [(i, (i + shift) % count) for i in range(count)],
        )
        total = total + piece.astype(jnp.float32)
    return total


def line_total(partial_value):
    count = lax.axis_size("mp")
    total = partial_value
    for shift in range(1, count):
        total = total + lax.ppermute(
            partial_value, "mp", [(i, (i + shift) % count) for i in range(count)]
        )
    return total


def shards(
    block_input,
    segment_ids,
    expert_ids,
    norm_gain,
    query_weight,
    latent_down,
    latent_gain,
    latent_up,
    output_weight,
    moe_gain,
    router_weight,
    shared_gate,
    shared_up,
    shared_down,
    expert_gate,
    expert_up,
    expert_down,
    output_grad,
):
    model_width = norm_gain.shape[0]
    tokens_here = block_input.shape[0]
    share_width = block_input.shape[1]
    mp_count = lax.axis_size("mp")
    mp_place = lax.axis_index("mp")
    dp_count = lax.axis_size("dp")
    heads_here = H // mp_count
    experts_all = router_weight.shape[0]
    experts_group = experts_all // dp_count
    chips = dp_count // 2
    own_expert = lax.axis_index("dp") * experts_group + mp_place // 2
    expert_places = jnp.arange(experts_all, dtype=jnp.int32)
    own_gate = expert_gate[0]
    own_up = expert_up[0]
    own_down = expert_down[0]
    cosine, sine_tab = rope_tables(LEN, DR)
    inputs = block_input.astype(jnp.float32)
    gain_one = lax.dynamic_slice_in_dim(norm_gain, mp_place * share_width, share_width)
    per_head = query_weight.reshape(heads_here, DN + DR, -1)
    query_rows = jnp.concatenate(
        [
            per_head[:, :DN].reshape(heads_here * DN, -1),
            per_head[:, DN : DN + DR // 2].reshape(heads_here * DR // 2, -1),
            per_head[:, DN + DR // 2 :].reshape(heads_here * DR // 2, -1),
        ],
        axis=0,
    )
    gathered = gather_all(
        block_input,
        (query_rows, latent_down, latent_up.T, output_weight, router_weight),
        (1, 1, 0, 1, 1),
        1,
    )
    inputs_full = gathered[0].astype(jnp.float32)
    query_w, down_w, up_wt, out_w, router_w = gathered[1:]
    scale_one = lax.rsqrt(jnp.mean(inputs_full * inputs_full, axis=1, keepdims=True) + epsilon)
    normed = (inputs_full * scale_one * norm_gain).astype(jnp.bfloat16)
    places = relative_devices()
    late_ids, _ = lax.optimization_barrier((expert_ids, gathered[0]))
    picked_mask = jnp.max((late_ids[..., None] == expert_places).astype(jnp.float32), axis=1)
    mask_pairs = spread_pairs(picked_mask)
    shared_parts, _ = lax.optimization_barrier(
        (jnp.concatenate([shared_gate, shared_up, shared_down], axis=0), gathered[0])
    )
    shared_pieces = [piece for pair in spread_pairs(shared_parts) for piece in pair]
    hidden_here = shared_gate.shape[0]
    places_flat = jnp.stack([place for pair in places for place in pair]).astype(jnp.int32)
    sgate_w, sup_w, sdown_w = assemble(shared_pieces, places_flat, 3)
    late_grad, _ = lax.optimization_barrier((output_grad, gathered[0]))
    grad_full = full_rows(late_grad)
    grad_pairs = spread_halves(grad_full)
    nope_width, rope_width = heads_here * DN, heads_here * DR
    query_all = jnp.dot(normed, query_w.T, preferred_element_type=jnp.float32)
    cosines, sines = jnp.tile(cosine, (1, heads_here)), jnp.tile(sine_tab, (1, heads_here))
    query_nope = query_all[:, :nope_width].astype(jnp.bfloat16)
    query_rope = rotate(query_all[:, nope_width:], cosines, sines).astype(jnp.bfloat16)
    score_scale = (DN + DR) ** (-0.5)
    latent_part = jnp.dot(normed, down_w.T, preferred_element_type=jnp.float32).astype(
        jnp.bfloat16
    )
    latent = full_rows(latent_part).astype(jnp.float32)
    latent_main = latent[:, :KVL]
    scale_lat = lax.rsqrt(jnp.mean(latent_main * latent_main, axis=-1, keepdims=True) + epsilon)
    latent_normed = (latent_main * scale_lat * latent_gain).astype(jnp.bfloat16)
    key_rope = rotate(latent[:, KVL:], cosine, sine_tab).astype(jnp.bfloat16)
    key_rope = jnp.concatenate(
        [key_rope[:, : DR // 2]] * heads_here + [key_rope[:, DR // 2 :]] * heads_here, axis=1
    )
    keys_values = jnp.dot(latent_normed, up_wt, preferred_element_type=jnp.float32).astype(
        jnp.bfloat16
    )
    attended_flat, probs = attend_forward(
        query_nope, query_rope, keys_values, key_rope, segment_ids, heads_here, score_scale
    )
    attended_part = jnp.dot(attended_flat, out_w, preferred_element_type=jnp.float32).astype(
        jnp.bfloat16
    )
    attended_sum = mp_share(attended_part)
    residual = inputs + attended_sum
    residual_rounded = residual.astype(jnp.bfloat16)
    gain_two = lax.dynamic_slice_in_dim(moe_gain, mp_place * share_width, share_width)
    residual_full = full_rows(residual_rounded)
    residual_full = residual_full.astype(jnp.float32)
    scale_two = lax.rsqrt(
        jnp.mean(residual_full * residual_full, axis=1, keepdims=True) + epsilon
    )
    moe_in = (residual_full * scale_two * moe_gain).astype(jnp.bfloat16)
    row_pairs = spread_halves(moe_in)
    router_logits = jnp.dot(moe_in, router_w.T, preferred_element_type=jnp.float32)

    def masked_gates(logits, mask):
        pick_exp = jnp.exp(jnp.where(mask > 0, logits, negative))
        return pick_exp / jnp.sum(pick_exp, axis=-1, keepdims=True)

    gate_prob = masked_gates(router_logits, picked_mask)
    shared_g = jnp.dot(moe_in, sgate_w.T, preferred_element_type=jnp.float32)
    shared_u = jnp.dot(moe_in, sup_w.T, preferred_element_type=jnp.float32)
    shared_act = (jax.nn.silu(shared_g) * shared_u).astype(jnp.bfloat16)
    shared_part = jnp.dot(shared_act, sdown_w, preferred_element_type=jnp.float32)
    up_router = jnp.concatenate([own_up, router_w], axis=0)
    own_column = (expert_places == own_expert).astype(jnp.float32)[:, None]
    backs, gate_grads, held = [None] * chips, [None] * chips, ()
    visits = [0]
    for hop in range(1, chips // 2):
        visits += [hop, chips - hop]
    visits.insert(len(visits) - 1, chips // 2)
    for k in visits:
        done = expert_rows(
            k,
            chips,
            row_pairs[k],
            grad_pairs[k],
            jnp.concatenate(mask_pairs[k]).T,
            own_column,
            own_gate,
            up_router,
            own_down,
            held,
        )
        *back, gate_grads[k] = done[:3]
        backs[k], held = tuple(back), done[3:]
    routed_back = collect(backs)
    act_late, _ = lax.optimization_barrier((held[0], routed_back))
    tokens_pair = 2 * tokens_here

    def out_rows(low):
        return jnp.dot(
            act_late[:, low : low + tokens_here].T,
            own_down,
            preferred_element_type=jnp.float32,
        ).astype(jnp.bfloat16)

    out_pairs = [
        (out_rows(k * tokens_pair), out_rows(k * tokens_pair + tokens_here))
        for k in range(chips)
    ]
    act_all, gate_pre_all, up_pre_all, rows_all, grads_all = held
    expert_down_grad = jnp.dot(act_all, grads_all, preferred_element_type=jnp.float32)[None]
    expert_gate_grad = jnp.dot(
        gate_pre_all, rows_all, preferred_element_type=jnp.float32
    )[None]
    expert_up_grad = jnp.dot(up_pre_all, rows_all, preferred_element_type=jnp.float32)[None]
    gate_grads, _ = lax.optimization_barrier((gate_grads, routed_back))
    _, ring_place, core_here, device_at = ring_neighbours(dp_count)
    gate_grad = jnp.zeros((tokens_here, experts_all), jnp.float32)
    for k, both in enumerate(gate_grads):
        same_from = device_at(ring_place + k)
        for swap in range(2):
            piece = both[0, swap * tokens_here : (swap + 1) * tokens_here]
            if k or swap:
                piece = direct_move(piece, -k, swap)
            device_from = same_from + swap * (1 - 2 * core_here)
            expert_from = device_from * experts_group + mp_place // 2
            gate_grad = gate_grad + piece[:, None] * (expert_places == expert_from).astype(
                jnp.float32
            )
    gate_grad = line_total(gate_grad)
    routed_part = collect(out_pairs)
    moe_total = mp_share(shared_part + routed_part)
    block_output = (residual + moe_total).astype(jnp.bfloat16)
    logit_grad = (
        gate_prob * (gate_grad - jnp.sum(gate_prob * gate_grad, axis=-1, keepdims=True))
    ).astype(jnp.bfloat16)
    router_back = jnp.dot(logit_grad, router_w, preferred_element_type=jnp.float32)
    shared_act_grad = jnp.dot(grad_full, sdown_w.T, preferred_element_type=jnp.float32)
    shared_gate_pre = (shared_act_grad * shared_u * silu_grad(shared_g)).astype(jnp.bfloat16)
    shared_up_pre = (shared_act_grad * jax.nn.silu(shared_g)).astype(jnp.bfloat16)
    moe_late, grad_late, shared_late, _ = lax.optimization_barrier(
        (
            moe_in,
            grad_full,
            (shared_act, shared_gate_pre, shared_up_pre, logit_grad),
            routed_back,
        )
    )
    sdown_grad = weight_grads(grad_late, shared_late[0], places)
    moe_rows_grad = weight_grads(moe_late, jnp.concatenate(shared_late[1:], axis=1), places)
    shared_back = jnp.dot(shared_gate_pre, sgate_w, preferred_element_type=jnp.float32)
    shared_back_up = jnp.dot(shared_up_pre, sup_w, preferred_element_type=jnp.float32)
    shared_back = shared_back + shared_back_up
    router_mine = lax.dynamic_slice_in_dim(router_back, mp_place * share_width, share_width, axis=1)
    back_share = mp_share(shared_back + routed_back)
    moe_in_grad = back_share + router_mine
    moe_in_grad_bf = moe_in_grad.astype(jnp.bfloat16)
    back_full = full_rows(moe_in_grad_bf)
    back_full = back_full.astype(jnp.float32)
    moe_gain_part = jnp.sum(back_full * residual_full * scale_two, axis=0)
    stat_two = jnp.mean(back_full * residual_full * moe_gain, axis=1, keepdims=True)
    residual_grad = (
        output_grad.astype(jnp.float32)
        + scale_two * gain_two * moe_in_grad
        - residual * scale_two**3 * stat_two
    )
    residual_bf = (
        grad_full.astype(jnp.float32)
        + scale_two * moe_gain * back_full
        - residual_full * scale_two**3 * stat_two
    ).astype(jnp.bfloat16)
    out_w_grad = weight_grads(residual_bf, attended_flat, places)
    attended_grad = jnp.dot(residual_bf, out_w.T, preferred_element_type=jnp.float32).astype(
        jnp.bfloat16
    )
    dq_nope, dq_rope, kv_grad, dk_ropes = attend_backward(
        probs,
        attended_grad,
        query_nope,
        query_rope,
        keys_values,
        key_rope,
        heads_here,
        score_scale,
    )
    query_grad = jnp.concatenate(
        [dq_nope, unrotate(dq_rope, cosines, sines).astype(jnp.bfloat16)], axis=1
    )
    dk_rope = jnp.sum(dk_ropes.reshape(-1, 2, heads_here, DR // 2), axis=2).reshape(-1, DR)
    up_w_grad = weight_grads(latent_normed, kv_grad, places)
    normed_lat_grad = jnp.dot(kv_grad, up_wt.T, preferred_element_type=jnp.float32)
    latent_gain_part = jnp.sum(normed_lat_grad * latent_main * scale_lat, axis=0)
    main_grad = scale_lat * latent_gain * normed_lat_grad - latent_main * scale_lat**3 * jnp.mean(
        normed_lat_grad * latent_main * latent_gain, axis=-1, keepdims=True
    )
    rope_grad = unrotate(dk_rope, cosine, sine_tab)
    latent_grad = line_share(jnp.concatenate([main_grad, rope_grad], axis=-1)).astype(jnp.bfloat16)
    query_rows_grad = weight_grads(
        normed, jnp.concatenate([query_grad, latent_grad], axis=1), places
    )
    normed_part = jnp.dot(query_grad, query_w, preferred_element_type=jnp.float32) + jnp.dot(
        latent_grad, down_w, preferred_element_type=jnp.float32
    )
    weighted_part = normed_part * inputs_full
    norm_gain_part = jnp.sum(weighted_part * scale_one, axis=0)
    stat_one = line_total(jnp.sum(weighted_part * norm_gain, axis=1))[:, None] / model_width
    moe_gain_part = jnp.where(mp_place == 0, moe_gain_part, 0.0)
    gain_total = small_total(
        jnp.concatenate([norm_gain_part, moe_gain_part, latent_gain_part]).reshape(-1, 128), 2
    ).reshape(-1)
    norm_gain_grad = gain_total[:model_width]
    moe_gain_grad = gain_total[model_width : 2 * model_width]
    latent_gain_grad = gain_total[2 * model_width :]
    normed_grad = mp_share(normed_part)
    input_grad = (
        residual_grad + scale_one * gain_one * normed_grad - inputs * scale_one**3 * stat_one
    )
    query_width = query_grad.shape[1]
    query_rows_grad, down_rows_grad = (
        query_rows_grad[:, :query_width].T,
        query_rows_grad[:, query_width:].T,
    )
    parts = [query_rows_grad[:nope_width].reshape(heads_here, DN, -1)]
    for half in range(2):
        low = nope_width + half * rope_width // 2
        parts.append(
            query_rows_grad[low : low + rope_width // 2].reshape(heads_here, DR // 2, -1)
        )
    query_weight_grad = jnp.concatenate(parts, axis=1).reshape(query_width, -1)
    latent_down_grad = down_rows_grad
    latent_up_grad = up_w_grad.T
    output_weight_grad = out_w_grad.T
    shared_gate_grad = moe_rows_grad[:, :hidden_here].T
    shared_up_grad = moe_rows_grad[:, hidden_here : 2 * hidden_here].T
    router_grad = moe_rows_grad[:, 2 * hidden_here :].T
    shared_down_grad = sdown_grad.T
    return (
        block_output,
        input_grad,
        norm_gain_grad,
        query_weight_grad,
        latent_down_grad,
        latent_gain_grad,
        latent_up_grad,
        output_weight_grad,
        moe_gain_grad,
        router_grad,
        shared_gate_grad,
        shared_up_grad,
        shared_down_grad,
        expert_gate_grad,
        expert_up_grad,
        expert_down_grad,
    )


def solution(mesh):
    in_specs = (
        P("dp", "mp"),
        P("dp", None),
        P("dp", None),
        P(),
        P("mp", "dp"),
        P("mp", "dp"),
        P(),
        P("mp", "dp"),
        P("mp", "dp"),
        P(),
        P(None, "dp"),
        P("mp", "dp"),
        P("mp", "dp"),
        P("mp", "dp"),
        P(("dp", "mp"), None, None),
        P(("dp", "mp"), None, None),
        P(("dp", "mp"), None, None),
        P("dp", "mp"),
    )
    out_specs = (
        P("dp", "mp"),
        P("dp", "mp"),
        P(),
        P("mp", "dp"),
        P("mp", "dp"),
        P(),
        P("mp", "dp"),
        P("mp", "dp"),
        P(),
        P(None, "dp"),
        P("mp", "dp"),
        P("mp", "dp"),
        P("mp", "dp"),
        P(("dp", "mp"), None, None),
        P(("dp", "mp"), None, None),
        P(("dp", "mp"), None, None),
    )

    return jax.shard_map(shards, mesh=mesh, in_specs=in_specs, out_specs=out_specs, check_vma=False)
```
